64 devices in a mesh: dp: 4 (over x, y), tp: 16 (over z, core).
Axes of the slice: x: 2, y: 2, z: 8, core: 2. Of those that a mesh axis runs over, the one named last changes fastest.
The devices are a block of a 4x4x8 slice.
Arguments:
- act_in: bfloat16 [384, 64, 2048], P('dp'), parts along dimension 0
- ln_gain: float32 [2, 2048], replicated
- ln_bias: float32 [2, 2048], replicated
- w_qkv: bfloat16 [2, 2048, 16, 384], P(None, None, 'tp')
- w_out: bfloat16 [2, 2048, 2048], P(None, 'tp')
- w_up: bfloat16 [2, 2048, 8192], P(None, None, 'tp')
- w_down: bfloat16 [2, 8192, 2048], P(None, 'tp')
Outputs:
- output: bfloat16 [384, 64, 2048], P('dp'), parts along dimension 0
There are 4 independent parts. The reference program is written for one: setup_inputs(seed, part) draws one part's arguments, and reference() takes and returns one part's arrays. A program takes and returns all parts, laid end to end along the dimension named above; an argument that names none is the same for every part.
All inputs are finite; a program needn't handle non-finite values.
Results may differ from the reference program's by a relative error of at most 0.02.
Values are sent between devices in bfloat16 or wider.
A program may use at most 768 MiB of HBM per device.

```python
import math
import jax
import jax.numpy as jnp
from jax import lax

D_MODEL = 2048
HEADS = 16
KV_HEADS = 16
HEAD_DIM = 128
FF_DIM = 8192
BATCH = 96
SEQ_LEN = 64
LAYERS = 2

GROUP_HEADS = HEADS // KV_HEADS
LN_EPS = 1e-5
ROPE_BASE = 10000.0
QUERY_GAIN = 2.0


def setup_inputs(seed: int = 0, part: int = 0) -> dict:
    base_key = jax.random.key(seed)
    part_key = jax.random.fold_in(base_key, part)
    key_list = jax.random.split(base_key, 6)
    group_cols = (GROUP_HEADS + 2) * HEAD_DIM
    col_gain = jnp.where(jnp.arange(group_cols) < GROUP_HEADS * HEAD_DIM, QUERY_GAIN, 1.0)
    act_in = jax.random.normal(part_key, (BATCH, SEQ_LEN, D_MODEL), jnp.float32)
    ln_gain = 1.0 + 0.2 * jax.random.normal(key_list[0], (LAYERS, D_MODEL), jnp.float32)
    ln_bias = 0.3 * jax.random.normal(key_list[1], (LAYERS, D_MODEL), jnp.float32)
    w_qkv = jax.random.normal(key_list[2], (LAYERS, D_MODEL, KV_HEADS, group_cols), jnp.float32) * col_gain * D_MODEL ** -0.5
    w_out = jax.random.normal(key_list[3], (LAYERS, HEADS * HEAD_DIM, D_MODEL), jnp.float32) * (1.5 * (HEADS * HEAD_DIM) ** -0.5)
    w_up = jax.random.normal(key_list[4], (LAYERS, D_MODEL, FF_DIM), jnp.float32) * D_MODEL ** -0.5
    w_down = jax.random.normal(key_list[5], (LAYERS, FF_DIM, D_MODEL), jnp.float32) * FF_DIM ** -0.5
    return {"act_in": act_in.astype(jnp.bfloat16), "ln_gain": ln_gain, "ln_bias": ln_bias, "w_qkv": w_qkv.astype(jnp.bfloat16), "w_out": w_out.astype(jnp.bfloat16), "w_up": w_up.astype(jnp.bfloat16), "w_down": w_down.astype(jnp.bfloat16)}


def layer_norm(hidden, gain, bias):
    hidden_f = hidden.astype(jnp.float32)
    row_mean = jnp.mean(hidden_f, axis=-1, keepdims=True)
    centered = hidden_f - row_mean
    row_var = jnp.mean(centered * centered, axis=-1, keepdims=True)
    return (centered * lax.rsqrt(row_var + LN_EPS) * gain + bias).astype(jnp.bfloat16)


def rope_tables():
    half_dim = HEAD_DIM // 2
    inv_freq = ROPE_BASE ** (-2.0 * jnp.arange(half_dim, dtype=jnp.float32) / HEAD_DIM)
    angles = jnp.arange(SEQ_LEN, dtype=jnp.float32)[:, None] * inv_freq[None, :]
    return jnp.cos(angles), jnp.sin(angles)


def apply_rope(proj, cos_tab, sin_tab):
    half_dim = proj.shape[-1] // 2
    first = proj[..., :half_dim]
    second = proj[..., half_dim:]
    return jnp.concatenate([first * cos_tab - second * sin_tab, second * cos_tab + first * sin_tab], axis=-1)


def attend_sequence(operands):
    query, keys, values = operands
    scores = jnp.einsum("sgrd,tgd->grst", query.astype(jnp.float32), keys.astype(jnp.float32)) / math.sqrt(HEAD_DIM)
    positions = jnp.arange(SEQ_LEN)
    allowed = positions[:, None] >= positions[None, :]
    scores = jnp.where(allowed, scores, -1e30)
    attn_probs = jax.nn.softmax(scores, axis=-1).astype(jnp.bfloat16)
    context = jnp.einsum("grst,tgd->sgrd", attn_probs.astype(jnp.float32), values.astype(jnp.float32))
    return context.astype(jnp.bfloat16)


def layer_step(hidden, params):
    gain, bias, w_qkv, w_out, w_up, w_down = params
    normed = layer_norm(hidden, gain, bias)
    flat = normed.reshape(BATCH * SEQ_LEN, D_MODEL)
    qkv_proj = jnp.dot(flat, w_qkv.reshape(D_MODEL, -1), preferred_element_type=jnp.float32)
    qkv_proj = qkv_proj.reshape(BATCH, SEQ_LEN, KV_HEADS, GROUP_HEADS + 2, HEAD_DIM)
    cos_tab, sin_tab = rope_tables()
    query = apply_rope(qkv_proj[:, :, :, :GROUP_HEADS], cos_tab[None, :, None, None, :], sin_tab[None, :, None, None, :]).astype(jnp.bfloat16)
    keys = apply_rope(qkv_proj[:, :, :, GROUP_HEADS], cos_tab[None, :, None, :], sin_tab[None, :, None, :]).astype(jnp.bfloat16)
    values = qkv_proj[:, :, :, GROUP_HEADS + 1].astype(jnp.bfloat16)
    context = lax.map(attend_sequence, (query, keys, values))
    attn_part = jnp.dot(context.reshape(BATCH * SEQ_LEN, HEADS * HEAD_DIM), w_out, preferred_element_type=jnp.float32)
    up_proj = jnp.dot(flat, w_up, preferred_element_type=jnp.float32)
    gelu_out = jax.nn.gelu(up_proj, approximate=False).astype(jnp.bfloat16)
    mlp_part = jnp.dot(gelu_out, w_down, preferred_element_type=jnp.float32)
    update = (attn_part + mlp_part).astype(jnp.bfloat16).reshape(BATCH, SEQ_LEN, D_MODEL)
    new_hidden = (hidden.astype(jnp.float32) + update.astype(jnp.float32)).astype(jnp.bfloat16)
    return new_hidden, None


def reference(act_in, ln_gain, ln_bias, w_qkv, w_out, w_up, w_down):
    act_out = lax.scan(layer_step, act_in, (ln_gain, ln_bias, w_qkv, w_out, w_up, w_down))[0]
    return act_out
```

```python
import functools
import math

import jax
import jax.numpy as jnp
from jax import lax
from jax.experimental import pallas as pl
from jax.experimental.pallas import tpu as pltpu
from jax.sharding import PartitionSpec as P

LN_EPS = 1e-5
ROPE_BASE = 10000.0
MESH = pl.DeviceIdType.MESH
BF16 = jnp.bfloat16
F32 = jnp.float32
LANES = 128
UP, Q, K, V, DOWN, OUT = range(6)


def norm_rows(hidden_f, gain, bias):
    row_mean = jnp.mean(hidden_f, axis=-1, keepdims=True)
    centered = hidden_f - row_mean
    row_var = jnp.mean(centered * centered, axis=-1, keepdims=True)
    return (centered * lax.rsqrt(row_var + LN_EPS) * gain + bias).astype(BF16)


def rope(heads, cos, sin):
    return (heads * cos + pltpu.roll(heads, heads.shape[-1] // 2, 1) * sin).astype(BF16)


def gelu(values):
    return (0.5 * values * (1.0 + lax.erf(values * math.sqrt(0.5)))).astype(BF16)


def attend(query, keys, values, seq_len):
    rows, head_dim = query.shape
    scores = lax.dot_general(query, keys, (((1,), (1,)), ((), ())), preferred_element_type=F32) * (head_dim ** -0.5)
    row = lax.broadcasted_iota(jnp.int32, (rows, rows), 0)
    col = lax.broadcasted_iota(jnp.int32, (rows, rows), 1)
    allowed = (row >= col) & (row // seq_len == col // seq_len)
    scores = jnp.where(allowed, scores, -1e30)
    weights = jnp.exp(scores - jnp.max(scores, axis=-1, keepdims=True))
    probs = (weights / jnp.sum(weights, axis=-1, keepdims=True)).astype(BF16)
    return jnp.dot(probs, values, preferred_element_type=F32).astype(BF16)


def branches(normed, qkv_w, up_w, cos_ref, sin_ref, ctx, act, seq_len):
    head_dim = cos_ref.shape[1]
    for head in range(ctx.shape[1] // head_dim):
        cols = pl.ds(3 * head_dim * head, 3 * head_dim)
        proj = jnp.dot(normed[...], qkv_w[:, cols], preferred_element_type=F32)
        query = rope(proj[:, :head_dim], cos_ref[...], sin_ref[...])
        keys = rope(proj[:, head_dim : 2 * head_dim], cos_ref[...], sin_ref[...])
        values = proj[:, 2 * head_dim :].astype(BF16)
        ctx[:, pl.ds(head * head_dim, head_dim)] = attend(query, keys, values, seq_len)
    step = 512
    for first in range(0, act.shape[1], step):
        cols = pl.ds(first, step)
        act[:, cols] = gelu(jnp.dot(normed[...], up_w[:, cols], preferred_element_type=F32))


class Place:
    def __init__(self, n_dp, n_tp):
        side = math.isqrt(n_dp)
        assert side * side == n_dp and side % 2 == 0 and n_tp % 4 == 0
        self.n_tp, self.nz = n_tp, n_tp // 2
        self.dp, self.tp = lax.axis_index("dp"), lax.axis_index("tp")
        self.z, self.core = self.tp // 2, self.tp % 2
        x, y = self.dp // side, self.dp % side
        xf, yf = x + 1 - 2 * (x % 2), y + 1 - 2 * (y % 2)
        self.q = (x % 2) * 2 + y % 2
        self.peers = [{"dp": xf * side + y}, {"dp": x * side + yf}, {"dp": xf * side + yf}]
        self.peer_q = [(1 - x % 2) * 2 + y % 2, (x % 2) * 2 + 1 - y % 2, (1 - x % 2) * 2 + 1 - y % 2]
        self.sib = {"tp": 2 * self.z + 1 - self.core}
        self.right = {"tp": 2 * ((self.z + 1) % self.nz) + self.core}
        self.left = {"tp": 2 * ((self.z + self.nz - 1) % self.nz) + self.core}

    def meet(self):
        barrier = pltpu.get_barrier_semaphore()
        others = [self.sib, self.right, self.left, *self.peers]
        for other in others:
            pl.semaphore_signal(barrier, inc=1, device_id=other, device_id_type=MESH)
        pl.semaphore_wait(barrier, len(others))


def remote(src, dst, send_sem, recv_sem, device):
    return pltpu.make_async_remote_copy(src_ref=src, dst_ref=dst, send_sem=send_sem, recv_sem=recv_sem, device_id=device, device_id_type=MESH)


def piece(kind, source, n_tp, cols, rows):
    if kind == UP:
        return cols.at[source]
    if kind == DOWN:
        return rows.at[source]
    if kind == OUT:
        return rows.at[n_tp + source // 4]
    return cols.at[n_tp + 3 * (source // 4) + kind - Q]


def first_kernel(n_dp, n_tp, x, gains, biases, cos_ref, sin_ref, qkv, out_w, up, down,
                 y1, nall, gcols, grows,
                 qkv_v, out_v, up_v, down_v, xbuf, normed, ctx, act, own, sib_out, sib_in, ring_r, ring_l, nown, st_cols, st_rows,
                 w_sem, x_sem, sib_send, sib_recv, r_send, r_recv, l_send, l_recv,
                 st_sem, own_sem, loc_sem, wr_recv, wr_send, ws_send, ws_recv, n_send, n_recv, n_loc):
    me = Place(n_dp, n_tp)
    nz, core, z, q = me.nz, me.core, me.z, me.q
    n_seq, seq_len, d_model = x.shape
    per = n_seq // n_tp
    half = per // 2
    steps = nz * half

    first_w = [pltpu.make_async_copy(src.at[0], dst, w_sem.at[i]) for i, (src, dst) in enumerate(((qkv, qkv_v), (up, up_v), (out_w, out_v), (down, down_v)))]

    def owner_seq(zo, co, j):
        return per * (2 * zo + co) + j

    def tile_seqs(i):
        s, j = i // half, i % half
        zr, zl = (z + 2 * nz - 1 - s) % nz, (z + 1 + s) % nz
        return [owner_seq(zr, core, j), owner_seq(zl, core, half + j), owner_seq(zr, 1 - core, j), owner_seq(zl, 1 - core, half + j)]

    def fetch(i):
        for place, seq in enumerate(tile_seqs(i)):
            pltpu.make_async_copy(x.at[seq], xbuf.at[i % 3, place], x_sem.at[i % 3]).start()

    fetch(0)
    for copy in first_w:
        copy.start()
    head_dim = out_w.shape[1]
    loads = {UP: (up.at[1, :, pl.ds(pl.multiple_of(q * LANES, LANES), LANES)], st_cols.at[UP]),
             DOWN: (down.at[1, pl.ds(pl.multiple_of(q * LANES, LANES), LANES), :], st_rows.at[0]),
             OUT: (out_w.at[1], st_rows.at[1])}
    for kind in (Q, K, V):
        loads[kind] = (qkv.at[1, :, pl.ds((kind - Q) * head_dim, head_dim)], st_cols.at[kind])
    kinds = (UP, DOWN, Q, K, V, OUT)
    loads = {kind: pltpu.make_async_copy(*loads[kind], st_sem.at[kind]) for kind in kinds}
    for kind in kinds:
        loads[kind].start()
    me.meet()

    def has(kind, source):
        return source >= 0 if kind in (UP, DOWN) else source % 4 == q

    def staged(kind):
        return st_rows.at[kind - DOWN] if kind >= DOWN else st_cols.at[kind]

    def first_hops(kind):
        src, dst = staged(kind), piece(kind, me.tp, n_tp, gcols, grows)
        return [remote(src, dst, own_sem.at[0, kind], wr_recv.at[0, 0, kind], me.right),
                remote(src, dst, own_sem.at[1, kind], wr_recv.at[1, 0, kind], me.left),
                remote(src, dst, own_sem.at[2, kind], ws_recv.at[z, kind], me.sib),
                pltpu.make_async_copy(src, dst, loc_sem.at[kind])]

    for kind in kinds:
        loads[kind].wait()

        @pl.when(has(kind, me.tp))
        def _():
            for copy in first_hops(kind):
                copy.start()

    for i in range(half):
        ring_r[i] = jnp.zeros(ring_r.shape[1:], BF16)
        ring_l[i] = jnp.zeros(ring_l.shape[1:], BF16)

    def send_sib(i):
        return remote(sib_out.at[i % 2], sib_in.at[i % 4], sib_send.at[i % 2], sib_recv.at[i % 4], me.sib)

    def send_r(i):
        return remote(ring_r.at[i], ring_r.at[i + half], r_send.at[i], r_recv.at[i + half], me.right)

    def send_l(i):
        return remote(ring_l.at[i], ring_l.at[i + half], l_send.at[i], l_recv.at[i + half], me.left)

    def send_n(seq, peer):
        return remote(nown.at[seq], nall.at[seq, q], n_send.at[peer, seq], n_recv.at[peer, seq], me.peers[peer])

    def wait_n(seq, peer):
        return remote(nown.at[seq], nall.at[seq, me.peer_q[peer]], n_send.at[peer, seq], n_recv.at[peer, seq], me.peers[peer])

    def keep_n(seq):
        return pltpu.make_async_copy(nown.at[seq], nall.at[seq, q], n_loc.at[seq])

    for copy in first_w:
        copy.wait()

    def compute(i):
        slot = i % 3
        pltpu.make_async_copy(x.at[pl.ds(0, 4)], xbuf.at[slot], x_sem.at[slot]).wait()

        @pl.when(i + 1 < steps)
        def _():
            fetch(i + 1)

        rows = 16

        def norm(k, carry):
            at = pl.ds(pl.multiple_of(k % (seq_len // rows) * rows, rows), rows)
            tile = xbuf[slot, k // (seq_len // rows), at, :].astype(F32)
            normed[pl.ds(pl.multiple_of(k * rows, rows), rows), :] = norm_rows(tile, gains[pl.ds(0, 1), :], biases[pl.ds(0, 1), :])
            return carry

        lax.fori_loop(0, 4 * seq_len // rows, norm, 0, unroll=2)
        branches(normed, qkv_v, up_v, cos_ref, sin_ref, ctx, act, seq_len)

        @pl.when(i >= 2)
        def _():
            send_sib(i - 2).wait_send()

        step = 512
        for first in range(0, d_model, step):
            cols = pl.ds(first, step)
            part = jnp.dot(ctx[...], out_v[:, cols], preferred_element_type=F32) + jnp.dot(act[...], down_v[:, cols], preferred_element_type=F32)
            own[i % 2, :, cols] = part[: 2 * seq_len]
            sib_out[i % 2, :, cols] = part[2 * seq_len :].astype(BF16)
        send_sib(i).start()

    def finish(i):
        send_sib(i).wait_recv()

        @pl.when(i >= half)
        def _():
            send_r(i - half).wait_recv()
            send_l(i - half).wait_recv()

        last = i >= steps - half

        @pl.when(jnp.logical_not(last))
        def _():
            for side, ring in enumerate((ring_r, ring_l)):
                at = pl.ds(side * seq_len, seq_len)
                ring[i] = (own[i % 2, at, :] + sib_in[i % 4, at, :].astype(F32) + ring[i].astype(F32)).astype(BF16)
            send_r(i).start()
            send_l(i).start()

        @pl.when(last)
        def _():
            rows = 16
            for side, ring in enumerate((ring_r, ring_l)):
                seq = side * half + i % half

                def close(k, carry):
                    at = pl.ds(pl.multiple_of(k * rows, rows), rows)
                    both = pl.ds(pl.multiple_of(side * seq_len + k * rows, rows), rows)
                    update = (own[i % 2, both, :] + sib_in[i % 4, both, :].astype(F32) + ring[i, at, :].astype(F32)).astype(BF16)
                    hidden = (xbuf[i % 3, side, at, :].astype(F32) + update.astype(F32)).astype(BF16)
                    y1[seq, at, :] = hidden
                    nown[seq, at, :] = norm_rows(hidden.astype(F32), gains[pl.ds(1, 1), :], biases[pl.ds(1, 1), :])
                    return carry

                lax.fori_loop(0, seq_len // rows, close, 0)
                for peer in range(3):
                    send_n(seq, peer).start()
                keep_n(seq).start()

    def turn(i, carry):
        @pl.when(i < steps)
        def _():
            compute(i)

        @pl.when(i >= 1)
        def _():
            finish(i - 1)

        return carry

    lax.fori_loop(0, steps + 1, turn, 0)

    hops = (nz // 2 - core, nz // 2 - 1 + core)
    to = (me.right, me.left)

    def source_of(side, s):
        zs = (z + nz - s) % nz if side == 0 else (z + s) % nz
        return 2 * zs + core

    def onward(side, s, kind):
        at = piece(kind, source_of(side, s), n_tp, gcols, grows)
        return remote(at, at, wr_send.at[side, s - 1, kind], wr_recv.at[side, s, kind], to[side])

    def arrival(side, s, kind):
        at = piece(kind, source_of(side, s), n_tp, gcols, grows)
        return remote(at, at, wr_send.at[side, s - 1, kind], wr_recv.at[side, s - 1, kind], to[side])

    def across(side, s, kind):
        source = source_of(side, s)
        at = piece(kind, source, n_tp, gcols, grows)
        return remote(at, at, ws_send.at[side, s - 1, kind], ws_recv.at[source // 2, kind], me.sib)

    for s in range(1, nz // 2 + 1):
        for kind in kinds:
            for side in range(2):
                @pl.when(has(kind, source_of(side, s)) & (s <= hops[side]))
                def _():
                    arrival(side, s, kind).wait_recv()

                    @pl.when(s < hops[side])
                    def _():
                        onward(side, s, kind).start()

                    across(side, s, kind).start()

    def drain(i, carry):
        send_r(i).wait_send()
        send_l(i).wait_send()
        return carry

    lax.fori_loop(0, steps - half, drain, 0)
    send_sib(steps - 2).wait_send()
    send_sib(steps - 1).wait_send()
    for seq in range(per):
        for peer in range(3):
            send_n(seq, peer).wait_send()
            wait_n(seq, peer).wait_recv()
        keep_n(seq).wait()
    for kind in kinds:
        @pl.when(has(kind, me.tp))
        def _():
            right, left, sib, local = first_hops(kind)
            right.wait_send()
            left.wait_send()
            sib.wait_send()
            local.wait()

        for s in range(1, nz // 2 + 1):
            for side in range(2):
                @pl.when(has(kind, source_of(side, s)) & (s <= hops[side]))
                def _():
                    @pl.when(s < hops[side])
                    def _():
                        onward(side, s, kind).wait_send()

                    across(side, s, kind).wait_send()

        for zs in range(nz):
            source = 2 * zs + 1 - core

            @pl.when(has(kind, source))
            def _():
                at = piece(kind, source, n_tp, gcols, grows)
                remote(at, at, own_sem.at[2, kind], ws_recv.at[zs, kind], me.sib).wait_recv()


def second_kernel(n_dp, n_tp, y1, nall, gcols, grows, cos_ref, sin_ref, out,
                  qkv_v, out_v, up_v, down_v, nbuf, normed, ctx, act, own, part_out, part_in, ybuf,
                  w_sem, n_sem, p_send, p_recv, own_send, loc_sem, r_recv, f_send, s_send, s_recv):
    me = Place(n_dp, n_tp)
    nz, core, z, q = me.nz, me.core, me.z, me.q
    per, members, seq_len, d_model = nall.shape
    head_dim = cos_ref.shape[1]

    def fetch(i):
        return pltpu.make_async_copy(nall.at[i], nbuf.at[i % 2], n_sem.at[i % 2])

    fetch(0).start()
    n_cols, n_rows = gcols.shape[0], grows.shape[0]
    loads = []
    for i in range(n_cols - n_tp):
        loads.append((gcols.at[n_tp + i], qkv_v.at[:, pl.ds(i * LANES, LANES)]))
    for i in range(n_tp):
        loads.append((gcols.at[i], up_v.at[:, pl.ds(i * LANES, LANES)]))
    for i in range(n_rows - n_tp):
        loads.append((grows.at[n_tp + i], out_v.at[pl.ds(i * LANES, LANES), :]))
    for i in range(n_tp):
        loads.append((grows.at[i], down_v.at[pl.ds(i * LANES, LANES), :]))
    loads = [pltpu.make_async_copy(src, dst, w_sem.at[i]) for i, (src, dst) in enumerate(loads)]
    for copy in loads:
        copy.start()
    me.meet()
    for copy in loads:
        copy.wait()

    def send_part(i, peer):
        return remote(part_out.at[i % 2, me.peer_q[peer]], part_in.at[i, peer], p_send.at[i % 2, peer], p_recv.at[i, peer], me.peers[peer])

    def seq_of(zs, co, i):
        return per * (2 * zs + co) + i

    def first_hops(i):
        src, dst = ybuf.at[i], out.at[seq_of(z, core, i)]
        return [remote(src, dst, own_send.at[0, i], r_recv.at[0, i, 0], me.right),
                remote(src, dst, own_send.at[1, i], r_recv.at[1, i, 0], me.left),
                remote(src, dst, own_send.at[2, i], s_recv.at[z, i], me.sib),
                pltpu.make_async_copy(src, dst, loc_sem.at[i])]

    to = (me.right, me.left)

    def hops(side, i):
        longer = (i + core) % 2
        return nz // 2 - longer if side == 0 else nz // 2 - 1 + longer

    def z_of(side, s):
        return (z + nz - s) % nz if side == 0 else (z + s) % nz

    def arrival(side, i, s):
        at = out.at[seq_of(z_of(side, s), core, i)]
        return remote(at, at, f_send.at[side, i, s - 1], r_recv.at[side, i, s - 1], to[side])

    def onward(side, i, s):
        at = out.at[seq_of(z_of(side, s), core, i)]
        return remote(at, at, f_send.at[side, i, s - 1], r_recv.at[side, i, s], to[side])

    def across(side, i, s):
        at = out.at[seq_of(z_of(side, s), core, i)]
        return remote(at, at, s_send.at[side, i, s - 1], s_recv.at[z_of(side, s), i], me.sib)

    def compute(i):
        fetch(i).wait()

        @pl.when(i + 1 < per)
        def _():
            fetch(i + 1).start()

        for member in range(members):
            normed[pl.ds(member * seq_len, seq_len), :] = nbuf[i % 2, member]
        branches(normed, qkv_v, up_v, cos_ref, sin_ref, ctx, act, seq_len)

        @pl.when(i >= 2)
        def _():
            for peer in range(3):
                send_part(i - 2, peer).wait_send()

        step = 512
        for first in range(0, d_model, step):
            cols = pl.ds(first, step)
            part = jnp.dot(ctx[...], out_v[:, cols], preferred_element_type=F32) + jnp.dot(act[...], down_v[:, cols], preferred_element_type=F32)
            for member in range(members):
                rows = part[member * seq_len : (member + 1) * seq_len]
                part_out[i % 2, member, :, cols] = rows.astype(BF16)

                @pl.when(q == member)
                def _():
                    own[i % 2, :, cols] = rows
        for peer in range(3):
            send_part(i, peer).start()

    def finish(i):
        for peer in range(3):
            send_part(i, peer).wait_recv()
        total = own[i % 2]
        for peer in range(3):
            total = total + part_in[i, peer].astype(F32)
        ybuf[i] = (y1[i].astype(F32) + total.astype(BF16).astype(F32)).astype(BF16)
        for copy in first_hops(i):
            copy.start()

    def turn(t, carry):
        @pl.when(t < per)
        def _():
            compute(t)

        @pl.when((t >= 1) & (t <= per))
        def _():
            finish(t - 1)

        for s in range(1, nz // 2 + 1):
            i = t - 1 - s

            @pl.when((i >= 0) & (i < per))
            def _():
                for side in range(2):
                    @pl.when(s <= hops(side, i))
                    def _():
                        arrival(side, i, s).wait_recv()

                        @pl.when(s < hops(side, i))
                        def _():
                            onward(side, i, s).start()

                        across(side, i, s).start()

        return carry

    lax.fori_loop(0, per + 1 + nz // 2, turn, 0)

    for peer in range(3):
        send_part(per - 2, peer).wait_send()
        send_part(per - 1, peer).wait_send()

    def drain(i, carry):
        right, left, sib, local = first_hops(i)
        right.wait_send()
        left.wait_send()
        sib.wait_send()
        local.wait()
        for s in range(1, nz // 2 + 1):
            for side in range(2):
                @pl.when(s <= hops(side, i))
                def _():
                    @pl.when(s < hops(side, i))
                    def _():
                        onward(side, i, s).wait_send()

                    across(side, i, s).wait_send()
        for zs in range(nz):
            at = out.at[seq_of(zs, 1 - core, i)]
            remote(at, at, own_send.at[2, i], s_recv.at[zs, i], me.sib).wait_recv()
        return carry

    lax.fori_loop(0, per, drain, 0)


def rope_rows(seq_len, head_dim, copies):
    half_dim = head_dim // 2
    inv_freq = ROPE_BASE ** (-2.0 * jnp.arange(half_dim, dtype=F32) / head_dim)
    angles = jnp.arange(seq_len, dtype=F32)[:, None] * inv_freq[None, :]
    cos, sin = jnp.cos(angles), jnp.sin(angles)
    return jnp.tile(jnp.concatenate([cos, cos], 1), (copies, 1)), jnp.tile(jnp.concatenate([-sin, sin], 1), (copies, 1))


def solution(mesh):
    n_dp, n_tp = mesh.shape["dp"], mesh.shape["tp"]
    nz = n_tp // 2
    any_spec = pl.BlockSpec(memory_space=pl.ANY)
    vmem_spec = pl.BlockSpec(memory_space=pltpu.VMEM)
    dma = pltpu.SemaphoreType.DMA

    def shard_body(act_in, ln_gain, ln_bias, w_qkv, w_out, w_up, w_down):
        n_seq, seq_len, d_model = act_in.shape
        layers, _, _, qkv_cols = w_qkv.shape
        head_dim, ff = w_out.shape[1], w_up.shape[2]
        per = n_seq // n_tp
        half = per // 2
        heads = n_tp // 4
        tile = 4 * seq_len
        w_qkv = w_qkv.reshape(layers, d_model, qkv_cols)
        cos, sin = rope_rows(seq_len, head_dim, 4)
        seq_block = (seq_len, d_model)
        n_cols, n_rows = n_tp + 3 * heads, n_tp + heads
        steps = nz * half
        y1, nall, gcols, grows = pl.pallas_call(
            functools.partial(first_kernel, n_dp, n_tp),
            name="layer_one",
            out_shape=(jax.ShapeDtypeStruct((per, *seq_block), BF16), jax.ShapeDtypeStruct((per, 4, *seq_block), BF16),
                       jax.ShapeDtypeStruct((n_cols, d_model, LANES), BF16), jax.ShapeDtypeStruct((n_rows, LANES, d_model), BF16)),
            in_specs=[any_spec] + [vmem_spec] * 4 + [any_spec] * 4,
            out_specs=(vmem_spec, any_spec, any_spec, any_spec),
            scratch_shapes=[
                pltpu.VMEM((d_model, qkv_cols), BF16), pltpu.VMEM((head_dim, d_model), BF16), pltpu.VMEM((d_model, ff), BF16), pltpu.VMEM((ff, d_model), BF16),
                pltpu.VMEM((3, 4, *seq_block), BF16), pltpu.VMEM((tile, d_model), BF16), pltpu.VMEM((tile, head_dim), BF16), pltpu.VMEM((tile, ff), BF16),
                pltpu.VMEM((2, 2 * seq_len, d_model), F32), pltpu.VMEM((2, 2 * seq_len, d_model), BF16), pltpu.VMEM((4, 2 * seq_len, d_model), BF16),
                pltpu.VMEM((steps, *seq_block), BF16), pltpu.VMEM((steps, *seq_block), BF16), pltpu.VMEM((per, *seq_block), BF16),
                pltpu.VMEM((4, d_model, LANES), BF16), pltpu.VMEM((2, LANES, d_model), BF16),
                dma((4,)), dma((3,)), dma((2,)), dma((4,)), dma((steps,)), dma((steps,)), dma((steps,)), dma((steps,)),
                dma((6,)), dma((3, 6)), dma((6,)), dma((2, nz // 2, 6)), dma((2, nz // 2, 6)), dma((2, nz // 2, 6)), dma((nz, 6)),
                dma((3, per)), dma((3, per)), dma((per,)),
            ],
            compiler_params=pltpu.CompilerParams(collective_id=1, has_side_effects=True, vmem_limit_bytes=60 * 2**20),
        )(act_in, ln_gain, ln_bias, cos, sin, w_qkv, w_out, w_up, w_down)
        return pl.pallas_call(
            functools.partial(second_kernel, n_dp, n_tp),
            name="layer_two",
            out_shape=jax.ShapeDtypeStruct(act_in.shape, BF16),
            in_specs=[vmem_spec] + [any_spec] * 3 + [vmem_spec] * 2,
            out_specs=any_spec,
            scratch_shapes=[
                pltpu.VMEM((d_model, heads * qkv_cols), BF16), pltpu.VMEM((heads * head_dim, d_model), BF16), pltpu.VMEM((d_model, n_tp * LANES), BF16), pltpu.VMEM((n_tp * LANES, d_model), BF16),
                pltpu.VMEM((2, 4, *seq_block), BF16), pltpu.VMEM((tile, d_model), BF16), pltpu.VMEM((tile, heads * head_dim), BF16), pltpu.VMEM((tile, n_tp * LANES), BF16),
                pltpu.VMEM((2, *seq_block), F32), pltpu.VMEM((2, 4, *seq_block), BF16), pltpu.VMEM((per, 3, *seq_block), BF16), pltpu.VMEM((per, *seq_block), BF16),
                dma((n_cols + n_rows,)), dma((2,)), dma((2, 3)), dma((per, 3)), dma((3, per)), dma((per,)),
                dma((2, per, nz // 2)), dma((2, per, nz // 2)), dma((2, per, nz // 2)), dma((nz, per)),
            ],
            compiler_params=pltpu.CompilerParams(collective_id=2, has_side_effects=True, vmem_limit_bytes=60 * 2**20),
        )(y1, nall, gcols, grows, cos, sin)

    return jax.shard_map(shard_body, mesh=mesh, in_specs=(P("dp", None, None), P(None, None), P(None, None), P(None, None, "tp", None), P(None, "tp", None), P(None, None, "tp"), P(None, "tp", None)), out_specs=P("dp", None, None), check_vma=False)
```

```python
import functools
import math

import jax
import jax.numpy as jnp
from jax import lax
from jax.experimental import pallas as pl
from jax.experimental.pallas import tpu as pltpu
from jax.sharding import PartitionSpec as P

LN_EPS = 1e-5
ROPE_BASE = 10000.0
MESH = pl.DeviceIdType.MESH
BF16 = jnp.bfloat16
F32 = jnp.float32
LANES = 128
UP, Q, K, V, DOWN, OUT = range(6)


def norm_rows(hidden_f, gain, bias):
    row_mean = jnp.mean(hidden_f, axis=-1, keepdims=True)
    centered = hidden_f - row_mean
    row_var = jnp.mean(centered * centered, axis=-1, keepdims=True)
    return (centered * lax.rsqrt(row_var + LN_EPS) * gain + bias).astype(BF16)


def rope(heads, cos, sin):
    return (heads * cos + pltpu.roll(heads, heads.shape[-1] // 2, 1) * sin).astype(BF16)


def gelu(values):
    return (0.5 * values * (1.0 + lax.erf(values * math.sqrt(0.5)))).astype(BF16)


def attend(query, keys, values, seq_len):
    rows, head_dim = query.shape
    scores = lax.dot_general(query, keys, (((1,), (1,)), ((), ())), preferred_element_type=F32) * (head_dim ** -0.5)
    row = lax.broadcasted_iota(jnp.int32, (rows, rows), 0)
    col = lax.broadcasted_iota(jnp.int32, (rows, rows), 1)
    allowed = (row >= col) & (row // seq_len == col // seq_len)
    scores = jnp.where(allowed, scores, -1e30)
    weights = jnp.exp(scores - jnp.max(scores, axis=-1, keepdims=True))
    probs = (weights / jnp.sum(weights, axis=-1, keepdims=True)).astype(BF16)
    return jnp.dot(probs, values, preferred_element_type=F32).astype(BF16)


def context_of(proj, cos_ref, sin_ref, seq_len):
    head_dim = cos_ref.shape[1]
    query = rope(proj[:, :head_dim], cos_ref[...], sin_ref[...])
    keys = rope(proj[:, head_dim : 2 * head_dim], cos_ref[...], sin_ref[...])
    return attend(query, keys, proj[:, 2 * head_dim :].astype(BF16), seq_len)


def head_context(normed, qkv_w, cos_ref, sin_ref, seq_len):
    return context_of(jnp.dot(normed, qkv_w, preferred_element_type=F32), cos_ref, sin_ref, seq_len)


class Place:
    def __init__(self, n_dp, n_tp):
        side = math.isqrt(n_dp)
        assert side * side == n_dp and side % 2 == 0 and n_tp % 4 == 0
        self.n_tp, self.nz = n_tp, n_tp // 2
        self.dp, self.tp = lax.axis_index("dp"), lax.axis_index("tp")
        self.z, self.core = self.tp // 2, self.tp % 2
        x, y = self.dp // side, self.dp % side
        xf, yf = x + 1 - 2 * (x % 2), y + 1 - 2 * (y % 2)
        self.q = (x % 2) * 2 + y % 2
        self.peers = [{"dp": xf * side + y}, {"dp": x * side + yf}, {"dp": xf * side + yf}]
        self.peer_q = [(1 - x % 2) * 2 + y % 2, (x % 2) * 2 + 1 - y % 2, (1 - x % 2) * 2 + 1 - y % 2]
        self.sib = {"tp": 2 * self.z + 1 - self.core}
        self.right = {"tp": 2 * ((self.z + 1) % self.nz) + self.core}
        self.left = {"tp": 2 * ((self.z + self.nz - 1) % self.nz) + self.core}

    def others(self):
        return [self.sib, self.right, self.left, *self.peers]

    def greet(self):
        barrier = pltpu.get_barrier_semaphore()
        for other in self.others():
            pl.semaphore_signal(barrier, inc=1, device_id=other, device_id_type=MESH)

    def meet(self):
        pl.semaphore_wait(pltpu.get_barrier_semaphore(), len(self.others()))


def remote(src, dst, send_sem, recv_sem, device):
    return pltpu.make_async_remote_copy(src_ref=src, dst_ref=dst, send_sem=send_sem, recv_sem=recv_sem, device_id=device, device_id_type=MESH)


def piece(kind, source, n_tp, cols, rows):
    if kind == UP:
        return cols.at[source]
    if kind == DOWN:
        return rows.at[source]
    head = source // 8 * 2 + source % 2
    if kind == OUT:
        return rows.at[n_tp + head]
    return cols.at[n_tp + 3 * head + kind - Q]


def first_kernel(n_dp, n_tp, x, gains, biases, cos_ref, sin_ref, qkv, out_w, up, down,
                 y1, nout, accout, gcols, grows,
                 qkv_v, out_v, up_v, down_v, xbuf, normed, ctx, act, own, sib_out, sib_in, ring_r, ring_l, nall, acc, st_cols, st_rows,
                 w_sem, x_sem, sib_send, sib_recv, r_send, r_recv, l_send, l_recv,
                 st_sem, own_sem, loc_sem, wr_recv, wr_send, ws_send, ws_recv, n_send, n_recv, slab_sem, nout_sem, acc_sem):
    me = Place(n_dp, n_tp)
    me.greet()
    nz, core, z, q = me.nz, me.core, me.z, me.q
    n_seq, seq_len, d_model = x.shape
    head_dim, ff = out_w.shape[1], up.shape[2]
    per = n_seq // n_tp
    half = per // 2
    steps = nz * half
    tile = 4 * seq_len

    first_w = [pltpu.make_async_copy(src.at[0], dst, w_sem.at[i]) for i, (src, dst) in
               enumerate(((qkv, qkv_v.at[:, pl.ds(0, qkv.shape[2])]), (up, up_v), (out_w, out_v.at[pl.ds(0, head_dim)]), (down, down_v)))]

    def owner_seq(zo, co, j):
        return per * (2 * zo + co) + j

    def tile_seqs(i):
        s, j = i // half, i % half
        zr, zl = (z + 2 * nz - 1 - s) % nz, (z + 1 + s) % nz
        return [owner_seq(zr, core, j), owner_seq(zl, core, half + j), owner_seq(zr, 1 - core, j), owner_seq(zl, 1 - core, half + j)]

    def fetch(i):
        for place, seq in enumerate(tile_seqs(i)):
            pltpu.make_async_copy(x.at[seq], xbuf.at[i % 3, place], x_sem.at[i % 3]).start()

    fetch(0)
    for copy in first_w[:2]:
        copy.start()
    loads = {UP: (up.at[1, :, pl.ds(pl.multiple_of(q * LANES, LANES), LANES)], st_cols.at[UP]),
             DOWN: (down.at[1, pl.ds(pl.multiple_of(q * LANES, LANES), LANES), :], st_rows.at[0]),
             OUT: (out_w.at[1], st_rows.at[1])}
    for kind in (Q, K, V):
        loads[kind] = (qkv.at[1, :, pl.ds((kind - Q) * head_dim, head_dim)], st_cols.at[kind])
    kinds = (Q, K, V, OUT, UP, DOWN)
    loads = {kind: pltpu.make_async_copy(*loads[kind], st_sem.at[kind]) for kind in kinds}
    loads[UP].start()
    for copy in first_w[2:]:
        copy.start()
    for kind in kinds:
        if kind != UP:
            loads[kind].start()

    def has(kind, source):
        return source >= 0 if kind in (UP, DOWN) else (source // 2 + 2 * (source % 2)) % 4 == q

    def staged(kind):
        return st_rows.at[kind - DOWN] if kind >= DOWN else st_cols.at[kind]

    def first_hops(kind):
        src, dst = staged(kind), piece(kind, me.tp, n_tp, gcols, grows)
        return [remote(src, dst, own_sem.at[0, kind], wr_recv.at[0, 0, kind], me.right),
                remote(src, dst, own_sem.at[1, kind], wr_recv.at[1, 0, kind], me.left),
                remote(src, dst, own_sem.at[2, kind], ws_recv.at[z, kind], me.sib),
                pltpu.make_async_copy(src, dst, loc_sem.at[kind])]

    def send_first(kind):
        loads[kind].wait()

        @pl.when(has(kind, me.tp))
        def _():
            for copy in first_hops(kind):
                copy.start()

    for i in range(half):
        ring_r[i] = jnp.zeros(ring_r.shape[1:], BF16)
        ring_l[i] = jnp.zeros(ring_l.shape[1:], BF16)

    def send_sib(i):
        return remote(sib_out.at[i % 2], sib_in.at[i % 4], sib_send.at[i % 2], sib_recv.at[i % 4], me.sib)

    def send_r(i):
        return remote(ring_r.at[i], ring_r.at[i + half], r_send.at[i], r_recv.at[i + half], me.right)

    def send_l(i):
        return remote(ring_l.at[i], ring_l.at[i + half], l_send.at[i], l_recv.at[i + half], me.left)

    def rows_of(member):
        return pl.ds(pl.multiple_of(member * seq_len, seq_len), seq_len)

    def send_n(seq, peer):
        at = nall.at[seq, rows_of(q)]
        return remote(at, at, n_send.at[peer, seq], n_recv.at[peer, seq], me.peers[peer])

    def wait_n(seq, peer):
        at = nall.at[seq, rows_of(me.peer_q[peer])]
        return remote(at, at, n_send.at[peer, seq], n_recv.at[peer, seq], me.peers[peer])

    def compute(i, waits=()):
        slot = i % 3
        pltpu.make_async_copy(x.at[pl.ds(0, 4)], xbuf.at[slot], x_sem.at[slot]).wait()

        @pl.when(i + 1 < steps)
        def _():
            fetch(i + 1)

        @pl.when(i >= 2)
        def _():
            send_sib(i - 2).wait_send()

        for member in range(4):
            normed[pl.ds(member * seq_len, seq_len), :] = norm_rows(xbuf[slot, member].astype(F32), gains[pl.ds(0, 1), :], biases[pl.ds(0, 1), :])
        for copy in waits[:2]:
            copy.wait()
        ctx[...] = head_context(normed[...], qkv_v[:, : 3 * head_dim], cos_ref, sin_ref, seq_len)
        act[...] = gelu(jnp.dot(normed[...], up_v[...], preferred_element_type=F32))
        for copy in waits[2:]:
            copy.wait()
        step = 512
        for first in range(0, d_model, step):
            cols = pl.ds(first, step)
            part = jnp.dot(ctx[...], out_v[:head_dim, cols], preferred_element_type=F32) + jnp.dot(act[...], down_v[:, cols], preferred_element_type=F32)
            own[i % 2, :, cols] = part[: 2 * seq_len]
            sib_out[i % 2, :, cols] = part[2 * seq_len :].astype(BF16)

    def finish(i):
        send_sib(i).wait_recv()

        @pl.when(i >= half)
        def _():
            send_r(i - half).wait_recv()
            send_l(i - half).wait_recv()

        last = i >= steps - half

        @pl.when(jnp.logical_not(last))
        def _():
            for side, ring in enumerate((ring_r, ring_l)):
                at = pl.ds(side * seq_len, seq_len)
                ring[i] = (own[i % 2, at, :] + sib_in[i % 4, at, :].astype(F32) + ring[i].astype(F32)).astype(BF16)
            send_r(i).start()
            send_l(i).start()

        @pl.when(i == steps - half - 1)
        def _():
            for kind in kinds:
                if kind != UP:
                    send_first(kind)

        @pl.when(last)
        def _():
            rows = 16
            for side, ring in enumerate((ring_r, ring_l)):
                seq = side * half + i % half

                def close(k, carry):
                    at = pl.ds(pl.multiple_of(k * rows, rows), rows)
                    both = pl.ds(pl.multiple_of(side * seq_len + k * rows, rows), rows)
                    update = (own[i % 2, both, :] + sib_in[i % 4, both, :].astype(F32) + ring[i, at, :].astype(F32)).astype(BF16)
                    hidden = (xbuf[i % 3, side, at, :].astype(F32) + update.astype(F32)).astype(BF16)
                    y1[seq, at, :] = hidden
                    mine = pl.ds(pl.multiple_of(q * seq_len + k * rows, rows), rows)
                    nall[seq, mine, :] = norm_rows(hidden.astype(F32), gains[pl.ds(1, 1), :], biases[pl.ds(1, 1), :])
                    return carry

                lax.fori_loop(0, seq_len // rows, close, 0)
                for peer in range(3):
                    send_n(seq, peer).start()

    compute(0, first_w)
    me.meet()
    send_first(UP)
    send_sib(0).start()

    def turn(i, carry):
        @pl.when(i < steps)
        def _():
            compute(i)
            send_sib(i).start()

        finish(i - 1)
        return carry

    lax.fori_loop(1, steps + 1, turn, 0)

    to = (me.right, me.left)

    def hops(side, kind):
        longer = (core + kind) % 2
        return nz // 2 - longer if side == 0 else nz // 2 - 1 + longer

    def z_at(side, s):
        return (z + nz - s) % nz if side == 0 else (z + s) % nz

    def source_of(side, s):
        return 2 * z_at(side, s) + core

    def onward(side, s, kind):
        at = piece(kind, source_of(side, s), n_tp, gcols, grows)
        return remote(at, at, wr_send.at[side, s - 1, kind], wr_recv.at[side, s, kind], to[side])

    def arrival(side, s, kind):
        at = piece(kind, source_of(side, s), n_tp, gcols, grows)
        return remote(at, at, wr_send.at[side, s - 1, kind], wr_recv.at[side, s - 1, kind], to[side])

    def across(side, s, kind):
        source = source_of(side, s)
        at = piece(kind, source, n_tp, gcols, grows)
        return remote(at, at, ws_send.at[side, s - 1, kind], ws_recv.at[source // 2, kind], me.sib)

    def take(side, s, kind):
        @pl.when(has(kind, source_of(side, s)) & (s <= hops(side, kind)))
        def _():
            arrival(side, s, kind).wait_recv()

            @pl.when(s < hops(side, kind))
            def _():
                onward(side, s, kind).start()

            across(side, s, kind).start()

    def from_sib(zs, kind):
        source = 2 * zs + 1 - core

        @pl.when(has(kind, source))
        def _():
            at = piece(kind, source, n_tp, gcols, grows)
            remote(at, at, own_sem.at[2, kind], ws_recv.at[zs, kind], me.sib).wait_recv()

    width = 2 * LANES

    def slab_loads(number, zs):
        slot = number % 2
        copies = []
        for c in range(2):
            copies.append((gcols.at[2 * zs + c], up_v.at[:, pl.ds(slot * width + c * LANES, LANES)], slab_sem.at[slot, c]))
            copies.append((grows.at[2 * zs + c], down_v.at[pl.ds(slot * width + c * LANES, LANES), :], slab_sem.at[slot, 2 + c]))
        return [pltpu.make_async_copy(*copy) for copy in copies]

    def head_loads(first):
        copies = []
        for n in range(2):
            for i in range(3):
                copies.append((gcols.at[n_tp + 3 * (first + n) + i], qkv_v.at[:, pl.ds((3 * n + i) * head_dim, head_dim)], slab_sem.at[2, 4 * n + i]))
            copies.append((grows.at[n_tp + first + n], out_v.at[pl.ds(n * head_dim, head_dim)], slab_sem.at[2, 4 * n + 3]))
        return [pltpu.make_async_copy(*copy) for copy in copies]

    def pair(p):
        return p, half + p

    def slab_pair(number, p):
        mine = pl.ds(number % 2 * width, width)
        hidden = [gelu(jnp.dot(nall[i], up_v[:, mine], preferred_element_type=F32)) for i in pair(p)]
        step = 512
        for first in range(0, d_model, step):
            cols = pl.ds(first, step)
            for i, rows in zip(pair(p), hidden):
                part = jnp.dot(rows, down_v[mine, cols], preferred_element_type=F32)
                acc[i, :, cols] = part if number == 0 else acc[i, :, cols] + part

    def head_pair(p):
        contexts = []
        for i in pair(p):
            proj = jnp.dot(nall[i], qkv_v[...], preferred_element_type=F32)
            contexts.append(jnp.concatenate([context_of(proj[:, 3 * head_dim * n : 3 * head_dim * (n + 1)], cos_ref, sin_ref, seq_len) for n in range(2)], axis=1))
        step = 512
        for first in range(0, d_model, step):
            cols = pl.ds(first, step)
            for i, rows in zip(pair(p), contexts):
                acc[i, :, cols] += jnp.dot(rows, out_v[:, cols], preferred_element_type=F32)

    def pairs(body):
        def one(p, carry):
            body(p)
            return carry

        lax.fori_loop(0, half, one, 0)

    order = [(0, 0), (0, 1), (1, 1)]

    def start_slab(number):
        zs = z_at(*order[number])
        for kind in (UP, DOWN):
            from_sib(zs, kind)
            if number == 0:
                first_hops(kind)[3].wait()
        for copy in slab_loads(number, zs):
            copy.start()

    def wait_slab(number):
        for copy in slab_loads(number, z_at(*order[number])):
            copy.wait()

    def take_all(stages, kinds):
        for s in stages:
            for kind in kinds:
                for side in range(2):
                    take(side, s, kind)

    def await_pair(p):
        for i in pair(p):
            for peer in range(3):
                wait_n(i, peer).wait_recv()
            pltpu.make_async_copy(nall.at[i], nout.at[i], nout_sem.at[i]).start()

    def slab(number):
        wait_slab(number)
        pairs(functools.partial(slab_pair, number))

    attn = (Q, K, V, OUT)
    take_all([1, 2], attn)
    start_slab(0)
    take_all([1], [UP, DOWN])
    wait_slab(0)
    await_pair(0)
    slab_pair(0, 0)
    take_all([3], attn)
    await_pair(1)
    slab_pair(0, 1)
    take_all([2], [UP])
    await_pair(2)
    slab_pair(0, 2)
    start_slab(1)
    take_all([2], [DOWN])
    take_all([4], attn)
    for kind in attn:
        @pl.when(has(kind, me.tp))
        def _():
            first_hops(kind)[3].wait()

        for zs in range(nz):
            from_sib(zs, kind)
    for copy in head_loads(0):
        copy.start()
    start_slab(2)
    for copy in head_loads(0):
        copy.wait()
    head_pair(0)
    take_all([3], [UP])
    head_pair(1)
    take_all([3], [DOWN])
    head_pair(2)
    slab(1)
    wait_slab(2)

    def last_part(p):
        slab_pair(2, p)
        for i in pair(p):
            pltpu.make_async_copy(acc.at[i], accout.at[i], acc_sem.at[i]).start()

    pairs(last_part)
    take_all([4], [UP, DOWN])

    def drain(i, carry):
        send_r(i).wait_send()
        send_l(i).wait_send()
        return carry

    lax.fori_loop(0, steps - half, drain, 0)
    send_sib(steps - 2).wait_send()
    send_sib(steps - 1).wait_send()
    for seq in range(per):
        for peer in range(3):
            send_n(seq, peer).wait_send()
        pltpu.make_async_copy(nall.at[seq], nout.at[seq], nout_sem.at[seq]).wait()
        pltpu.make_async_copy(acc.at[seq], accout.at[seq], acc_sem.at[seq]).wait()
    for kind in kinds:
        @pl.when(has(kind, me.tp))
        def _():
            for copy in first_hops(kind)[:3]:
                copy.wait_send()

        for s in range(1, nz // 2 + 1):
            for side in range(2):
                @pl.when(has(kind, source_of(side, s)) & (s <= hops(side, kind)))
                def _():
                    @pl.when(s < hops(side, kind))
                    def _():
                        onward(side, s, kind).wait_send()

                    across(side, s, kind).wait_send()
    for side, s in late_slabs(nz):
        for kind in (UP, DOWN):
            from_sib(z_at(side, s), kind)


def late_slabs(nz):
    return [(side, s) for s in range(2, nz // 2) for side in range(2)] + [(0, nz // 2)]


def second_kernel(n_dp, n_tp, y1, cos_ref, sin_ref, nout, accout, gcols, grows, out,
                  qkv_v, out_v, up_v, down_v, nbuf, ctx, act, accbuf, own, part_out, part_in,
                  w_sem, n_sem, a_sem, p_send, p_recv, own_send, r_recv, f_send, s_send, s_recv):
    me = Place(n_dp, n_tp)
    me.greet()
    nz, core, z, q = me.nz, me.core, me.z, me.q
    per, tile, d_model = nout.shape
    members = 4
    seq_len = tile // members

    def z_of(side, s):
        return (z + nz - s) % nz if side == 0 else (z + s) % nz

    def fetch(i):
        return [pltpu.make_async_copy(nout.at[i], nbuf.at[i % 2], n_sem.at[i % 2]),
                pltpu.make_async_copy(accout.at[i], accbuf.at[i % 2], a_sem.at[i % 2])]

    for copy in fetch(0):
        copy.start()
    head_dim = cos_ref.shape[1]
    firsts, seconds = [], []
    for n in range(2):
        head = grows.shape[0] - n_tp - 2 + n
        for i in range(3):
            firsts.append((gcols.at[n_tp + 3 * head + i], qkv_v.at[:, pl.ds((3 * n + i) * head_dim, head_dim)]))
        seconds.append((grows.at[n_tp + head], out_v.at[pl.ds(n * head_dim, head_dim)]))
    for n, (side, s) in enumerate(late_slabs(nz)):
        for c in range(2):
            source, at = 2 * z_of(side, s) + c, pl.ds((2 * n + c) * LANES, LANES)
            firsts.append((gcols.at[source], up_v.at[:, at]))
            seconds.append((grows.at[source], down_v.at[at, :]))
    loads = [pltpu.make_async_copy(src, dst, w_sem.at[i]) for i, (src, dst) in enumerate(firsts + seconds)]
    firsts, seconds = loads[: len(firsts)], loads[len(firsts) :]
    for copy in loads:
        copy.start()

    def send_part(i, peer):
        at = pl.ds(pl.multiple_of(me.peer_q[peer] * seq_len, seq_len), seq_len)
        return remote(part_out.at[i % 4, at], part_in.at[i, peer], p_send.at[i % 4, peer], p_recv.at[i, peer], me.peers[peer])

    def seq_of(zs, co, i):
        return per * (2 * zs + co) + i

    def first_hops(i):
        at = out.at[seq_of(z, core, i)]
        return [remote(at, at, own_send.at[0, i], r_recv.at[0, i, 0], me.right),
                remote(at, at, own_send.at[1, i], r_recv.at[1, i, 0], me.left),
                remote(at, at, own_send.at[2, i], s_recv.at[z, i], me.sib)]

    to = (me.right, me.left)

    def hops(side, i):
        longer = (i + core) % 2
        return nz // 2 - longer if side == 0 else nz // 2 - 1 + longer

    def arrival(side, i, s):
        at = out.at[seq_of(z_of(side, s), core, i)]
        return remote(at, at, f_send.at[side, i, s - 1], r_recv.at[side, i, s - 1], to[side])

    def onward(side, i, s):
        at = out.at[seq_of(z_of(side, s), core, i)]
        return remote(at, at, f_send.at[side, i, s - 1], r_recv.at[side, i, s], to[side])

    def across(side, i, s):
        at = out.at[seq_of(z_of(side, s), core, i)]
        return remote(at, at, s_send.at[side, i, s - 1], s_recv.at[z_of(side, s), i], me.sib)

    def when_first(i, copies):
        @pl.when(i == 0)
        def _():
            for copy in copies:
                copy.wait()

    def compute(i):
        for copy in fetch(i):
            copy.wait()

        @pl.when(i + 1 < per)
        def _():
            for copy in fetch(i + 1):
                copy.start()

        @pl.when(i >= 4)
        def _():
            for peer in range(3):
                send_part(i - 4, peer).wait_send()

        when_first(i, firsts)
        proj = jnp.dot(nbuf[i % 2], qkv_v[...], preferred_element_type=F32)
        ctx[...] = jnp.concatenate([context_of(proj[:, 3 * head_dim * n : 3 * head_dim * (n + 1)], cos_ref, sin_ref, seq_len) for n in range(2)], axis=1)
        act[...] = gelu(jnp.dot(nbuf[i % 2], up_v[...], preferred_element_type=F32))
        when_first(i, seconds)
        step = 512
        for first in range(0, d_model, step):
            cols = pl.ds(first, step)
            part = accbuf[i % 2, :, cols] + jnp.dot(act[...], down_v[:, cols], preferred_element_type=F32)
            part += jnp.dot(ctx[...], out_v[:, cols], preferred_element_type=F32)
            accbuf[i % 2, :, cols] = part
            part_out[i % 4, :, cols] = part.astype(BF16)

        @pl.when(i == 0)
        def _():
            me.meet()

        for peer in range(3):
            send_part(i, peer).start()
        own[i % 4] = accbuf[i % 2, pl.ds(pl.multiple_of(q * seq_len, seq_len), seq_len), :]

    def finish(i):
        for peer in range(3):
            send_part(i, peer).wait_recv()
        total = own[i % 4]
        for peer in range(3):
            total = total + part_in[i, peer].astype(F32)
        out[seq_of(z, core, i)] = (y1[i].astype(F32) + total.astype(BF16).astype(F32)).astype(BF16)
        for copy in first_hops(i):
            copy.start()

    def pass_on(i, s):
        for side in range(2):
            @pl.when(s <= hops(side, i))
            def _():
                arrival(side, i, s).wait_recv()

                @pl.when(s < hops(side, i))
                def _():
                    onward(side, i, s).start()

                across(side, i, s).start()

    def stage(name):
        i, s = int(name[0]), int(name[1])
        if s == 0:
            finish(i)
        else:
            pass_on(i, s)

    assert (per, nz) == (6, 8)
    beside = {2: "00", 3: "01", 4: "10 02", 5: "11 20"}

    def turn(i, carry):
        compute(i)
        for at, names in beside.items():
            @pl.when(i == at)
            def _():
                for name in names.split():
                    stage(name)

        return carry

    lax.fori_loop(0, per, turn, 0)
    for name in "03 12 30 21 04 13 40 31 22 50 14 41 32 23 51 42 33 52 24 43 34 53 44 54".split():
        stage(name)

    for i in range(per - 4, per):
        for peer in range(3):
            send_part(i, peer).wait_send()

    def drain(i, carry):
        for copy in first_hops(i):
            copy.wait_send()
        for s in range(1, nz // 2 + 1):
            for side in range(2):
                @pl.when(s <= hops(side, i))
                def _():
                    @pl.when(s < hops(side, i))
                    def _():
                        onward(side, i, s).wait_send()

                    across(side, i, s).wait_send()
        for zs in range(nz):
            at = out.at[seq_of(zs, 1 - core, i)]
            remote(at, at, own_send.at[2, i], s_recv.at[zs, i], me.sib).wait_recv()
        return carry

    lax.fori_loop(0, per, drain, 0)


def rope_rows(seq_len, head_dim, copies):
    half_dim = head_dim // 2
    inv_freq = ROPE_BASE ** (-2.0 * jnp.arange(half_dim, dtype=F32) / head_dim)
    angles = jnp.arange(seq_len, dtype=F32)[:, None] * inv_freq[None, :]
    cos, sin = jnp.cos(angles), jnp.sin(angles)
    return jnp.tile(jnp.concatenate([cos, cos], 1), (copies, 1)), jnp.tile(jnp.concatenate([-sin, sin], 1), (copies, 1))


def solution(mesh):
    n_dp, n_tp = mesh.shape["dp"], mesh.shape["tp"]
    nz = n_tp // 2
    any_spec = pl.BlockSpec(memory_space=pl.ANY)
    vmem_spec = pl.BlockSpec(memory_space=pltpu.VMEM)
    dma = pltpu.SemaphoreType.DMA

    def shard_body(act_in, ln_gain, ln_bias, w_qkv, w_out, w_up, w_down):
        n_seq, seq_len, d_model = act_in.shape
        layers, _, _, qkv_cols = w_qkv.shape
        head_dim, ff = w_out.shape[1], w_up.shape[2]
        per = n_seq // n_tp
        half = per // 2
        heads = n_tp // 4
        tile = 4 * seq_len
        w_qkv = w_qkv.reshape(layers, d_model, qkv_cols)
        cos, sin = rope_rows(seq_len, head_dim, 4)
        seq_block = (seq_len, d_model)
        n_cols, n_rows = n_tp + 3 * heads, n_tp + heads
        steps = nz * half
        n_late = 2 * len(late_slabs(nz)) * LANES
        y1, nout, accout, gcols, grows = pl.pallas_call(
            functools.partial(first_kernel, n_dp, n_tp),
            name="layer_one",
            out_shape=(jax.ShapeDtypeStruct((per, *seq_block), BF16), jax.ShapeDtypeStruct((per, tile, d_model), BF16), jax.ShapeDtypeStruct((per, tile, d_model), F32),
                       jax.ShapeDtypeStruct((n_cols, d_model, LANES), BF16), jax.ShapeDtypeStruct((n_rows, LANES, d_model), BF16)),
            in_specs=[any_spec] + [vmem_spec] * 4 + [any_spec] * 4,
            out_specs=(vmem_spec, any_spec, any_spec, any_spec, any_spec),
            scratch_shapes=[
                pltpu.VMEM((d_model, 2 * qkv_cols), BF16), pltpu.VMEM((2 * head_dim, d_model), BF16), pltpu.VMEM((d_model, ff), BF16), pltpu.VMEM((ff, d_model), BF16),
                pltpu.VMEM((3, 4, *seq_block), BF16), pltpu.VMEM((tile, d_model), BF16), pltpu.VMEM((tile, head_dim), BF16), pltpu.VMEM((tile, ff), BF16),
                pltpu.VMEM((2, 2 * seq_len, d_model), F32), pltpu.VMEM((2, 2 * seq_len, d_model), BF16), pltpu.VMEM((4, 2 * seq_len, d_model), BF16),
                pltpu.VMEM((steps, *seq_block), BF16), pltpu.VMEM((steps, *seq_block), BF16), pltpu.VMEM((per, tile, d_model), BF16), pltpu.VMEM((per, tile, d_model), F32),
                pltpu.VMEM((4, d_model, LANES), BF16), pltpu.VMEM((2, LANES, d_model), BF16),
                dma((4,)), dma((3,)), dma((2,)), dma((4,)), dma((steps,)), dma((steps,)), dma((steps,)), dma((steps,)),
                dma((6,)), dma((3, 6)), dma((6,)), dma((2, nz // 2, 6)), dma((2, nz // 2, 6)), dma((2, nz // 2, 6)), dma((nz, 6)),
                dma((3, per)), dma((3, per)), dma((3, 8)), dma((per,)), dma((per,)),
            ],
            compiler_params=pltpu.CompilerParams(collective_id=1, has_side_effects=True, vmem_limit_bytes=63 * 2**20),
        )(act_in, ln_gain, ln_bias, cos, sin, w_qkv, w_out, w_up, w_down)
        return pl.pallas_call(
            functools.partial(second_kernel, n_dp, n_tp),
            name="layer_two",
            out_shape=pltpu.VMEM(act_in.shape, BF16),
            in_specs=[vmem_spec] * 3 + [any_spec] * 4,
            out_specs=vmem_spec,
            scratch_shapes=[
                pltpu.VMEM((d_model, 2 * qkv_cols), BF16), pltpu.VMEM((2 * head_dim, d_model), BF16), pltpu.VMEM((d_model, n_late), BF16), pltpu.VMEM((n_late, d_model), BF16),
                pltpu.VMEM((2, tile, d_model), BF16), pltpu.VMEM((tile, 2 * head_dim), BF16), pltpu.VMEM((tile, n_late), BF16), pltpu.VMEM((2, tile, d_model), F32), pltpu.VMEM((4, *seq_block), F32),
                pltpu.VMEM((4, tile, d_model), BF16), pltpu.VMEM((per, 3, *seq_block), BF16),
                dma((2 * n_late // LANES + 8,)), dma((2,)), dma((2,)), dma((4, 3)), dma((per, 3)), dma((3, per)),
                dma((2, per, nz // 2)), dma((2, per, nz // 2)), dma((2, per, nz // 2)), dma((nz, per)),
            ],
            compiler_params=pltpu.CompilerParams(collective_id=2, has_side_effects=True, vmem_limit_bytes=38 * 2**20),
        )(y1, cos, sin, nout, accout, gcols, grows)

    return jax.shard_map(shard_body, mesh=mesh, in_specs=(P("dp", None, None), P(None, None), P(None, None), P(None, None, "tp", None), P(None, "tp", None), P(None, None, "tp"), P(None, "tp", None)), out_specs=P("dp", None, None), check_vma=False)
```

```python
import functools
import math

import jax
import jax.numpy as jnp
import numpy as np
from jax import lax
from jax.experimental import pallas as pl
from jax.experimental.pallas import tpu as pltpu
from jax.sharding import PartitionSpec as P

LN_EPS = 1e-5
ROPE_BASE = 10000.0
MESH = pl.DeviceIdType.MESH
BF16 = jnp.bfloat16
F32 = jnp.float32
LANES = 128
UP, Q, K, V, DOWN, OUT = range(6)


def norm_rows(hidden_f, gain, bias):
    row_mean = jnp.mean(hidden_f, axis=-1, keepdims=True)
    centered = hidden_f - row_mean
    row_var = jnp.mean(centered * centered, axis=-1, keepdims=True)
    return (centered * lax.rsqrt(row_var + LN_EPS) * gain + bias).astype(BF16)


def rope(heads, cos, sin):
    return (heads * cos + pltpu.roll(heads, heads.shape[-1] // 2, 1) * sin).astype(BF16)


def gelu(values):
    return (0.5 * values * (1.0 + lax.erf(values * math.sqrt(0.5)))).astype(BF16)


def attend(query, keys, values, seq_len):
    rows, head_dim = query.shape
    block = 2 * seq_len
    row = lax.broadcasted_iota(jnp.int32, (block, block), 0)
    col = lax.broadcasted_iota(jnp.int32, (block, block), 1)
    allowed = (row >= col) & (row // seq_len == col // seq_len)
    contexts = []
    for first in range(0, rows, block):
        at = slice(first, first + block)
        scores = lax.dot_general(query[at], keys[at], (((1,), (1,)), ((), ())), preferred_element_type=F32) * (head_dim ** -0.5)
        scores = jnp.where(allowed, scores, -1e30)
        weights = jnp.exp(scores - jnp.max(scores, axis=-1, keepdims=True))
        probs = (weights / jnp.sum(weights, axis=-1, keepdims=True)).astype(BF16)
        contexts.append(jnp.dot(probs, values[at], preferred_element_type=F32).astype(BF16))
    return jnp.concatenate(contexts, axis=0)


def context_of(proj, cos_ref, sin_ref, seq_len):
    head_dim = cos_ref.shape[1]
    query = rope(proj[:, :head_dim], cos_ref[...], sin_ref[...])
    keys = rope(proj[:, head_dim : 2 * head_dim], cos_ref[...], sin_ref[...])
    return attend(query, keys, proj[:, 2 * head_dim :].astype(BF16), seq_len)


def head_context(normed, qkv_w, cos_ref, sin_ref, seq_len):
    return context_of(jnp.dot(normed, qkv_w, preferred_element_type=F32), cos_ref, sin_ref, seq_len)


class Place:
    def __init__(self, n_dp, n_tp):
        side = math.isqrt(n_dp)
        assert side * side == n_dp and side % 2 == 0 and n_tp % 4 == 0
        self.n_tp, self.nz = n_tp, n_tp // 2
        self.dp, self.tp = lax.axis_index("dp"), lax.axis_index("tp")
        self.z, self.core = self.tp // 2, self.tp % 2
        x, y = self.dp // side, self.dp % side
        xf, yf = x + 1 - 2 * (x % 2), y + 1 - 2 * (y % 2)
        self.q = (x % 2) * 2 + y % 2
        self.peers = [{"dp": xf * side + y}, {"dp": x * side + yf}, {"dp": xf * side + yf}]
        self.peer_q = [(1 - x % 2) * 2 + y % 2, (x % 2) * 2 + 1 - y % 2, (1 - x % 2) * 2 + 1 - y % 2]
        self.sib = {"tp": 2 * self.z + 1 - self.core}
        self.right = {"tp": 2 * ((self.z + 1) % self.nz) + self.core}
        self.left = {"tp": 2 * ((self.z + self.nz - 1) % self.nz) + self.core}

    def z_at(self, side, s):
        return (self.z + self.nz - s) % self.nz if side == 0 else (self.z + s) % self.nz

    def others(self):
        return [self.sib, self.right, self.left, *self.peers]

    def greet(self):
        barrier = pltpu.get_barrier_semaphore()
        for other in self.others():
            pl.semaphore_signal(barrier, inc=1, device_id=other, device_id_type=MESH)

    def meet(self):
        pl.semaphore_wait(pltpu.get_barrier_semaphore(), len(self.others()))


def remote(src, dst, send_sem, recv_sem, device):
    return pltpu.make_async_remote_copy(src_ref=src, dst_ref=dst, send_sem=send_sem, recv_sem=recv_sem, device_id=device, device_id_type=MESH)


def piece(kind, source, n_tp, cols, rows):
    if kind == UP:
        return cols.at[source]
    if kind == DOWN:
        return rows.at[source]
    head = source // 8 * 2 + source % 2
    if kind == OUT:
        return rows.at[n_tp + head]
    return cols.at[n_tp + 3 * head + kind - Q]


class SecondLayer:
    def __init__(self, place, nall, acc, qkv_v, out_v, up_v, down_v, gcols, grows, cos_ref, sin_ref, sem):
        self.place, self.nall, self.acc, self.sem = place, nall, acc, sem
        self.qkv_v, self.out_v, self.up_v, self.down_v = qkv_v, out_v, up_v, down_v
        self.gcols, self.grows, self.cos_ref, self.sin_ref = gcols, grows, cos_ref, sin_ref
        self.seq_len = nall.shape[1] // 4
        far = place.nz // 2
        self.order = [(0, 0)] + [(side, s) for s in range(1, far) for side in range(2)] + [(0, far)]

    def slab_loads(self, number):
        slot, zs = number % 2, self.place.z_at(*self.order[number])
        copies = []
        for c in range(2):
            at = pl.ds(c * LANES, LANES)
            copies.append((self.gcols.at[2 * zs + c], self.up_v.at[slot, :, at], self.sem.at[slot, 0]))
            copies.append((self.grows.at[2 * zs + c], self.down_v.at[slot, at, :], self.sem.at[slot, 1]))
        return [pltpu.make_async_copy(*copy) for copy in copies]

    def head_loads(self, first):
        n_tp, head_dim = self.place.n_tp, self.cos_ref.shape[1]
        copies = []
        for n in range(2):
            for i in range(3):
                at = pl.ds((3 * n + i) * head_dim, head_dim)
                copies.append((self.gcols.at[n_tp + 3 * (first + n) + i], self.qkv_v.at[:, at], self.sem.at[2, 0]))
            copies.append((self.grows.at[n_tp + first + n], self.out_v.at[pl.ds(n * head_dim, head_dim)], self.sem.at[2, 1]))
        return [pltpu.make_async_copy(*copy) for copy in copies]

    def wait_slab(self, number):
        slot = number % 2
        settle(self.up_v.at[slot], self.sem.at[slot, 0])
        settle(self.down_v.at[slot], self.sem.at[slot, 1])

    def wait_heads(self):
        settle(self.qkv_v, self.sem.at[2, 0])
        settle(self.out_v, self.sem.at[2, 1])

    def clear(self):
        for i in range(self.acc.shape[0]):
            self.acc[i] = jnp.zeros(self.acc.shape[1:], F32)

    def slab(self, slot, p):
        nall, acc = self.nall, self.acc
        pair = (2 * p, 2 * p + 1)
        hidden = [gelu(jnp.dot(nall[i], self.up_v[slot], preferred_element_type=F32)) for i in pair]
        step = 512
        for first in range(0, acc.shape[2], step):
            cols = pl.ds(first, step)
            for i, rows in zip(pair, hidden):
                acc[i, :, cols] += jnp.dot(rows, self.down_v[slot, :, cols], preferred_element_type=F32)

    def heads(self, i):
        nall, acc, head_dim = self.nall, self.acc, self.cos_ref.shape[1]
        proj = jnp.dot(nall[i], self.qkv_v[...], preferred_element_type=F32)
        both = [context_of(proj[:, 3 * head_dim * n : 3 * head_dim * (n + 1)], self.cos_ref, self.sin_ref, self.seq_len) for n in range(2)]
        context = jnp.concatenate(both, axis=1)
        step = 512
        for first in range(0, acc.shape[2], step):
            cols = pl.ds(first, step)
            acc[i, :, cols] += jnp.dot(context, self.out_v[:, cols], preferred_element_type=F32)

    def round_off(self, i):
        self.nall[i] = self.acc[i].astype(BF16)

    def run(self, plan, late_step=None):
        def pick(values, default):
            def at(u):
                found = jnp.int32(default)
                for k, value in enumerate(values):
                    if value is not None:
                        found = jnp.where(u == k, value, found)
                return found
            return at

        late = pick([entry[1] for entry in plan], -1)
        slot = pick([entry[2][0] % 2 if len(entry[2]) == 2 else None for entry in plan], -1)
        pair = pick([entry[2][1] if len(entry[2]) == 2 else None for entry in plan], 0)
        tile = pick([entry[2][0] if len(entry[2]) == 1 else None for entry in plan], -1)

        def turn(u, carry):
            for k, entry in enumerate(plan):
                if entry[0]:
                    @pl.when(u == k)
                    def _():
                        for event in entry[0]:
                            event()

            if late_step:
                @pl.when(late(u) >= 0)
                def _():
                    late_step(late(u))

            @pl.when(slot(u) >= 0)
            def _():
                self.slab(slot(u), pair(u))

            @pl.when(tile(u) >= 0)
            def _():
                self.heads(tile(u))

            return carry

        lax.fori_loop(0, len(plan), turn, 0)


def settle(ref, sem):
    pltpu.make_async_copy(ref, ref, sem).wait()


def call(function, *args):
    return lambda: function(*args)


def start(copies):
    for copy in copies:
        copy.start()


def wait(copies):
    for copy in copies:
        copy.wait()


def first_kernel(n_dp, n_tp, x, gains_h, biases_h, cos_h, sin_h, qkv, out_w, up, down,
                 done_h, nown_h, pout, pown, gcols, grows,
                 gains, biases, cos_ref, sin_ref, done, nown, qkv_v, out_v, up_v, down_v, xbuf, normed, ctx, act, own, sib_out, sib_in, ring_r, ring_l, loc, nall, acc, part_in, st_cols, st_rows,
                 w_sem, x_sem, sib_send, sib_recv, r_send, r_recv, e_send, e_recv,
                 st_sem, loc_sem, w_send, wr_recv, ws_recv, n_send, n_recv, slab_sem, p_send, p_recv, o_sem, small_sem, done_sem):
    me = Place(n_dp, n_tp)
    me.greet()
    nz, core, z, q = me.nz, me.core, me.z, me.q
    n_seq, seq_len, d_model = x.shape
    head_dim, ff = out_w.shape[1], up.shape[2]
    per = n_seq // n_tp
    half = per // 2
    steps = nz * half

    wide = ff // 2
    first_w = [pltpu.make_async_copy(src, dst, w_sem.at[i]) for i, (src, dst) in
               enumerate(((qkv.at[0], qkv_v.at[:, pl.ds(0, qkv.shape[2])]), (up.at[0, :, pl.ds(0, wide)], up_v.at[0]), (up.at[0, :, pl.ds(wide, wide)], up_v.at[1]),
                         (out_w.at[0], out_v.at[pl.ds(0, head_dim)]), (down.at[0, pl.ds(0, wide)], down_v.at[0]), (down.at[0, pl.ds(wide, wide)], down_v.at[1])))]

    def owner_seq(zo, co, j):
        return per * (2 * zo + co) + j

    def tile_seqs(i):
        s, j = i // half, i % half
        zr, zl = (z + 2 * nz - 1 - s) % nz, (z + 1 + s) % nz
        return [owner_seq(zr, core, j), owner_seq(zl, core, half + j), owner_seq(zr, 1 - core, j), owner_seq(zl, 1 - core, half + j)]

    def fetch(i):
        for place, seq in enumerate(tile_seqs(i)):
            pltpu.make_async_copy(x.at[seq], xbuf.at[i % 3, place], x_sem.at[i % 3]).start()

    small = [pltpu.make_async_copy(src, dst, small_sem.at[i]) for i, (src, dst) in enumerate(((gains_h, gains), (biases_h, biases), (cos_h, cos_ref), (sin_h, sin_ref)))]
    fetch(0)
    start(small)
    start(first_w[:3])
    loads = {UP: (up.at[1, :, pl.ds(pl.multiple_of(q * LANES, LANES), LANES)], st_cols.at[UP]),
             DOWN: (down.at[1, pl.ds(pl.multiple_of(q * LANES, LANES), LANES), :], st_rows.at[0]),
             OUT: (out_w.at[1], st_rows.at[1])}
    for kind in (Q, K, V):
        loads[kind] = (qkv.at[1, :, pl.ds((kind - Q) * head_dim, head_dim)], st_cols.at[kind])
    kinds = (Q, K, V, OUT, UP, DOWN)
    loads = {kind: pltpu.make_async_copy(*loads[kind], st_sem.at[kind]) for kind in kinds}

    def start_rest():
        wait(small)
        start(first_w[3:])
        start([loads[UP], *(loads[kind] for kind in kinds if kind != UP)])

    def has(kind, source):
        return source >= 0 if kind in (UP, DOWN) else (source // 2 + 2 * (source % 2)) % 4 == q

    def staged(kind):
        return st_rows.at[kind - DOWN] if kind >= DOWN else st_cols.at[kind]

    def first_hops(kind):
        src, dst = staged(kind), piece(kind, me.tp, n_tp, gcols, grows)
        return [remote(src, dst, w_send.at[kind], wr_recv.at[0, 0, kind], me.right),
                remote(src, dst, w_send.at[kind], wr_recv.at[1, 0, kind], me.left),
                remote(src, dst, w_send.at[kind], sib_sem(z, kind), me.sib),
                pltpu.make_async_copy(src, dst, loc_sem.at[kind])]

    def sib_sem(zs, kind):
        return ws_recv.at[zs] if kind in (UP, DOWN) else ws_recv.at[nz]

    def send_first(kind):
        loads[kind].wait()

        @pl.when(has(kind, me.tp))
        def _():
            start(first_hops(kind))

    rings = (ring_r, ring_l)
    for i in range(half):
        for ring in rings:
            ring[i] = jnp.zeros(ring.shape[1:], BF16)

    def send_sib(i):
        return remote(sib_out.at[i % 2], sib_in.at[i % 4], sib_send.at[i % 2], sib_recv.at[i % 4], me.sib)

    def early(i):
        return i // half * (half - 1) + i % half

    def send_r(i):
        return remote(ring_r.at[i], ring_r.at[i + half], r_send.at[0], r_recv.at[0, early(i)], me.right)

    def send_l(i):
        return remote(ring_l.at[i], ring_l.at[i + half], r_send.at[1], r_recv.at[1, early(i)], me.left)

    def rows_of(member):
        return pl.ds(pl.multiple_of(member * seq_len, seq_len), seq_len)

    def send_n(tile, peer):
        at = nall.at[tile, rows_of(q)]
        return remote(at, at, n_send.at[tile], n_recv.at[tile // 2], me.peers[peer])

    def compute(i, waits=(), then=None):
        slot = i % 3
        pltpu.make_async_copy(x.at[pl.ds(0, 4)], xbuf.at[slot], x_sem.at[slot]).wait()
        if then:
            then()

        @pl.when(i + 1 < steps)
        def _():
            fetch(i + 1)

        @pl.when(i >= 2)
        def _():
            send_sib(i - 2).wait_send()

        for member in range(4):
            normed[pl.ds(member * seq_len, seq_len), :] = norm_rows(xbuf[slot, member].astype(F32), gains[pl.ds(0, 1), :], biases[pl.ds(0, 1), :])
        wait(waits[:3])
        ctx[...] = head_context(normed[...], qkv_v[:, : 3 * head_dim], cos_ref, sin_ref, seq_len)
        for n in range(2):
            act[:, n * wide : (n + 1) * wide] = gelu(jnp.dot(normed[...], up_v[n], preferred_element_type=F32))
        wait(waits[3:])
        step = 512
        for first in range(0, d_model, step):
            cols = pl.ds(first, step)
            part = jnp.dot(ctx[...], out_v[:head_dim, cols], preferred_element_type=F32)
            for n in range(2):
                part += jnp.dot(act[:, n * wide : (n + 1) * wide], down_v[n, :, cols], preferred_element_type=F32)
            own[i % 2, :, cols] = part[: 2 * seq_len]
            sib_out[i % 2, :, cols] = part[2 * seq_len :].astype(BF16)

    def finish(i):
        send_sib(i).wait_recv()
        late = i % half == half - 1
        last = i >= steps - half

        @pl.when(late)
        def _():
            for side in range(2):
                at = pl.ds(side * seq_len, seq_len)
                loc[side, i // half] = (own[i % 2, at, :] + sib_in[i % 4, at, :].astype(F32)).astype(BF16)

        @pl.when((i >= half) & jnp.logical_not(late))
        def _():
            send_r(i - half).wait_recv()
            send_l(i - half).wait_recv()

        @pl.when(jnp.logical_not(last | late))
        def _():
            for side, ring in enumerate(rings):
                at = pl.ds(side * seq_len, seq_len)
                ring[i] = (own[i % 2, at, :] + sib_in[i % 4, at, :].astype(F32) + ring[i].astype(F32)).astype(BF16)
            send_r(i).start()
            send_l(i).start()

        @pl.when(i == steps - half - 2)
        def _():
            for kind in kinds:
                if kind != UP:
                    send_first(kind)

        @pl.when(last & jnp.logical_not(late))
        def _():
            rows = seq_len // 2
            for side, ring in enumerate(rings):
                tile = 2 * (i % half) + side
                for first in range(0, seq_len, rows):
                    at, both = pl.ds(first, rows), pl.ds(side * seq_len + first, rows)
                    update = (own[i % 2, both, :] + sib_in[i % 4, both, :].astype(F32) + ring[i, at, :].astype(F32)).astype(BF16)
                    close(side, tile, at, i % 3, update, nall.at[tile, pl.ds(pl.multiple_of(q * seq_len + first, rows), rows)])
                for peer in range(3):
                    send_n(tile, peer).start()

    def close(side, tile, at, slot, update, normed_at):
        hidden = (xbuf[slot, side, at, :].astype(F32) + update.astype(F32)).astype(BF16)
        done[tile, at, :] = hidden
        normed_at[...] = norm_rows(hidden.astype(F32), gains[pl.ds(1, 1), :], biases[pl.ds(1, 1), :])

    compute(0, first_w, start_rest)
    me.meet()
    send_first(UP)
    send_sib(0).start()

    def turn(i, carry):
        @pl.when(i < steps)
        def _():
            compute(i)
            send_sib(i).start()

        finish(i - 1)
        return carry

    lax.fori_loop(1, steps + 1, turn, 0)

    to = (me.right, me.left)

    def hops(side, kind):
        longer = (core + (kind in (Q, V, DOWN))) % 2
        return nz // 2 - longer if side == 0 else nz // 2 - 1 + longer

    def source_of(side, s):
        return 2 * me.z_at(side, s) + core

    def onward(side, s, kind):
        at = piece(kind, source_of(side, s), n_tp, gcols, grows)
        return remote(at, at, w_send.at[kind], wr_recv.at[side, s, kind], to[side])

    def arrival(side, s, kind):
        at = piece(kind, source_of(side, s), n_tp, gcols, grows)
        return remote(at, at, w_send.at[kind], wr_recv.at[side, s - 1, kind], to[side])

    def across(side, s, kind):
        source = source_of(side, s)
        at = piece(kind, source, n_tp, gcols, grows)
        return remote(at, at, w_send.at[kind], sib_sem(source // 2, kind), me.sib)

    def take(side, s, kind):
        @pl.when(has(kind, source_of(side, s)) & (s <= hops(side, kind)))
        def _():
            arrival(side, s, kind).wait_recv()

            @pl.when(s < hops(side, kind))
            def _():
                onward(side, s, kind).start()

            across(side, s, kind).start()

    def take_both(s, kind):
        for side in range(2):
            take(side, s, kind)

    cut = seq_len // 2

    def late_send(side, s, h):
        at, ring = pl.ds(h * cut, cut), rings[side]
        return remote(ring.at[half * s + half - 1, at], ring.at[half * (s + 1) + half - 1, at], e_send.at[side], e_recv.at[side, s, h], to[side])

    def late_step(s):
        for h in range(2):
            at, i = pl.ds(h * cut, cut), half * s + half - 1
            for side, ring in enumerate(rings):
                @pl.when(s > 0)
                def _():
                    late_send(side, s - 1, h).wait_recv()

                total = loc[side, s, at, :].astype(F32) + ring[i, at, :].astype(F32)

                @pl.when(s < nz - 1)
                def _():
                    ring[i, at, :] = total.astype(BF16)

                @pl.when(s == nz - 1)
                def _():
                    close(side, 2 * (half - 1) + side, at, (steps - 1) % 3, total.astype(BF16), nown.at[side, at])

            @pl.when(s < nz - 1)
            def _():
                for side in range(2):
                    late_send(side, s, h).start()

    layer = SecondLayer(me, nall, acc, qkv_v, out_v, up_v, down_v, gcols, grows, cos_ref, sin_ref, slab_sem)

    def start_slab(number):
        settle(gcols.at[pl.ds(0, 2)], ws_recv.at[me.z_at(*layer.order[number])])
        if number == 0:
            for kind in (UP, DOWN):
                first_hops(kind)[3].wait()
        start(layer.slab_loads(number))

    def wait_slab(number):
        layer.wait_slab(number)

    def start_heads(first):
        start(layer.head_loads(first))

    def wait_heads():
        layer.wait_heads()

    def await_pair(p):
        settle(nall.at[pl.ds(2 * p, 2), pl.ds(0, 3 * seq_len)], n_recv.at[p])

    def send_part(tile, peer):
        return remote(nall.at[tile, rows_of(me.peer_q[peer])], part_in.at[tile, peer], p_send.at[tile], p_recv.at[tile], me.peers[peer])

    def keep_part(tile):
        return [pltpu.make_async_copy(nall.at[tile], pout.at[tile - 2], o_sem.at[tile - 2, 0]),
                pltpu.make_async_copy(acc.at[tile, rows_of(q)], pown.at[tile - 2], o_sem.at[tile - 2, 1])]

    def hand_out(tile):
        settle(nall.at[tile, pl.ds(0, 3 * seq_len)], n_send.at[tile])
        layer.round_off(tile)
        if tile < 2:
            for peer in range(3):
                send_part(tile, peer).start()
        else:
            start(keep_part(tile))

    def finish_tile(tile):
        settle(part_in.at[tile], p_recv.at[tile])
        total = acc[tile, rows_of(q), :]
        for peer in range(3):
            total = total + part_in[tile, peer].astype(F32)
        done[tile] = (done[tile].astype(F32) + total.astype(BF16).astype(F32)).astype(BF16)

    def keep_done(which):
        start([pltpu.make_async_copy(done.at[k], done_h.at[k], done_sem.at[0]) for k in which])

    keep_n = [pltpu.make_async_copy(nown.at[side], nown_h.at[side], done_sem.at[1]) for side in range(2)]

    def drain_rings():
        for side, ring in enumerate(rings):
            settle(ring.at[pl.ds(0, (nz - 1) * (half - 1))], r_send.at[side])
        send_sib(steps - 2).wait_send()
        send_sib(steps - 1).wait_send()

    def drain_weights():
        for kind in kinds:
            sent = jnp.where(has(kind, me.tp), 3, 0)
            for s in range(1, nz // 2 + 1):
                for side in range(2):
                    here = has(kind, source_of(side, s))
                    sent += jnp.where(here & (s <= hops(side, kind)), 1, 0) + jnp.where(here & (s < hops(side, kind)), 1, 0)
            for count in [2 * nz - 1] if kind in (UP, DOWN) else [3, 4]:
                @pl.when(sent == count)
                def _():
                    settle(gcols.at[pl.ds(0, count)], w_send.at[kind])

    attn = (Q, K, V, OUT)

    def own_heads_kept():
        for kind in attn:
            @pl.when(has(kind, me.tp))
            def _():
                first_hops(kind)[3].wait()

        settle(gcols.at[pl.ds(0, 2 * len(attn))], ws_recv.at[nz])

    layer.clear()
    def reload():
        start(layer.slab_loads(5))

    layer.run([
        ([call(start_slab, 0), call(take_both, 1, K), call(take_both, 2, K), call(take_both, 1, V), call(take_both, 1, OUT), call(take_both, 2, V), call(take_both, 2, OUT), call(take_both, 1, Q), call(take_both, 2, Q), call(take_both, 1, DOWN), call(await_pair, 0), call(take_both, 3, V), call(take_both, 1, UP), call(await_pair, 1), call(wait_slab, 0)], None, (0, 0)),
        ([call(start_slab, 1)], None, (0, 1)),
        ([drain_rings, call(keep_done, range(2, 4)), call(start_slab, 2), call(take_both, 3, K), call(wait_slab, 1)], None, (1, 0)),
        ([], None, (1, 1)),
        ([call(take_both, 3, Q), call(take_both, 3, OUT), call(take_both, 4, OUT), call(take_both, 2, DOWN), call(take_both, 2, UP), call(take_both, 4, K), call(start_slab, 3), call(take_both, 4, Q), call(take_both, 4, V), call(wait_slab, 2)], None, (2, 0)),
        ([own_heads_kept, call(start_heads, 0)], None, (2, 1)),
        ([call(start_slab, 4), wait_heads], None, (0,)),
        ([], None, (1,)),
        ([], None, (2,)),
        ([], None, (3,)),
        ([call(start_heads, 2)], 0, ()),
        ([call(wait_slab, 3)], None, (3, 0)),
        ([call(take_both, 3, UP)], None, (3, 1)),
        ([call(take_both, 3, DOWN), call(start_slab, 5), call(wait_slab, 4)], None, (4, 0)),
        ([], None, (4, 1)),
        ([call(start_slab, 6)], 1, ()),
        ([wait_heads], None, (0,)),
        ([], None, (1,)),
        ([call(wait_slab, 5)], None, (5, 0)),
        ([call(take_both, 4, DOWN), call(wait_slab, 6)], None, (6, 0)),
        ([call(take_both, 4, UP)], 2, ()),
        ([call(start_slab, 7), call(wait_slab, 7)], None, (7, 0)),
        ([call(hand_out, 0)], 3, ()),
        ([call(hand_out, 1)], None, (2,)),
        ([], 4, (3,)),
        ([], 5, (7, 1)),
        ([], 6, ()),
        ([reload], None, (6, 1)),
        ([call(wait_slab, 5)], None, (5, 1)),
        ([call(hand_out, 2), call(hand_out, 3), drain_weights, call(finish_tile, 0)], 7, ()),
    ], late_step)
    finish_tile(1)
    keep_done(range(0, 2))
    keep_done(range(4, per))
    start(keep_n)
    for side, ring in enumerate(rings):
        settle(ring.at[pl.ds(0, nz - 1)], e_send.at[side])
    for tile in range(2):
        settle(part_in.at[tile], p_send.at[tile])
        wait(keep_part(2 + tile))
    settle(done, done_sem.at[0])
    settle(nown, done_sem.at[1])


def second_kernel(n_dp, n_tp, done_h, nown, cos_h, sin_h, pout, pown, gcols, grows, out,
                  cos_ref, sin_ref, done, qkv_v, out_v, up_v, down_v, nall, acc, own, part_in,
                  slab_sem, o_sem, n_sem, p_send, p_recv, g_send, r_recv, s_recv):
    me = Place(n_dp, n_tp)
    me.greet()
    nz, core, z, q = me.nz, me.core, me.z, me.q
    per, seq_len, d_model = done_h.shape
    half = per // 2
    layer = SecondLayer(me, nall, acc, qkv_v, out_v, up_v, down_v, gcols, grows, cos_ref, sin_ref, slab_sem)
    keep = [pltpu.make_async_copy(pown, own, o_sem.at[0]), pltpu.make_async_copy(done_h, done, o_sem.at[1])]
    tables = [pltpu.make_async_copy(cos_h, cos_ref, o_sem.at[2]), pltpu.make_async_copy(sin_h, sin_ref, o_sem.at[3])]
    start(keep + tables)
    start(layer.slab_loads(0))
    start(layer.slab_loads(1))
    start(layer.head_loads(0))

    def rows_of(member):
        return pl.ds(pl.multiple_of(member * seq_len, seq_len), seq_len)

    def seq_of(zs, co, k):
        return per * (2 * zs + co) + k % 2 * half + k // 2

    def send_n(side, peer):
        return remote(nown.at[side], nall.at[side, rows_of(q)], n_sem.at[0], n_sem.at[1], me.peers[peer])

    def send_part(k, peer):
        at = rows_of(me.peer_q[peer])
        src = pout.at[k - 2, at] if k < 4 else nall.at[k - 4, at]
        return remote(src, part_in.at[k - 2, peer], p_send.at[k - 2], p_recv.at[k - 2], me.peers[peer])

    def start_parts(k):
        for peer in range(3):
            send_part(k, peer).start()

    def first_hops(k, src=None):
        at = out.at[seq_of(z, core, k)]
        src = at if src is None else src
        return [remote(src, at, g_send.at[k], r_recv.at[0, k, 0], me.right),
                remote(src, at, g_send.at[k], r_recv.at[1, k, 0], me.left),
                remote(src, at, g_send.at[k], s_recv.at[k], me.sib)]

    ready = [pltpu.make_async_copy(done_h.at[k], out.at[seq_of(z, core, k)], o_sem.at[4 + k]) for k in range(2)]
    mine = [pltpu.make_async_copy(nown.at[side], nall.at[side, rows_of(q)], o_sem.at[6 + side]) for side in range(2)]
    start(ready + mine)

    to = (me.right, me.left)

    def hops(side, k):
        longer = (k + core) % 2
        return nz // 2 - longer if side == 0 else nz // 2 - 1 + longer

    def arrival(side, k, s):
        at = out.at[seq_of(me.z_at(side, s), core, k)]
        return remote(at, at, g_send.at[k], r_recv.at[side, k, s - 1], to[side])

    def onward(side, k, s):
        at = out.at[seq_of(me.z_at(side, s), core, k)]
        return remote(at, at, g_send.at[k], r_recv.at[side, k, s], to[side])

    def across(side, k, s):
        at = out.at[seq_of(me.z_at(side, s), core, k)]
        return remote(at, at, g_send.at[k], s_recv.at[k], me.sib)

    def finish(k):
        settle(part_in.at[k - 2], p_recv.at[k - 2])
        if k == 2:
            wait(keep)
        total = own[k - 2] if k < 4 else acc[k - 4, rows_of(q), :]
        for peer in range(3):
            total = total + part_in[k - 2, peer].astype(F32)
        out[seq_of(z, core, k)] = (done[k].astype(F32) + total.astype(BF16).astype(F32)).astype(BF16)
        start(first_hops(k))

    def pass_on(k, s):
        for side in range(2):
            @pl.when(s <= hops(side, k))
            def _():
                arrival(side, k, s).wait_recv()

                @pl.when(s < hops(side, k))
                def _():
                    onward(side, k, s).start()

                across(side, k, s).start()

    me.meet()
    for k in range(2):
        start(first_hops(k, done_h.at[k]))
    for side in range(2):
        for peer in range(3):
            send_n(side, peer).start()
    start_parts(2)
    start_parts(3)

    def await_all():
        settle(nall.at[:, pl.ds(0, 3 * seq_len)], n_sem.at[1])
        wait(mine)

    def hand_out(side):
        layer.round_off(side)
        start_parts(4 + side)

    def start_slab(number):
        start(layer.slab_loads(number))

    def wait_slab(number):
        layer.wait_slab(number)

    def start_heads(first):
        start(layer.head_loads(first))

    def wait_heads():
        layer.wait_heads()

    def stages(*names):
        for k, s in names:
            if s == 0:
                finish(k)
            else:
                pass_on(k, s)

    layer.clear()
    assert (per, nz, n_tp // 4) == (6, 8, 4)
    layer.run([
        ([call(stages, (0, 1), (1, 1), (0, 2)), await_all, call(stages, (1, 2)), call(wait_slab, 0)], None, (0, 0)),
        ([call(stages, (0, 3), (2, 0)), call(start_slab, 2), call(wait_slab, 1)], None, (1, 0)),
        ([call(start_slab, 3), call(wait_slab, 2)], None, (2, 0)),
        ([call(start_slab, 4), call(wait_slab, 3)], None, (3, 0)),
        ([call(stages, (0, 4)), call(start_slab, 5), call(wait_slab, 4)], None, (4, 0)),
        ([call(stages, (1, 3)), call(start_slab, 6), wait_heads, call(wait, tables)], None, (0,)),
        ([call(stages, (2, 1))], None, (1,)),
        ([call(start_heads, 2), call(wait_slab, 5)], None, (5, 0)),
        ([call(stages, (3, 0)), call(start_slab, 7), call(wait_slab, 6)], None, (6, 0)),
        ([call(wait_slab, 7)], None, (7, 0)),
        ([wait_heads], None, (0,)),
        ([call(stages, (2, 2)), call(hand_out, 0), call(stages, (1, 4), (3, 1), (2, 3))], None, (1,)),
        ([call(hand_out, 1)], None, ()),
    ])
    stages((3, 2), (4, 0), (5, 0), (3, 3), (5, 1), (4, 1))

    def drain(k):
        settle(out.at[pl.ds(0, 2 * nz - 1)], g_send.at[k])
        settle(out.at[pl.ds(0, nz)], s_recv.at[k])

    wait(ready)
    for k in range(2, per):
        settle(part_in.at[k - 2], p_send.at[k - 2])
    settle(nall.at[:, pl.ds(0, 3 * seq_len)], n_sem.at[0])
    for k in range(2):
        drain(k)
    stages((5, 2), (4, 2), (5, 3), (2, 4), (4, 3), (4, 4), (5, 4), (3, 4))
    for k in range(2, per):
        drain(k)


def rope_rows(seq_len, head_dim, copies):
    inv_freq = ROPE_BASE ** (-2.0 * np.arange(head_dim // 2) / head_dim)
    angles = np.arange(seq_len)[:, None] * inv_freq[None, :]
    cos, sin = np.cos(angles), np.sin(angles)
    return [np.tile(np.concatenate(halves, 1), (copies, 1)).astype(np.float32) for halves in ((cos, cos), (-sin, sin))]


def solution(mesh):
    n_dp, n_tp = mesh.shape["dp"], mesh.shape["tp"]
    nz = n_tp // 2
    any_spec = pl.BlockSpec(memory_space=pl.ANY)
    vmem_spec = pl.BlockSpec(memory_space=pltpu.VMEM)
    dma = pltpu.SemaphoreType.DMA

    def shard_body(act_in, ln_gain, ln_bias, w_qkv, w_out, w_up, w_down):
        n_seq, seq_len, d_model = act_in.shape
        layers, _, _, qkv_cols = w_qkv.shape
        head_dim, ff = w_out.shape[1], w_up.shape[2]
        per = n_seq // n_tp
        half = per // 2
        heads = n_tp // 4
        tile = 4 * seq_len
        w_qkv = w_qkv.reshape(layers, d_model, qkv_cols)
        cos, sin = rope_rows(seq_len, head_dim, 4)
        seq_block = (seq_len, d_model)
        n_cols, n_rows = n_tp + 3 * heads, n_tp + heads
        steps = nz * half
        done, nown, pout, pown, gcols, grows = pl.pallas_call(
            functools.partial(first_kernel, n_dp, n_tp),
            name="layer_one",
            out_shape=(jax.ShapeDtypeStruct((per, *seq_block), BF16), jax.ShapeDtypeStruct((2, *seq_block), BF16), jax.ShapeDtypeStruct((2, tile, d_model), BF16), jax.ShapeDtypeStruct((2, *seq_block), F32),
                       jax.ShapeDtypeStruct((n_cols, d_model, LANES), BF16), jax.ShapeDtypeStruct((n_rows, LANES, d_model), BF16)),
            in_specs=[any_spec] * 9,
            out_specs=(any_spec,) * 6,
            scratch_shapes=[
                pltpu.VMEM(ln_gain.shape, F32), pltpu.VMEM(ln_bias.shape, F32), pltpu.VMEM(cos.shape, F32), pltpu.VMEM(sin.shape, F32),
                pltpu.VMEM((per, *seq_block), BF16), pltpu.VMEM((2, *seq_block), BF16),
                pltpu.VMEM((d_model, 2 * qkv_cols), BF16), pltpu.VMEM((2 * head_dim, d_model), BF16), pltpu.VMEM((2, d_model, ff // 2), BF16), pltpu.VMEM((2, ff // 2, d_model), BF16),
                pltpu.VMEM((3, 4, *seq_block), BF16), pltpu.VMEM((tile, d_model), BF16), pltpu.VMEM((tile, head_dim), BF16), pltpu.VMEM((tile, ff), BF16),
                pltpu.VMEM((2, 2 * seq_len, d_model), F32), pltpu.VMEM((2, 2 * seq_len, d_model), BF16), pltpu.VMEM((4, 2 * seq_len, d_model), BF16),
                pltpu.VMEM((steps, *seq_block), BF16), pltpu.VMEM((steps, *seq_block), BF16), pltpu.VMEM((2, nz, *seq_block), BF16),
                pltpu.VMEM((4, tile, d_model), BF16), pltpu.VMEM((4, tile, d_model), F32), pltpu.VMEM((2, 3, *seq_block), BF16),
                pltpu.VMEM((4, d_model, LANES), BF16), pltpu.VMEM((2, LANES, d_model), BF16),
                dma((6,)), dma((3,)), dma((2,)), dma((4,)), dma((2,)), dma((2, (nz - 1) * (half - 1))), dma((2,)), dma((2, nz - 1, 2)),
                dma((6,)), dma((6,)), dma((6,)), dma((2, nz // 2, 6)), dma((nz + 1,)), dma((4,)), dma((2,)), dma((3, 2)), dma((2,)), dma((2,)), dma((2, 2)), dma((4,)), dma((2,)),
            ],
            compiler_params=pltpu.CompilerParams(collective_id=1, has_side_effects=True, vmem_limit_bytes=63 * 2**20),
        )(act_in, ln_gain, ln_bias, cos, sin, w_qkv, w_out, w_up, w_down)
        return pl.pallas_call(
            functools.partial(second_kernel, n_dp, n_tp),
            name="layer_two",
            out_shape=pltpu.VMEM(act_in.shape, BF16),
            in_specs=[any_spec] * 8,
            out_specs=vmem_spec,
            scratch_shapes=[
                pltpu.VMEM(cos.shape, F32), pltpu.VMEM(sin.shape, F32), pltpu.VMEM((per, *seq_block), BF16),
                pltpu.VMEM((d_model, 2 * qkv_cols), BF16), pltpu.VMEM((2 * head_dim, d_model), BF16), pltpu.VMEM((2, d_model, 2 * LANES), BF16), pltpu.VMEM((2, 2 * LANES, d_model), BF16),
                pltpu.VMEM((2, tile, d_model), BF16), pltpu.VMEM((2, tile, d_model), F32), pltpu.VMEM((2, *seq_block), F32), pltpu.VMEM((4, 3, *seq_block), BF16),
                dma((3, 2)), dma((8,)), dma((2,)), dma((4,)), dma((4,)), dma((per,)), dma((2, per, nz // 2)), dma((per,)),
            ],
            compiler_params=pltpu.CompilerParams(collective_id=2, has_side_effects=True, vmem_limit_bytes=38 * 2**20),
        )(done, nown, cos, sin, pout, pown, gcols, grows)

    return jax.shard_map(shard_body, mesh=mesh, in_specs=(P("dp", None, None), P(None, None), P(None, None), P(None, None, "tp", None), P(None, "tp", None), P(None, None, "tp"), P(None, "tp", None)), out_specs=P("dp", None, None), check_vma=False)
```

```python
import functools
import math

import jax
import jax.numpy as jnp
import numpy as np
from jax import lax
from jax.experimental import pallas as pl
from jax.experimental.pallas import tpu as pltpu
from jax.sharding import PartitionSpec as P

LN_EPS = 1e-5
ROPE_BASE = 10000.0
MESH = pl.DeviceIdType.MESH
BF16 = jnp.bfloat16
F32 = jnp.float32
LANES = 128
MIB = 1 << 20
SIDES = range(2)
PEERS = range(3)
UP, Q, K, V, DOWN, OUT = range(6)


def norm_rows(hidden_f, gain, bias):
    row_mean = jnp.mean(hidden_f, axis=-1, keepdims=True)
    centered = hidden_f - row_mean
    row_var = jnp.mean(centered * centered, axis=-1, keepdims=True)
    return (centered * lax.rsqrt(row_var + LN_EPS) * gain + bias).astype(BF16)


def rope(heads, cos, sin):
    return (heads * cos + pltpu.roll(heads, heads.shape[-1] // 2, 1) * sin).astype(BF16)


def gelu(values):
    return (0.5 * values * (1.0 + lax.erf(values * math.sqrt(0.5)))).astype(BF16)


def attend(query, keys, values, seq_len):
    rows, head_dim = query.shape
    block = 2 * seq_len
    row = lax.broadcasted_iota(jnp.int32, (block, block), 0)
    col = lax.broadcasted_iota(jnp.int32, (block, block), 1)
    allowed = (row >= col) & (row // seq_len == col // seq_len)
    contexts = []
    for first in range(0, rows, block):
        at = slice(first, first + block)
        scores = lax.dot_general(query[at], keys[at], (((1,), (1,)), ((), ())), preferred_element_type=F32) * (head_dim ** -0.5)
        scores = jnp.where(allowed, scores, -1e30)
        weights = jnp.exp(scores - jnp.max(scores, axis=-1, keepdims=True))
        probs = (weights / jnp.sum(weights, axis=-1, keepdims=True)).astype(BF16)
        contexts.append(jnp.dot(probs, values[at], preferred_element_type=F32).astype(BF16))
    return jnp.concatenate(contexts, axis=0)


def context_of(proj, cos_ref, sin_ref, seq_len):
    head_dim = cos_ref.shape[1]
    query = rope(proj[:, :head_dim], cos_ref[...], sin_ref[...])
    keys = rope(proj[:, head_dim : 2 * head_dim], cos_ref[...], sin_ref[...])
    return attend(query, keys, proj[:, 2 * head_dim :].astype(BF16), seq_len)


def head_context(normed, qkv_w, cos_ref, sin_ref, seq_len):
    return context_of(jnp.dot(normed, qkv_w, preferred_element_type=F32), cos_ref, sin_ref, seq_len)


class Place:
    def __init__(self, n_dp, n_tp):
        side = math.isqrt(n_dp)
        assert side * side == n_dp and side % 2 == 0 and n_tp % 4 == 0
        self.n_tp, self.nz = n_tp, n_tp // 2
        self.dp, self.tp = lax.axis_index("dp"), lax.axis_index("tp")
        self.z, self.core = self.tp // 2, self.tp % 2
        x, y = self.dp // side, self.dp % side
        xf, yf = x + 1 - 2 * (x % 2), y + 1 - 2 * (y % 2)
        self.q = (x % 2) * 2 + y % 2
        self.peers = [{"dp": xf * side + y}, {"dp": x * side + yf}, {"dp": xf * side + yf}]
        self.peer_q = [(1 - x % 2) * 2 + y % 2, (x % 2) * 2 + 1 - y % 2, (1 - x % 2) * 2 + 1 - y % 2]
        self.sib = {"tp": 2 * self.z + 1 - self.core}
        self.right = {"tp": 2 * ((self.z + 1) % self.nz) + self.core}
        self.left = {"tp": 2 * ((self.z + self.nz - 1) % self.nz) + self.core}

    def z_at(self, side, s):
        return (self.z + self.nz - s) % self.nz if side == 0 else (self.z + s) % self.nz

    def others(self):
        return [self.sib, self.right, self.left, *self.peers]

    def greet(self):
        barrier = pltpu.get_barrier_semaphore()
        for other in self.others():
            pl.semaphore_signal(barrier, inc=1, device_id=other, device_id_type=MESH)

    def meet(self):
        pl.semaphore_wait(pltpu.get_barrier_semaphore(), len(self.others()))


def remote(src, dst, send_sem, recv_sem, device):
    return pltpu.make_async_remote_copy(src_ref=src, dst_ref=dst, send_sem=send_sem, recv_sem=recv_sem, device_id=device, device_id_type=MESH)


def piece(kind, source, n_tp, cols, rows):
    if kind == UP:
        return cols.at[source]
    if kind == DOWN:
        return rows.at[source]
    head = source // 8 * 2 + source % 2
    if kind == OUT:
        return rows.at[n_tp + head]
    return cols.at[n_tp + 3 * head + kind - Q]


class SecondLayer:
    def __init__(self, place, nall, acc, qkv_v, out_v, up_v, down_v, gcols, grows, cos_ref, sin_ref, sem):
        self.place, self.nall, self.acc, self.sem = place, nall, acc, sem
        self.qkv_v, self.out_v, self.up_v, self.down_v = qkv_v, out_v, up_v, down_v
        self.gcols, self.grows, self.cos_ref, self.sin_ref = gcols, grows, cos_ref, sin_ref
        self.seq_len = nall.shape[1] // 4
        far = place.nz // 2
        self.order = [(0, 0)] + [(side, s) for s in range(1, far) for side in SIDES] + [(0, far)]

    def slab_loads(self, number):
        slot, zs = number % 2, self.place.z_at(*self.order[number])
        copies = []
        for c in SIDES:
            at = pl.ds(c * LANES, LANES)
            copies.append((self.gcols.at[2 * zs + c], self.up_v.at[slot, :, at], self.sem.at[slot, 0]))
            copies.append((self.grows.at[2 * zs + c], self.down_v.at[slot, at, :], self.sem.at[slot, 1]))
        return [pltpu.make_async_copy(*copy) for copy in copies]

    def head_loads(self, first):
        n_tp, head_dim = self.place.n_tp, self.cos_ref.shape[1]
        copies = []
        for n in SIDES:
            for i in range(3):
                at = pl.ds((3 * n + i) * head_dim, head_dim)
                copies.append((self.gcols.at[n_tp + 3 * (first + n) + i], self.qkv_v.at[:, at], self.sem.at[2, 0]))
            copies.append((self.grows.at[n_tp + first + n], self.out_v.at[pl.ds(n * head_dim, head_dim)], self.sem.at[2, 1]))
        return [pltpu.make_async_copy(*copy) for copy in copies]

    def wait_slab(self, number):
        slot = number % 2
        settle(self.up_v.at[slot], self.sem.at[slot, 0])
        settle(self.down_v.at[slot], self.sem.at[slot, 1])

    def wait_heads(self):
        settle(self.qkv_v, self.sem.at[2, 0])
        settle(self.out_v, self.sem.at[2, 1])

    def clear(self):
        for i in range(self.acc.shape[0]):
            self.acc[i] = jnp.zeros(self.acc.shape[1:], F32)

    def slab(self, slot, p):
        nall, acc = self.nall, self.acc
        pair = (2 * p, 2 * p + 1)
        hidden = [gelu(jnp.dot(nall[i], self.up_v[slot], preferred_element_type=F32)) for i in pair]
        step = 512
        for first in range(0, acc.shape[2], step):
            cols = pl.ds(first, step)
            for i, rows in zip(pair, hidden):
                acc[i, :, cols] += jnp.dot(rows, self.down_v[slot, :, cols], preferred_element_type=F32)

    def heads(self, i):
        nall, acc, head_dim = self.nall, self.acc, self.cos_ref.shape[1]
        proj = jnp.dot(nall[i], self.qkv_v[...], preferred_element_type=F32)
        both = [context_of(proj[:, 3 * head_dim * n : 3 * head_dim * (n + 1)], self.cos_ref, self.sin_ref, self.seq_len) for n in SIDES]
        context = jnp.concatenate(both, axis=1)
        step = 512
        for first in range(0, acc.shape[2], step):
            cols = pl.ds(first, step)
            acc[i, :, cols] += jnp.dot(context, self.out_v[:, cols], preferred_element_type=F32)

    def round_off(self, i):
        self.nall[i] = self.acc[i].astype(BF16)

    def run(self, program, actions, late_step=None):
        steps, events, late = [], [], None

        def end(unit):
            nonlocal events, late
            steps.append((events, late, unit))
            events, late = [], None

        for word in " ".join(program).split():
            letter, rest = word[0], word[1:]
            if letter in "SH":
                end([int(digit) for digit in rest])
                continue
            if late is not None:
                end([])
            if letter == "R":
                late = int(rest)
            else:
                events.append(functools.partial(actions[letter], rest))
        if events or late is not None:
            end([])

        def pick(values, default):
            def at(u):
                found = jnp.int32(default)
                for k, value in enumerate(values):
                    if value is not None:
                        found = jnp.where(u == k, value, found)
                return found
            return at

        late = pick([step[1] for step in steps], -1)
        slab = [step[2] if len(step[2]) == 2 else [None, None] for step in steps]
        slot = pick([number if number is None else number % 2 for number, _ in slab], -1)
        pair = pick([p for _, p in slab], 0)
        tile = pick([step[2][0] if len(step[2]) == 1 else None for step in steps], -1)

        def turn(u, carry):
            for k, step in enumerate(steps):
                if step[0]:
                    @pl.when(u == k)
                    def _():
                        for event in step[0]:
                            event()

            if late_step:
                @pl.when(late(u) >= 0)
                def _():
                    late_step(late(u))

            @pl.when(slot(u) >= 0)
            def _():
                self.slab(slot(u), pair(u))

            @pl.when(tile(u) >= 0)
            def _():
                self.heads(tile(u))

            return carry

        lax.fori_loop(0, len(steps), turn, 0)


def settle(ref, sem):
    pltpu.make_async_copy(ref, ref, sem).wait()


def start(copies):
    for copy in copies:
        copy.start()


def wait(copies):
    for copy in copies:
        copy.wait()


def first_kernel(n_dp, n_tp, x, gains_h, biases_h, cos_h, sin_h, qkv, out_w, up, down,
                 done_h, nown_h, pout, pown, gcols, grows,
                 gains, biases, cos_ref, sin_ref, done, nown, qkv_v, out_v, up_v, down_v, xbuf, normed, ctx, act, own, sib_out, sib_in, ring_r, ring_l, loc, nall, acc, part_in, st_cols, st_rows,
                 w_sem, x_sem, sib_send, sib_recv, r_send, r_recv, e_send, e_recv,
                 st_sem, loc_sem, w_send, wr_recv, ws_recv, n_send, n_recv, slab_sem, p_send, p_recv, o_sem, small_sem, done_sem):
    me = Place(n_dp, n_tp)
    me.greet()
    nz, core, z, q = me.nz, me.core, me.z, me.q
    n_seq, seq_len, d_model = x.shape
    head_dim, ff = out_w.shape[1], up.shape[2]
    per = n_seq // n_tp
    half = per // 2
    steps = nz * half

    wide = ff // 2
    first_w = [pltpu.make_async_copy(src, dst, w_sem.at[i]) for i, (src, dst) in
               enumerate(((qkv.at[0], qkv_v.at[:, pl.ds(0, qkv.shape[2])]), (up.at[0, :, pl.ds(0, wide)], up_v.at[0]), (up.at[0, :, pl.ds(wide, wide)], up_v.at[1]),
                         (out_w.at[0], out_v.at[pl.ds(0, head_dim)]), (down.at[0, pl.ds(0, wide)], down_v.at[0]), (down.at[0, pl.ds(wide, wide)], down_v.at[1])))]

    def owner_seq(zo, co, j):
        return per * (2 * zo + co) + j

    def tile_seqs(i):
        s, j = i // half, i % half
        zr, zl = (z + 2 * nz - 1 - s) % nz, (z + 1 + s) % nz
        return [owner_seq(zr, core, j), owner_seq(zl, core, half + j), owner_seq(zr, 1 - core, j), owner_seq(zl, 1 - core, half + j)]

    def fetch(i):
        for place, seq in enumerate(tile_seqs(i)):
            pltpu.make_async_copy(x.at[seq], xbuf.at[i % 3, place], x_sem.at[i % 3]).start()

    small = [pltpu.make_async_copy(src, dst, small_sem.at[i]) for i, (src, dst) in enumerate(((gains_h, gains), (biases_h, biases), (cos_h, cos_ref), (sin_h, sin_ref)))]
    loads = {UP: (up.at[1, :, pl.ds(pl.multiple_of(q * LANES, LANES), LANES)], st_cols.at[UP]),
             DOWN: (down.at[1, pl.ds(pl.multiple_of(q * LANES, LANES), LANES), :], st_rows.at[0]),
             OUT: (out_w.at[1], st_rows.at[1])}
    for kind in (Q, K, V):
        loads[kind] = (qkv.at[1, :, pl.ds((kind - Q) * head_dim, head_dim)], st_cols.at[kind])
    kinds = (Q, K, V, OUT, UP, DOWN)
    loads = {kind: pltpu.make_async_copy(*loads[kind], st_sem.at[kind]) for kind in kinds}

    loads[UP].start()
    fetch(0)
    start(small)
    start(first_w[:3])

    def start_rest():
        wait(small)
        start(first_w[3:])
        start([loads[kind] for kind in kinds if kind != UP])

    def has(kind, source):
        return source >= 0 if kind in (UP, DOWN) else (source // 2 + 2 * (source % 2)) % 4 == q

    def staged(kind):
        return st_rows.at[kind - DOWN] if kind >= DOWN else st_cols.at[kind]

    def first_hops(kind):
        src, dst = staged(kind), piece(kind, me.tp, n_tp, gcols, grows)
        return [remote(src, dst, w_send.at[kind], wr_recv.at[0, 0, kind], me.right),
                remote(src, dst, w_send.at[kind], wr_recv.at[1, 0, kind], me.left),
                remote(src, dst, w_send.at[kind], sib_sem(z, kind), me.sib),
                pltpu.make_async_copy(src, dst, loc_sem.at[kind])]

    def sib_sem(zs, kind):
        return ws_recv.at[zs] if kind in (UP, DOWN) else ws_recv.at[nz]

    def send_first(kind):
        loads[kind].wait()

        @pl.when(has(kind, me.tp))
        def _():
            start(first_hops(kind))

    rings = (ring_r, ring_l)
    for i in range(half):
        for ring in rings:
            ring[i] = jnp.zeros(ring.shape[1:], BF16)

    def send_sib(i):
        return remote(sib_out.at[i % 2], sib_in.at[i % 4], sib_send.at[i % 2], sib_recv.at[i % 4], me.sib)

    def early(i):
        return i // half * (half - 1) + i % half

    def send_r(i):
        return remote(ring_r.at[i], ring_r.at[i + half], r_send.at[0], r_recv.at[0, early(i)], me.right)

    def send_l(i):
        return remote(ring_l.at[i], ring_l.at[i + half], r_send.at[1], r_recv.at[1, early(i)], me.left)

    def rows_of(member):
        return pl.ds(pl.multiple_of(member * seq_len, seq_len), seq_len)

    def send_n(tile, peer):
        at = nall.at[tile, rows_of(q)]
        return remote(at, at, n_send.at[tile], n_recv.at[tile // 2], me.peers[peer])

    def compute(i, waits=(), then=None):
        slot = i % 3
        pltpu.make_async_copy(x.at[pl.ds(0, 4)], xbuf.at[slot], x_sem.at[slot]).wait()
        if then:
            then()

        @pl.when(i + 1 < steps)
        def _():
            fetch(i + 1)

        @pl.when(i >= 2)
        def _():
            send_sib(i - 2).wait_send()

        for member in range(4):
            normed[pl.ds(member * seq_len, seq_len), :] = norm_rows(xbuf[slot, member].astype(F32), gains[pl.ds(0, 1), :], biases[pl.ds(0, 1), :])
        wait(waits[:3])
        ctx[...] = head_context(normed[...], qkv_v[:, : 3 * head_dim], cos_ref, sin_ref, seq_len)
        for n in SIDES:
            act[:, n * wide : (n + 1) * wide] = gelu(jnp.dot(normed[...], up_v[n], preferred_element_type=F32))
        wait(waits[3:])
        step = 512
        for first in range(0, d_model, step):
            cols = pl.ds(first, step)
            part = jnp.dot(ctx[...], out_v[:head_dim, cols], preferred_element_type=F32)
            for n in SIDES:
                part += jnp.dot(act[:, n * wide : (n + 1) * wide], down_v[n, :, cols], preferred_element_type=F32)
            own[i % 2, :, cols] = part[: 2 * seq_len]
            sib_out[i % 2, :, cols] = part[2 * seq_len :].astype(BF16)

    def finish(i):
        send_sib(i).wait_recv()
        late = i % half == half - 1
        last = i >= steps - half

        @pl.when(late)
        def _():
            for side in SIDES:
                at = pl.ds(side * seq_len, seq_len)
                loc[side, i // half] = (own[i % 2, at, :] + sib_in[i % 4, at, :].astype(F32)).astype(BF16)

        @pl.when((i >= half) & jnp.logical_not(late))
        def _():
            send_r(i - half).wait_recv()
            send_l(i - half).wait_recv()

        @pl.when(jnp.logical_not(last | late))
        def _():
            for side, ring in enumerate(rings):
                at = pl.ds(side * seq_len, seq_len)
                ring[i] = (own[i % 2, at, :] + sib_in[i % 4, at, :].astype(F32) + ring[i].astype(F32)).astype(BF16)
            send_r(i).start()
            send_l(i).start()

        @pl.when(i == steps - half - 2)
        def _():
            for kind in kinds:
                if kind != UP:
                    send_first(kind)

        @pl.when(last & jnp.logical_not(late))
        def _():
            rows = seq_len // 2
            for side, ring in enumerate(rings):
                tile = 2 * (i % half) + side
                for first in range(0, seq_len, rows):
                    at, both = pl.ds(first, rows), pl.ds(side * seq_len + first, rows)
                    update = (own[i % 2, both, :] + sib_in[i % 4, both, :].astype(F32) + ring[i, at, :].astype(F32)).astype(BF16)
                    close(side, tile, at, i % 3, update, nall.at[tile, pl.ds(pl.multiple_of(q * seq_len + first, rows), rows)])
                for peer in PEERS:
                    send_n(tile, peer).start()

    def close(side, tile, at, slot, update, normed_at):
        hidden = (xbuf[slot, side, at, :].astype(F32) + update.astype(F32)).astype(BF16)
        done[tile, at, :] = hidden
        normed_at[...] = norm_rows(hidden.astype(F32), gains[pl.ds(1, 1), :], biases[pl.ds(1, 1), :])

    me.meet()
    send_first(UP)
    compute(0, first_w, start_rest)
    send_sib(0).start()

    def turn(i, carry):
        @pl.when(i < steps)
        def _():
            compute(i)
            send_sib(i).start()

        finish(i - 1)
        return carry

    lax.fori_loop(1, steps + 1, turn, 0)

    to = (me.right, me.left)

    def hops(side, kind):
        longer = (core + (kind in (Q, V, DOWN))) % 2
        return nz // 2 - longer if side == 0 else nz // 2 - 1 + longer

    def source_of(side, s):
        return 2 * me.z_at(side, s) + core

    def onward(side, s, kind):
        at = piece(kind, source_of(side, s), n_tp, gcols, grows)
        return remote(at, at, w_send.at[kind], wr_recv.at[side, s, kind], to[side])

    def arrival(side, s, kind):
        at = piece(kind, source_of(side, s), n_tp, gcols, grows)
        return remote(at, at, w_send.at[kind], wr_recv.at[side, s - 1, kind], to[side])

    def across(side, s, kind):
        source = source_of(side, s)
        at = piece(kind, source, n_tp, gcols, grows)
        return remote(at, at, w_send.at[kind], sib_sem(source // 2, kind), me.sib)

    def take(side, s, kind):
        @pl.when(has(kind, source_of(side, s)) & (s <= hops(side, kind)))
        def _():
            arrival(side, s, kind).wait_recv()

            @pl.when(s < hops(side, kind))
            def _():
                onward(side, s, kind).start()

            across(side, s, kind).start()

    def take_both(s, kind):
        for side in SIDES:
            take(side, s, kind)

    cut = seq_len // 2

    def late_send(side, s, h):
        at, ring = pl.ds(h * cut, cut), rings[side]
        return remote(ring.at[half * s + half - 1, at], ring.at[half * (s + 1) + half - 1, at], e_send.at[side], e_recv.at[side, s, h], to[side])

    def late_step(s):
        for h in SIDES:
            at, i = pl.ds(h * cut, cut), half * s + half - 1
            for side, ring in enumerate(rings):
                @pl.when(s > 0)
                def _():
                    late_send(side, s - 1, h).wait_recv()

                total = loc[side, s, at, :].astype(F32) + ring[i, at, :].astype(F32)

                @pl.when(s < nz - 1)
                def _():
                    ring[i, at, :] = total.astype(BF16)

                @pl.when(s == nz - 1)
                def _():
                    close(side, 2 * (half - 1) + side, at, (steps - 1) % 3, total.astype(BF16), nown.at[side, at])

            @pl.when(s < nz - 1)
            def _():
                for side in SIDES:
                    late_send(side, s, h).start()

    layer = SecondLayer(me, nall, acc, qkv_v, out_v, up_v, down_v, gcols, grows, cos_ref, sin_ref, slab_sem)

    def start_slab(number):
        settle(gcols.at[pl.ds(0, 2)], ws_recv.at[me.z_at(*layer.order[number])])
        if number == 0:
            for kind in (UP, DOWN):
                first_hops(kind)[3].wait()
        start(layer.slab_loads(number))

    def await_pair(p):
        settle(nall.at[pl.ds(2 * p, 2), pl.ds(0, 3 * seq_len)], n_recv.at[p])

    def send_part(tile, peer):
        return remote(nall.at[tile, rows_of(me.peer_q[peer])], part_in.at[tile, peer], p_send.at[tile], p_recv.at[tile], me.peers[peer])

    def keep_part(tile):
        return [pltpu.make_async_copy(nall.at[tile], pout.at[tile - 2], o_sem.at[tile - 2, 0]),
                pltpu.make_async_copy(acc.at[tile, rows_of(q)], pown.at[tile - 2], o_sem.at[tile - 2, 1])]

    def hand_out(tile):
        settle(nall.at[tile, pl.ds(0, 3 * seq_len)], n_send.at[tile])
        layer.round_off(tile)
        if tile < 2:
            for peer in PEERS:
                send_part(tile, peer).start()
        else:
            start(keep_part(tile))

    def finish_tile(tile):
        settle(part_in.at[tile], p_recv.at[tile])
        total = acc[tile, rows_of(q), :]
        for peer in PEERS:
            total = total + part_in[tile, peer].astype(F32)
        done[tile] = (done[tile].astype(F32) + total.astype(BF16).astype(F32)).astype(BF16)

    def keep_done(which):
        start([pltpu.make_async_copy(done.at[k], done_h.at[k], done_sem.at[0]) for k in which])

    keep_n = [pltpu.make_async_copy(nown.at[side], nown_h.at[side], done_sem.at[1]) for side in SIDES]

    def drain_rings():
        for side, ring in enumerate(rings):
            settle(ring.at[pl.ds(0, (nz - 1) * (half - 1))], r_send.at[side])
        send_sib(steps - 2).wait_send()
        send_sib(steps - 1).wait_send()

    def drain_weights():
        for kind in kinds:
            sent = jnp.where(has(kind, me.tp), 3, 0)
            for s in range(1, nz // 2 + 1):
                for side in SIDES:
                    here = has(kind, source_of(side, s))
                    sent += jnp.where(here & (s <= hops(side, kind)), 1, 0) + jnp.where(here & (s < hops(side, kind)), 1, 0)
            for count in [2 * nz - 1] if kind in (UP, DOWN) else [3, 4]:
                @pl.when(sent == count)
                def _():
                    settle(gcols.at[pl.ds(0, count)], w_send.at[kind])

    attn = (Q, K, V, OUT)

    def own_heads_kept():
        for kind in attn:
            @pl.when(has(kind, me.tp))
            def _():
                first_hops(kind)[3].wait()

        settle(gcols.at[pl.ds(0, 2 * len(attn))], ws_recv.at[nz])

    layer.clear()
    actions = {
        "T": lambda rest: take_both(int(rest[0]), letters[rest[1]]),
        "N": lambda rest: await_pair(int(rest)),
        "L": lambda rest: start_slab(int(rest)),
        "M": lambda rest: start(layer.slab_loads(int(rest))),
        "W": lambda rest: layer.wait_slab(int(rest)),
        "A": lambda rest: own_heads_kept(),
        "X": lambda rest: start(layer.head_loads(int(rest))),
        "Y": lambda rest: layer.wait_heads(),
        "P": lambda rest: hand_out(int(rest)),
        "B": lambda rest: (drain_rings(), keep_done(range(2, 4))),
        "Z": lambda rest: (drain_weights(), finish_tile(0)),
    }
    letters = {"U": UP, "D": DOWN, "Q": Q, "K": K, "V": V, "O": OUT}
    layer.run([
        "L0 T1K T2K T1V",
        "T1O T2V T2O T1Q",
        "T2Q T1D N0 T3V",
        "T1U N1 W0 S00",
        "L1 S01 L2 T3K",
        "B W1 S10 S11",
        "T3Q T3O T4O T2D",
        "T2U T4K L3 T4Q",
        "T4V W2 S20 A",
        "X0 S21 L4 Y",
        "H0 H1 H2 H3",
        "X2 R0 W3 S30",
        "T3U S31 T3D L5",
        "W4 S40 S41 L6",
        "R1 Y H0 H1",
        "W5 S50 T4D W6",
        "S60 T4U R2 L7",
        "W7 S70 P0 R3",
        "P1 H2 R4 H3",
        "R5 S71 R6 M5",
        "S61 W5 S51 P2",
        "P3 Z R7",
    ], actions, late_step)
    finish_tile(1)
    keep_done(range(0, 2))
    keep_done(range(4, per))
    start(keep_n)
    for side, ring in enumerate(rings):
        settle(ring.at[pl.ds(0, nz - 1)], e_send.at[side])
    for tile in range(2):
        settle(part_in.at[tile], p_send.at[tile])
        wait(keep_part(2 + tile))
    settle(done, done_sem.at[0])
    settle(nown, done_sem.at[1])


def second_kernel(n_dp, n_tp, done_h, nown, cos_h, sin_h, pout, pown, gcols, grows, out,
                  cos_ref, sin_ref, done, qkv_v, out_v, up_v, down_v, nall, acc, own, part_in,
                  slab_sem, o_sem, n_sem, p_send, p_recv, g_send, r_recv, s_recv):
    me = Place(n_dp, n_tp)
    me.greet()
    nz, core, z, q = me.nz, me.core, me.z, me.q
    per, seq_len, d_model = done_h.shape
    half = per // 2
    layer = SecondLayer(me, nall, acc, qkv_v, out_v, up_v, down_v, gcols, grows, cos_ref, sin_ref, slab_sem)
    keep = [pltpu.make_async_copy(pown, own, o_sem.at[0]), pltpu.make_async_copy(done_h, done, o_sem.at[1])]
    tables = [pltpu.make_async_copy(cos_h, cos_ref, o_sem.at[2]), pltpu.make_async_copy(sin_h, sin_ref, o_sem.at[3])]
    start(keep + tables)
    start(layer.slab_loads(0))
    start(layer.slab_loads(1))
    start(layer.head_loads(0))

    def rows_of(member):
        return pl.ds(pl.multiple_of(member * seq_len, seq_len), seq_len)

    def seq_of(zs, co, k):
        return per * (2 * zs + co) + k % 2 * half + k // 2

    def send_n(side, peer):
        return remote(nown.at[side], nall.at[side, rows_of(q)], n_sem.at[0], n_sem.at[1], me.peers[peer])

    def send_part(k, peer):
        at = rows_of(me.peer_q[peer])
        src = pout.at[k - 2, at] if k < 4 else nall.at[k - 4, at]
        return remote(src, part_in.at[k - 2, peer], p_send.at[k - 2], p_recv.at[k - 2], me.peers[peer])

    def start_parts(k):
        for peer in PEERS:
            send_part(k, peer).start()

    def first_hops(k, src=None):
        at = out.at[seq_of(z, core, k)]
        src = at if src is None else src
        return [remote(src, at, g_send.at[k], r_recv.at[0, k, 0], me.right),
                remote(src, at, g_send.at[k], r_recv.at[1, k, 0], me.left),
                remote(src, at, g_send.at[k], s_recv.at[k], me.sib)]

    ready = [pltpu.make_async_copy(done_h.at[k], out.at[seq_of(z, core, k)], o_sem.at[4 + k]) for k in range(2)]
    mine = [pltpu.make_async_copy(nown.at[side], nall.at[side, rows_of(q)], o_sem.at[6 + side]) for side in SIDES]
    start(ready + mine)

    to = (me.right, me.left)

    def hops(side, k):
        longer = (k + core) % 2
        return nz // 2 - longer if side == 0 else nz // 2 - 1 + longer

    def arrival(side, k, s):
        at = out.at[seq_of(me.z_at(side, s), core, k)]
        return remote(at, at, g_send.at[k], r_recv.at[side, k, s - 1], to[side])

    def onward(side, k, s):
        at = out.at[seq_of(me.z_at(side, s), core, k)]
        return remote(at, at, g_send.at[k], r_recv.at[side, k, s], to[side])

    def across(side, k, s):
        at = out.at[seq_of(me.z_at(side, s), core, k)]
        return remote(at, at, g_send.at[k], s_recv.at[k], me.sib)

    def finish(k):
        settle(part_in.at[k - 2], p_recv.at[k - 2])
        if k == 2:
            wait(keep)
        total = own[k - 2] if k < 4 else acc[k - 4, rows_of(q), :]
        for peer in PEERS:
            total = total + part_in[k - 2, peer].astype(F32)
        out[seq_of(z, core, k)] = (done[k].astype(F32) + total.astype(BF16).astype(F32)).astype(BF16)
        start(first_hops(k))

    def pass_on(k, s):
        for side in SIDES:
            @pl.when(s <= hops(side, k))
            def _():
                arrival(side, k, s).wait_recv()

                @pl.when(s < hops(side, k))
                def _():
                    onward(side, k, s).start()

                across(side, k, s).start()

    me.meet()
    for k in range(2):
        start(first_hops(k, done_h.at[k]))
    for side in SIDES:
        for peer in PEERS:
            send_n(side, peer).start()
    start_parts(2)
    start_parts(3)

    def await_all():
        settle(nall.at[:, pl.ds(0, 3 * seq_len)], n_sem.at[1])
        wait(mine)

    def hand_out(side):
        layer.round_off(side)
        start_parts(4 + side)

    def stage(name):
        k, s = int(name[0]), int(name[1])
        if s == 0:
            finish(k)
        else:
            pass_on(k, s)

    actions = {
        "A": stage,
        "N": lambda rest: await_all(),
        "L": lambda rest: start(layer.slab_loads(int(rest))),
        "W": lambda rest: layer.wait_slab(int(rest)),
        "X": lambda rest: start(layer.head_loads(int(rest))),
        "Y": lambda rest: layer.wait_heads(),
        "C": lambda rest: wait(tables),
        "P": lambda rest: hand_out(int(rest)),
    }

    layer.clear()
    assert (per, nz, n_tp // 4) == (6, 8, 4)
    def drain(k):
        settle(out.at[pl.ds(0, 2 * nz - 1)], g_send.at[k])
        settle(out.at[pl.ds(0, nz)], s_recv.at[k])

    layer.run([
        "A01 A11 A02 N",
        "A12 W0 S00 A03",
        "A20 L2 W1 S10",
        "L3 W2 S20 L4",
        "W3 S30 A04 L5",
        "W4 S40 A13 L6",
        "Y C H0 A21",
        "H1 X2 W5 S50",
        "A30 L7 W6 S60",
        "W7 S70 Y H0",
        "A22 P0 A14 A31",
        "A23 H1 P1",
    ], actions)
    for name in (*"32 40 50".split(), *"33 51 41".split()):
        stage(name)

    wait(ready)
    for k in range(2, per):
        settle(part_in.at[k - 2], p_send.at[k - 2])
    settle(nall.at[:, pl.ds(0, 3 * seq_len)], n_sem.at[0])
    first = 2
    for k in range(first):
        drain(k)
    for name in (*"52 42 53 24".split(), *"43 44 54 34".split()):
        stage(name)
    for k in range(first, per):
        drain(k)


def rope_rows(seq_len, head_dim, copies):
    inv_freq = ROPE_BASE ** (-2.0 * np.arange(head_dim // 2) / head_dim)
    angles = np.arange(seq_len)[:, None] * inv_freq[None, :]
    cos, sin = np.cos(angles), np.sin(angles)
    return [np.tile(np.concatenate(halves, 1), (copies, 1)).astype(np.float32) for halves in ((cos, cos), (-sin, sin))]


def solution(mesh):
    n_dp, n_tp = mesh.shape["dp"], mesh.shape["tp"]
    nz = n_tp // 2
    any_spec = pl.BlockSpec(memory_space=pl.ANY)
    vmem_spec = pl.BlockSpec(memory_space=pltpu.VMEM)
    dma = pltpu.SemaphoreType.DMA

    def sems(counts):
        return [dma((int(count),)) for count in counts.split()]

    def shard_body(act_in, ln_gain, ln_bias, w_qkv, w_out, w_up, w_down):
        n_seq, seq_len, d_model = act_in.shape
        layers, _, _, qkv_cols = w_qkv.shape
        head_dim, ff = w_out.shape[1], w_up.shape[2]
        per = n_seq // n_tp
        half = per // 2
        heads = n_tp // 4
        tile = 4 * seq_len
        w_qkv = w_qkv.reshape(layers, d_model, qkv_cols)
        cos, sin = rope_rows(seq_len, head_dim, 4)
        seq_block = (seq_len, d_model)
        n_cols, n_rows = n_tp + 3 * heads, n_tp + heads
        steps = nz * half
        done, nown, pout, pown, gcols, grows = pl.pallas_call(
            functools.partial(first_kernel, n_dp, n_tp),
            name="layer_one",
            out_shape=(jax.ShapeDtypeStruct((per, *seq_block), BF16), jax.ShapeDtypeStruct((2, *seq_block), BF16), jax.ShapeDtypeStruct((2, tile, d_model), BF16), jax.ShapeDtypeStruct((2, *seq_block), F32),
                       jax.ShapeDtypeStruct((n_cols, d_model, LANES), BF16), jax.ShapeDtypeStruct((n_rows, LANES, d_model), BF16)),
            in_specs=[any_spec] * 9,
            out_specs=(any_spec,) * 6,
            scratch_shapes=[
                pltpu.VMEM(ln_gain.shape, F32), pltpu.VMEM(ln_bias.shape, F32), pltpu.VMEM(cos.shape, F32), pltpu.VMEM(sin.shape, F32),
                pltpu.VMEM((per, *seq_block), BF16), pltpu.VMEM((2, *seq_block), BF16),
                pltpu.VMEM((d_model, 2 * qkv_cols), BF16), pltpu.VMEM((2 * head_dim, d_model), BF16), pltpu.VMEM((2, d_model, ff // 2), BF16), pltpu.VMEM((2, ff // 2, d_model), BF16),
                pltpu.VMEM((3, 4, *seq_block), BF16), pltpu.VMEM((tile, d_model), BF16), pltpu.VMEM((tile, head_dim), BF16), pltpu.VMEM((tile, ff), BF16),
                pltpu.VMEM((2, 2 * seq_len, d_model), F32), pltpu.VMEM((2, 2 * seq_len, d_model), BF16), pltpu.VMEM((4, 2 * seq_len, d_model), BF16),
                pltpu.VMEM((steps, *seq_block), BF16), pltpu.VMEM((steps, *seq_block), BF16), pltpu.VMEM((2, nz, *seq_block), BF16),
                pltpu.VMEM((4, tile, d_model), BF16), pltpu.VMEM((4, tile, d_model), F32), pltpu.VMEM((2, 3, *seq_block), BF16),
                pltpu.VMEM((4, d_model, LANES), BF16), pltpu.VMEM((2, LANES, d_model), BF16),
                *sems("6 3 2 4"), dma((2,)), dma((2, (nz - 1) * (half - 1))), dma((2,)), dma((2, nz - 1, 2)),
                *sems("6 6 6"), dma((2, nz // 2, 6)), dma((nz + 1,)), *sems("4 2"), dma((3, 2)), *sems("2 2"), dma((2, 2)), *sems("4 2"),
            ],
            compiler_params=pltpu.CompilerParams(collective_id=1, has_side_effects=True, vmem_limit_bytes=63 * MIB),
        )(act_in, ln_gain, ln_bias, cos, sin, w_qkv, w_out, w_up, w_down)
        return pl.pallas_call(
            functools.partial(second_kernel, n_dp, n_tp),
            name="layer_two",
            out_shape=pltpu.VMEM(act_in.shape, BF16),
            in_specs=[any_spec] * 8,
            out_specs=vmem_spec,
            scratch_shapes=[
                pltpu.VMEM(cos.shape, F32), pltpu.VMEM(sin.shape, F32), pltpu.VMEM((per, *seq_block), BF16),
                pltpu.VMEM((d_model, 2 * qkv_cols), BF16), pltpu.VMEM((2 * head_dim, d_model), BF16), pltpu.VMEM((2, d_model, 2 * LANES), BF16), pltpu.VMEM((2, 2 * LANES, d_model), BF16),
                pltpu.VMEM((2, tile, d_model), BF16), pltpu.VMEM((2, tile, d_model), F32), pltpu.VMEM((2, *seq_block), F32), pltpu.VMEM((4, 3, *seq_block), BF16),
                dma((3, 2)), *sems("8 2 4 4"), dma((per,)), dma((2, per, nz // 2)), dma((per,)),
            ],
            compiler_params=pltpu.CompilerParams(collective_id=2, has_side_effects=True, vmem_limit_bytes=38 * MIB),
        )(done, nown, cos, sin, pout, pown, gcols, grows)

    return jax.shard_map(shard_body, mesh=mesh, in_specs=(P("dp"), P(), P(), P(None, None, "tp"), P(None, "tp"), P(None, None, "tp"), P(None, "tp")), out_specs=P("dp"), check_vma=False)
```

```python
import functools
import math

import jax
import jax.numpy as jnp
import numpy as np
from jax import lax
from jax.experimental import pallas as pl
from jax.experimental.pallas import tpu as pltpu
from jax.sharding import PartitionSpec as P

LN_EPS = 1e-5
ROPE_BASE = 10000.0
MESH = pl.DeviceIdType.MESH
BF16 = jnp.bfloat16
F32 = jnp.float32
LANES = 128
MIB = 1 << 20
SIDES = range(2)
PEERS = range(3)
UP, Q, K, V, DOWN, OUT = range(6)


def norm_rows(hidden_f, gain, bias):
    row_mean = jnp.mean(hidden_f, axis=-1, keepdims=True)
    centered = hidden_f - row_mean
    row_var = jnp.mean(centered * centered, axis=-1, keepdims=True)
    return (centered * lax.rsqrt(row_var + LN_EPS) * gain + bias).astype(BF16)


def rope(heads, cos, sin):
    return (heads * cos + pltpu.roll(heads, heads.shape[-1] // 2, 1) * sin).astype(BF16)


def gelu(values):
    return (0.5 * values * (1.0 + lax.erf(values * math.sqrt(0.5)))).astype(BF16)


def attend(query, keys, values, seq_len):
    rows, head_dim = query.shape
    block = 2 * seq_len
    row = lax.broadcasted_iota(jnp.int32, (block, block), 0)
    col = lax.broadcasted_iota(jnp.int32, (block, block), 1)
    allowed = (row >= col) & (row // seq_len == col // seq_len)
    contexts = []
    for first in range(0, rows, block):
        at = slice(first, first + block)
        scores = lax.dot_general(query[at], keys[at], (((1,), (1,)), ((), ())), preferred_element_type=F32) * (head_dim ** -0.5)
        scores = jnp.where(allowed, scores, -1e30)
        weights = jnp.exp(scores - jnp.max(scores, axis=-1, keepdims=True))
        probs = (weights / jnp.sum(weights, axis=-1, keepdims=True)).astype(BF16)
        contexts.append(jnp.dot(probs, values[at], preferred_element_type=F32).astype(BF16))
    return jnp.concatenate(contexts, axis=0)


def context_of(proj, cos_ref, sin_ref, seq_len):
    head_dim = cos_ref.shape[1]
    query = rope(proj[:, :head_dim], cos_ref[...], sin_ref[...])
    keys = rope(proj[:, head_dim : 2 * head_dim], cos_ref[...], sin_ref[...])
    return attend(query, keys, proj[:, 2 * head_dim :].astype(BF16), seq_len)


def head_context(normed, qkv_w, cos_ref, sin_ref, seq_len):
    return context_of(jnp.dot(normed, qkv_w, preferred_element_type=F32), cos_ref, sin_ref, seq_len)


class Place:
    def __init__(self, n_dp, n_tp):
        side = math.isqrt(n_dp)
        assert side * side == n_dp and side % 2 == 0 and n_tp % 4 == 0
        self.n_tp, self.nz = n_tp, n_tp // 2
        self.dp, self.tp = lax.axis_index("dp"), lax.axis_index("tp")
        self.z, self.core = self.tp // 2, self.tp % 2
        x, y = self.dp // side, self.dp % side
        xf, yf = x + 1 - 2 * (x % 2), y + 1 - 2 * (y % 2)
        self.q = (x % 2) * 2 + y % 2
        self.peers = [{"dp": xf * side + y}, {"dp": x * side + yf}, {"dp": xf * side + yf}]
        self.peer_q = [(1 - x % 2) * 2 + y % 2, (x % 2) * 2 + 1 - y % 2, (1 - x % 2) * 2 + 1 - y % 2]
        self.sib = {"tp": 2 * self.z + 1 - self.core}
        self.right = {"tp": 2 * ((self.z + 1) % self.nz) + self.core}
        self.left = {"tp": 2 * ((self.z + self.nz - 1) % self.nz) + self.core}

    def z_at(self, side, s):
        return (self.z + self.nz - s) % self.nz if side == 0 else (self.z + s) % self.nz

    def others(self):
        return [self.sib, self.right, self.left, *self.peers]

    def greet(self):
        barrier = pltpu.get_barrier_semaphore()
        for other in self.others():
            pl.semaphore_signal(barrier, inc=1, device_id=other, device_id_type=MESH)

    def meet(self):
        pl.semaphore_wait(pltpu.get_barrier_semaphore(), len(self.others()))


def remote(src, dst, send_sem, recv_sem, device):
    return pltpu.make_async_remote_copy(src_ref=src, dst_ref=dst, send_sem=send_sem, recv_sem=recv_sem, device_id=device, device_id_type=MESH)


def piece(kind, source, n_tp, cols, rows):
    if kind == UP:
        return cols.at[source]
    if kind == DOWN:
        return rows.at[source]
    head = source // 8 * 2 + source % 2
    if kind == OUT:
        return rows.at[n_tp + head]
    return cols.at[n_tp + 3 * head + kind - Q]


class SecondLayer:
    def __init__(self, place, nall, acc, qkv_v, out_v, up_v, down_v, gcols, grows, cos_ref, sin_ref, sem):
        self.place, self.nall, self.acc, self.sem = place, nall, acc, sem
        self.qkv_v, self.out_v, self.up_v, self.down_v = qkv_v, out_v, up_v, down_v
        self.gcols, self.grows, self.cos_ref, self.sin_ref = gcols, grows, cos_ref, sin_ref
        self.seq_len = nall.shape[1] // 4
        far = place.nz // 2
        self.order = [(0, 0)] + [(side, s) for s in range(1, far) for side in SIDES] + [(0, far)]

    def slab_loads(self, number):
        slot, zs = number % 2, self.place.z_at(*self.order[number])
        copies = []
        for c in SIDES:
            at = pl.ds(c * LANES, LANES)
            copies.append((self.gcols.at[2 * zs + c], self.up_v.at[slot, :, at], self.sem.at[slot, 0]))
            copies.append((self.grows.at[2 * zs + c], self.down_v.at[slot, at, :], self.sem.at[slot, 1]))
        return [pltpu.make_async_copy(*copy) for copy in copies]

    def head_loads(self, first):
        n_tp, head_dim = self.place.n_tp, self.cos_ref.shape[1]
        copies = []
        for n in SIDES:
            for i in range(3):
                at = pl.ds((3 * n + i) * head_dim, head_dim)
                copies.append((self.gcols.at[n_tp + 3 * (first + n) + i], self.qkv_v.at[:, at], self.sem.at[2, 0]))
            copies.append((self.grows.at[n_tp + first + n], self.out_v.at[pl.ds(n * head_dim, head_dim)], self.sem.at[2, 1]))
        return [pltpu.make_async_copy(*copy) for copy in copies]

    def wait_slab(self, number):
        slot = number % 2
        settle(self.up_v.at[slot], self.sem.at[slot, 0])
        settle(self.down_v.at[slot], self.sem.at[slot, 1])

    def wait_heads(self):
        settle(self.qkv_v, self.sem.at[2, 0])
        settle(self.out_v, self.sem.at[2, 1])

    def clear(self, tiles):
        for i in tiles:
            self.acc[i] = jnp.zeros(self.acc.shape[1:], F32)

    def slab(self, slot, p):
        nall, acc = self.nall, self.acc
        pair, kept = (2 * p, 2 * p + 1), acc.shape[0]
        hidden = [gelu(jnp.dot(nall[i], self.up_v[slot], preferred_element_type=F32)) for i in pair]
        step = 512
        for first in range(0, acc.shape[2], step):
            cols = pl.ds(first, step)
            for i, rows in zip(pair, hidden):
                acc[i % kept, :, cols] += jnp.dot(rows, self.down_v[slot, :, cols], preferred_element_type=F32)

    def heads(self, i):
        nall, acc, head_dim = self.nall, self.acc, self.cos_ref.shape[1]
        proj = jnp.dot(nall[i], self.qkv_v[...], preferred_element_type=F32)
        both = [context_of(proj[:, 3 * head_dim * n : 3 * head_dim * (n + 1)], self.cos_ref, self.sin_ref, self.seq_len) for n in SIDES]
        context = jnp.concatenate(both, axis=1)
        step = 512
        for first in range(0, acc.shape[2], step):
            cols = pl.ds(first, step)
            acc[i % acc.shape[0], :, cols] += jnp.dot(context, self.out_v[:, cols], preferred_element_type=F32)

    def round_off(self, i):
        self.nall[i] = self.acc[i % self.acc.shape[0]].astype(BF16)

    def run(self, program, actions, late_step=None):
        steps, events, late = [], [], None

        def end(unit):
            nonlocal events, late
            steps.append((events, late, unit))
            events, late = [], None

        for word in " ".join(program).split():
            letter, rest = word[0], word[1:]
            if letter in "SH":
                end([int(digit) for digit in rest])
                continue
            if late is not None:
                end([])
            if letter == "R":
                late = int(rest)
            else:
                events.append(functools.partial(actions[letter], rest))
        if events or late is not None:
            end([])

        def pick(values, default):
            def at(u):
                found = jnp.int32(default)
                for k, value in enumerate(values):
                    if value is not None:
                        found = jnp.where(u == k, value, found)
                return found
            return at

        late = pick([step[1] for step in steps], -1)
        slab = [step[2] if len(step[2]) == 2 else [None, None] for step in steps]
        slot = pick([number if number is None else number % 2 for number, _ in slab], -1)
        pair = pick([p for _, p in slab], 0)
        tile = pick([step[2][0] if len(step[2]) == 1 else None for step in steps], -1)

        def turn(u, carry):
            for k, step in enumerate(steps):
                if step[0]:
                    @pl.when(u == k)
                    def _():
                        for event in step[0]:
                            event()

            if late_step:
                @pl.when(late(u) >= 0)
                def _():
                    late_step(late(u))

            @pl.when(slot(u) >= 0)
            def _():
                self.slab(slot(u), pair(u))

            @pl.when(tile(u) >= 0)
            def _():
                self.heads(tile(u))

            return carry

        lax.fori_loop(0, len(steps), turn, 0)


def settle(ref, sem):
    pltpu.make_async_copy(ref, ref, sem).wait()


def start(copies):
    for copy in copies:
        copy.start()


def wait(copies):
    for copy in copies:
        copy.wait()


def kernel(n_dp, n_tp, x, gains_h, biases_h, cos_h, sin_h, qkv, out_w, up, down,
           out, gcols, grows,
           gains, biases, cos_ref, sin_ref, done, qkv_v, out_v, up_v, down_v, normed, ctx, act, own, nall, acc, part_in, st_cols, st_rows,
           w_sem, x_sem, sib_send, sib_recv, r_send, r_recv, e_send, e_recv,
           st_sem, loc_sem, w_send, wr_recv, ws_recv, n_send, n_recv, slab_sem, p_send, p_recv, small_sem, g_send, g_recv, s_recv):
    me = Place(n_dp, n_tp)
    me.greet()
    nz, core, z, q = me.nz, me.core, me.z, me.q
    n_seq, seq_len, d_model = x.shape
    head_dim, ff = out_w.shape[1], up.shape[2]
    per = n_seq // n_tp
    half = per // 2
    steps = nz * half

    wide = ff // 2
    assert (per, nz, n_tp // 4) == (6, 8, 4)

    def ring_at(side, i):
        s, j = i // half, i % half
        return jnp.where(j == half - 1, per * (2 * s + side) + j, per * s + half * side + j)

    def loc_at(side, s):
        return per * (2 * s + side) + per - 1

    def sib_in(i):
        return out.at[pl.ds(per * (nz + i % 4), 2)]

    def sib_out(i):
        return out.at[pl.ds(per * (nz + 4 + i % 2), 2)]

    def x_at(i, place):
        return per * (nz + 2 * (i % 3) + place // 2) + half + place % 2

    first_w = [pltpu.make_async_copy(src, dst, w_sem.at[i]) for i, (src, dst) in
               enumerate(((qkv.at[0], qkv_v.at[:, pl.ds(0, qkv.shape[2])]), (up.at[0, :, pl.ds(0, wide)], up_v.at[0]), (up.at[0, :, pl.ds(wide, wide)], up_v.at[1]),
                         (out_w.at[0], out_v.at[pl.ds(0, head_dim)]), (down.at[0, pl.ds(0, wide)], down_v.at[0]), (down.at[0, pl.ds(wide, wide)], down_v.at[1])))]

    def owner_seq(zo, co, j):
        return per * (2 * zo + co) + j

    def tile_seqs(i):
        s, j = i // half, i % half
        zr, zl = (z + 2 * nz - 1 - s) % nz, (z + 1 + s) % nz
        return [owner_seq(zr, core, j), owner_seq(zl, core, half + j), owner_seq(zr, 1 - core, j), owner_seq(zl, 1 - core, half + j)]

    def fetch(i):
        for place, seq in enumerate(tile_seqs(i)):
            pltpu.make_async_copy(x.at[seq], out.at[x_at(i, place)], x_sem.at[i % 3]).start()

    small = [pltpu.make_async_copy(src, dst, small_sem.at[i]) for i, (src, dst) in enumerate(((gains_h, gains), (biases_h, biases), (cos_h, cos_ref), (sin_h, sin_ref)))]
    loads = {UP: (up.at[1, :, pl.ds(pl.multiple_of(q * LANES, LANES), LANES)], st_cols.at[UP]),
             DOWN: (down.at[1, pl.ds(pl.multiple_of(q * LANES, LANES), LANES), :], st_rows.at[0]),
             OUT: (out_w.at[1], st_rows.at[1])}
    for kind in (Q, K, V):
        loads[kind] = (qkv.at[1, :, pl.ds((kind - Q) * head_dim, head_dim)], st_cols.at[kind])
    kinds = (Q, K, V, OUT, UP, DOWN)
    loads = {kind: pltpu.make_async_copy(*loads[kind], st_sem.at[kind]) for kind in kinds}

    loads[UP].start()
    fetch(0)
    start(small)
    start(first_w[:3])

    def start_rest():
        wait(small)
        start(first_w[3:])
        start([loads[kind] for kind in kinds if kind != UP])

    def has(kind, source):
        return source >= 0 if kind in (UP, DOWN) else (source // 2 + 2 * (source % 2)) % 4 == q

    def staged(kind):
        return st_rows.at[kind - DOWN] if kind >= DOWN else st_cols.at[kind]

    def piece_hops(kind):
        src, dst = staged(kind), piece(kind, me.tp, n_tp, gcols, grows)
        return [remote(src, dst, w_send.at[kind], wr_recv.at[0, 0, kind], me.right),
                remote(src, dst, w_send.at[kind], wr_recv.at[1, 0, kind], me.left),
                remote(src, dst, w_send.at[kind], sib_sem(z, kind), me.sib),
                pltpu.make_async_copy(src, dst, loc_sem.at[kind])]

    def sib_sem(zs, kind):
        return ws_recv.at[zs] if kind in (UP, DOWN) else ws_recv.at[nz]

    def send_first(kind):
        loads[kind].wait()

        @pl.when(has(kind, me.tp))
        def _():
            start(piece_hops(kind))

    for side in SIDES:
        for i in range(half):
            out[ring_at(side, i)] = jnp.zeros(out.shape[1:], BF16)

    to = (me.right, me.left)

    def send_sib(i):
        return remote(sib_out(i), sib_in(i), sib_send.at[i % 2], sib_recv.at[i % 4], me.sib)

    def send_ring(side, i):
        return remote(out.at[ring_at(side, i)], out.at[ring_at(side, i + half)], r_send.at[side], r_recv.at[side, i // half * (half - 1) + i % half], to[side])

    def rows_of(member):
        return pl.ds(pl.multiple_of(member * seq_len, seq_len), seq_len)

    def send_n(tile, peer):
        at = nall.at[tile, rows_of(q)]
        return remote(at, at, n_send.at[tile], n_recv.at[tile // 2], me.peers[peer])

    def compute(i, waits=(), then=None):
        slot = i % 3
        settle(out.at[pl.ds(0, 4)], x_sem.at[slot])
        if then:
            then()

        @pl.when(i + 1 < steps)
        def _():
            fetch(i + 1)

        @pl.when(i >= 2)
        def _():
            send_sib(i - 2).wait_send()

        for member in range(4):
            normed[pl.ds(member * seq_len, seq_len), :] = norm_rows(out[x_at(i, member)].astype(F32), gains[pl.ds(0, 1), :], biases[pl.ds(0, 1), :])
        wait(waits[:3])
        ctx[...] = head_context(normed[...], qkv_v[:, : 3 * head_dim], cos_ref, sin_ref, seq_len)
        for n in SIDES:
            act[:, n * wide : (n + 1) * wide] = gelu(jnp.dot(normed[...], up_v[n], preferred_element_type=F32))
        wait(waits[3:])
        step = 512
        for first in range(0, d_model, step):
            cols = pl.ds(first, step)
            part = jnp.dot(ctx[...], out_v[:head_dim, cols], preferred_element_type=F32)
            for n in SIDES:
                part += jnp.dot(act[:, n * wide : (n + 1) * wide], down_v[n, :, cols], preferred_element_type=F32)
            own[i % 2, :, cols] = part[: 2 * seq_len]
            for side in SIDES:
                sib_out(i)[side, :, cols] = part[(2 + side) * seq_len : (3 + side) * seq_len].astype(BF16)

    def finish(i):
        send_sib(i).wait_recv()
        late = i % half == half - 1
        last = i >= steps - half

        def local(side, at):
            return own[i % 2, pl.ds(side * seq_len + at.start, at.size), :] + sib_in(i)[side, at, :].astype(F32)

        whole = pl.ds(0, seq_len)

        @pl.when(late)
        def _():
            for side in SIDES:
                out[loc_at(side, i // half)] = local(side, whole).astype(BF16)

        @pl.when(late & last)
        def _():
            for side in SIDES:
                done[per - 2 + side] = out[x_at(i, side)]

        @pl.when((i >= half) & jnp.logical_not(late))
        def _():
            for side in SIDES:
                send_ring(side, i - half).wait_recv()

        @pl.when(jnp.logical_not(last | late))
        def _():
            for side in SIDES:
                at = ring_at(side, i)
                out[at] = (local(side, whole) + out[at].astype(F32)).astype(BF16)
            for side in SIDES:
                send_ring(side, i).start()

        @pl.when(i == steps - half - 2)
        def _():
            for kind in kinds:
                if kind != UP:
                    send_first(kind)

        @pl.when(last & jnp.logical_not(late))
        def _():
            rows = seq_len // 2
            for side in SIDES:
                tile = 2 * (i % half) + side
                for h in SIDES:
                    at = pl.ds(h * rows, rows)
                    update = (local(side, at) + out[ring_at(side, i), at, :].astype(F32)).astype(BF16)
                    close(tile, at, out[x_at(i, side), at, :], update)
                start_n(tile)

    def close(tile, at, hidden, update):
        hidden = (hidden.astype(F32) + update.astype(F32)).astype(BF16)
        done[tile, at, :] = hidden
        mine = pl.ds(pl.multiple_of(q * seq_len + at.start, at.size), at.size)
        nall[tile, mine, :] = norm_rows(hidden.astype(F32), gains[pl.ds(1, 1), :], biases[pl.ds(1, 1), :])

    def start_n(tile):
        for peer in PEERS:
            send_n(tile, peer).start()

    me.meet()
    send_first(UP)
    compute(0, first_w, start_rest)
    send_sib(0).start()

    def turn(i, carry):
        @pl.when(i < steps)
        def _():
            compute(i)
            send_sib(i).start()

        finish(i - 1)
        return carry

    lax.fori_loop(1, steps + 1, turn, 0)

    def hops(side, kind):
        longer = (core + (kind in (Q, V, DOWN))) % 2
        return nz // 2 - longer if side == 0 else nz // 2 - 1 + longer

    def source_of(side, s):
        return 2 * me.z_at(side, s) + core

    def onward(side, s, kind):
        at = piece(kind, source_of(side, s), n_tp, gcols, grows)
        return remote(at, at, w_send.at[kind], wr_recv.at[side, s, kind], to[side])

    def arrival(side, s, kind):
        at = piece(kind, source_of(side, s), n_tp, gcols, grows)
        return remote(at, at, w_send.at[kind], wr_recv.at[side, s - 1, kind], to[side])

    def across(side, s, kind):
        source = source_of(side, s)
        at = piece(kind, source, n_tp, gcols, grows)
        return remote(at, at, w_send.at[kind], sib_sem(source // 2, kind), me.sib)

    def take(side, s, kind):
        @pl.when(has(kind, source_of(side, s)) & (s <= hops(side, kind)))
        def _():
            arrival(side, s, kind).wait_recv()

            @pl.when(s < hops(side, kind))
            def _():
                onward(side, s, kind).start()

            across(side, s, kind).start()

    def take_both(s, kind):
        for side in SIDES:
            take(side, s, kind)

    cut = seq_len // 2

    def late_send(side, s, h):
        at, i = pl.ds(h * cut, cut), half * s + half - 1
        return remote(out.at[ring_at(side, i), at], out.at[ring_at(side, i + half), at], e_send.at[side], e_recv.at[side, s, h], to[side])

    def late_step(s):
        for h in SIDES:
            at, i = pl.ds(h * cut, cut), half * s + half - 1
            for side in SIDES:
                @pl.when(s > 0)
                def _():
                    late_send(side, s - 1, h).wait_recv()

                total = (out[loc_at(side, s), at, :].astype(F32) + out[ring_at(side, i), at, :].astype(F32)).astype(BF16)

                @pl.when(s < nz - 1)
                def _():
                    out[ring_at(side, i), at, :] = total

                @pl.when(s == nz - 1)
                def _():
                    tile = per - 2 + side
                    close(tile, at, done[tile, at, :], total)

            @pl.when(s < nz - 1)
            def _():
                for side in SIDES:
                    late_send(side, s, h).start()

    layer = SecondLayer(me, nall, acc, qkv_v, out_v, up_v, down_v, gcols, grows, cos_ref, sin_ref, slab_sem)

    def start_slab(number):
        settle(gcols.at[pl.ds(0, 2)], ws_recv.at[me.z_at(*layer.order[number])])
        if number == 0:
            for kind in (UP, DOWN):
                piece_hops(kind)[3].wait()
        start(layer.slab_loads(number))

    def await_pair(p):
        settle(nall.at[pl.ds(2 * p, 2), pl.ds(0, 3 * seq_len)], n_recv.at[p])

    def send_part(k, peer):
        return remote(nall.at[k, rows_of(me.peer_q[peer])], part_in.at[k, peer], p_send.at[k], p_recv.at[k], me.peers[peer])

    def start_parts(k):
        for peer in PEERS:
            send_part(k, peer).start()

    def hand_out(k):
        settle(nall.at[k, pl.ds(0, 3 * seq_len)], n_send.at[k])
        layer.round_off(k)
        if k not in (2, 3):
            start_parts(k)

    def summed(k):
        settle(part_in.at[k], p_recv.at[k])
        total = acc[k % acc.shape[0], rows_of(q), :]
        for peer in PEERS:
            total = total + part_in[k, peer].astype(F32)
        return (done[k].astype(F32) + total.astype(BF16).astype(F32)).astype(BF16)

    def seq_of(zs, co, k):
        return per * (2 * zs + co) + k % 2 * half + k // 2

    def first_hops(k):
        at = out.at[seq_of(z, core, k)]
        return [remote(at, at, g_send.at[k], g_recv.at[0, k, 0], me.right),
                remote(at, at, g_send.at[k], g_recv.at[1, k, 0], me.left),
                remote(at, at, g_send.at[k], s_recv.at[k], me.sib)]

    def reach(side, k):
        longer = (k + core) % 2
        return nz // 2 - longer if side == 0 else nz // 2 - 1 + longer

    def passing(side, k, s, hop):
        at = out.at[seq_of(me.z_at(side, s), core, k)]
        return remote(at, at, g_send.at[k], g_recv.at[side, k, hop], to[side])

    def stage(name):
        k, s = int(name[0]), int(name[1])
        if s == 0:
            out[seq_of(z, core, k)] = summed(k)
            start(first_hops(k))
            return
        for side in SIDES:
            @pl.when(s <= reach(side, k))
            def _():
                passing(side, k, s, s - 1).wait_recv()

                @pl.when(s < reach(side, k))
                def _():
                    passing(side, k, s, s).start()

                at = out.at[seq_of(me.z_at(side, s), core, k)]
                remote(at, at, g_send.at[k], s_recv.at[k], me.sib).start()

    def drain(k):
        settle(out.at[pl.ds(0, 2 * nz - 1)], g_send.at[k])
        settle(out.at[pl.ds(0, nz)], s_recv.at[k])

    def late_pair():
        for side in SIDES:
            start_n(per - 2 + side)
        start_parts(2)
        start_parts(3)
        for side in SIDES:
            settle(out.at[pl.ds(0, nz - 1)], e_send.at[side])

    def drain_rings():
        for side in SIDES:
            settle(out.at[pl.ds(0, (nz - 1) * (half - 1))], r_send.at[side])
        send_sib(steps - 2).wait_send()
        send_sib(steps - 1).wait_send()

    def drain_weights():
        for kind in kinds:
            sent = jnp.where(has(kind, me.tp), 3, 0)
            for s in range(1, nz // 2 + 1):
                for side in SIDES:
                    here = has(kind, source_of(side, s))
                    sent += jnp.where(here & (s <= hops(side, kind)), 1, 0) + jnp.where(here & (s < hops(side, kind)), 1, 0)
            for count in [2 * nz - 1] if kind in (UP, DOWN) else [3, 4]:
                @pl.when(sent == count)
                def _():
                    settle(gcols.at[pl.ds(0, count)], w_send.at[kind])

    attn = (Q, K, V, OUT)

    def own_heads_kept():
        for kind in attn:
            @pl.when(has(kind, me.tp))
            def _():
                piece_hops(kind)[3].wait()

        settle(gcols.at[pl.ds(0, 2 * len(attn))], ws_recv.at[nz])

    layer.clear(range(acc.shape[0]))
    actions = {
        "T": lambda rest: take_both(int(rest[0]), letters[rest[1]]),
        "N": lambda rest: await_pair(int(rest)),
        "L": lambda rest: start_slab(int(rest)),
        "M": lambda rest: start(layer.slab_loads(int(rest))),
        "W": lambda rest: layer.wait_slab(int(rest)),
        "A": lambda rest: own_heads_kept(),
        "X": lambda rest: start(layer.head_loads(int(rest))),
        "Y": lambda rest: layer.wait_heads(),
        "P": lambda rest: hand_out(int(rest)),
        "B": lambda rest: drain_rings(),
        "Z": lambda rest: drain_weights(),
        "G": stage,
        "E": lambda rest: late_pair(),
        "F": lambda rest: layer.clear(SIDES),
    }
    letters = {"U": UP, "D": DOWN, "Q": Q, "K": K, "V": V, "O": OUT}
    layer.run([
        "L0 T1K T2K T1V",
        "T1O T2V T2O T1Q",
        "T2Q T1D N0 T3V",
        "T1U N1 W0 S00",
        "L1 S01 L2 T3K",
        "B W1 S10 S11",
        "T3Q T3O T4O T2D",
        "T2U T4K L3 T4Q",
        "T4V W2 S20 A",
        "X0 S21 L4 Y",
        "H0 H1 H2 H3",
        "X2 R0 W3 S30",
        "T3U S31 T3D L5",
        "W4 S40 S41 L6",
        "R1 Y H0 H1",
        "W5 S50 T4D W6",
        "S60 T4U R2 L7",
        "W7 S70 P0 R3",
        "P1 H2 R4 H3",
        "R5 S71 R6 M5",
        "S61 W5 S51 P2",
        "P3 Z M0 M1",
        "X0 G00 R7 E",
        "G10 F G01 G11",
        "G02 N2 G12 W0",
        "S02 M2 W1 S12",
        "G03 M3 W2 S22",
        "M4 W3 S32 M5",
        "W4 S42 G13 Y",
        "H4 G04 G20 M6",
        "H5 X2 W5 S52",
        "G21 M7 W6 S62",
        "G14 W7 S72 G30",
        "Y H4 P4 H5",
        "G22 G31 P5",
    ], actions, late_step)
    early = 2
    for k in range(early):
        drain(k)
    for name in (*"40 32 50".split(), *"33 41 51".split()):
        stage(name)
    for k in range(per):
        settle(part_in.at[k], p_send.at[k])
    for name in (*"42 52 43 23".split(), *"34 53 24".split(), *"44 54".split()):
        stage(name)
    for k in range(early, per):
        drain(k)


def rope_rows(seq_len, head_dim, copies):
    inv_freq = ROPE_BASE ** (-2.0 * np.arange(head_dim // 2) / head_dim)
    angles = np.arange(seq_len)[:, None] * inv_freq[None, :]
    cos, sin = np.cos(angles), np.sin(angles)
    return [np.tile(np.concatenate(halves, 1), (copies, 1)).astype(np.float32) for halves in ((cos, cos), (-sin, sin))]


def solution(mesh):
    n_dp, n_tp = mesh.shape["dp"], mesh.shape["tp"]
    nz = n_tp // 2
    any_spec = pl.BlockSpec(memory_space=pl.ANY)
    vmem_spec = pl.BlockSpec(memory_space=pltpu.VMEM)
    dma = pltpu.SemaphoreType.DMA

    def sems(counts):
        return [dma((int(count),)) for count in counts.split()]

    def shard_body(act_in, ln_gain, ln_bias, w_qkv, w_out, w_up, w_down):
        n_seq, seq_len, d_model = act_in.shape
        layers, _, _, qkv_cols = w_qkv.shape
        head_dim, ff = w_out.shape[1], w_up.shape[2]
        per = n_seq // n_tp
        half = per // 2
        heads = n_tp // 4
        tile = 4 * seq_len
        w_qkv = w_qkv.reshape(layers, d_model, qkv_cols)
        cos, sin = rope_rows(seq_len, head_dim, 4)
        seq_block = (seq_len, d_model)
        n_cols, n_rows = n_tp + 3 * heads, n_tp + heads
        steps = nz * half
        return pl.pallas_call(
            functools.partial(kernel, n_dp, n_tp),
            name="two_layers",
            out_shape=(pltpu.VMEM(act_in.shape, BF16), jax.ShapeDtypeStruct((n_cols, d_model, LANES), BF16), jax.ShapeDtypeStruct((n_rows, LANES, d_model), BF16)),
            in_specs=[any_spec] * 9,
            out_specs=(vmem_spec, any_spec, any_spec),
            scratch_shapes=[
                pltpu.VMEM(ln_gain.shape, F32), pltpu.VMEM(ln_bias.shape, F32), pltpu.VMEM(cos.shape, F32), pltpu.VMEM(sin.shape, F32), pltpu.VMEM((per, *seq_block), BF16),
                pltpu.VMEM((d_model, 2 * qkv_cols), BF16), pltpu.VMEM((2 * head_dim, d_model), BF16), pltpu.VMEM((2, d_model, ff // 2), BF16), pltpu.VMEM((2, ff // 2, d_model), BF16),
                pltpu.VMEM((tile, d_model), BF16), pltpu.VMEM((tile, head_dim), BF16), pltpu.VMEM((tile, ff), BF16), pltpu.VMEM((2, 2 * seq_len, d_model), F32),
                pltpu.VMEM((per, tile, d_model), BF16), pltpu.VMEM((4, tile, d_model), F32), pltpu.VMEM((per, 3, *seq_block), BF16),
                pltpu.VMEM((4, d_model, LANES), BF16), pltpu.VMEM((2, LANES, d_model), BF16),
                *sems("6 3 2 4"), dma((2,)), dma((2, (nz - 1) * (half - 1))), dma((2,)), dma((2, nz - 1, 2)),
                *sems("6 6 6"), dma((2, nz // 2, 6)), dma((nz + 1,)), *sems("6 3"), dma((3, 2)), *sems("6 6 4 6"), dma((2, per, nz // 2)), dma((per,)),
            ],
            compiler_params=pltpu.CompilerParams(collective_id=1, has_side_effects=True, vmem_limit_bytes=39 * MIB),
        )(act_in, ln_gain, ln_bias, cos, sin, w_qkv, w_out, w_up, w_down)[0]

    return jax.shard_map(shard_body, mesh=mesh, in_specs=(P("dp"), P(), P(), P(None, None, "tp"), P(None, "tp"), P(None, None, "tp"), P(None, "tp")), out_specs=P("dp"), check_vma=False)
```

```python
import functools
import math

import jax
import jax.numpy as jnp
import numpy as np
from jax import lax
from jax.experimental import pallas as pl
from jax.experimental.pallas import tpu as pltpu
from jax.sharding import PartitionSpec as P

LN_EPS = 1e-5
ROPE_BASE = 10000.0
MESH = pl.DeviceIdType.MESH
BF16 = jnp.bfloat16
F32 = jnp.float32
LANES = 128
MIB = 1 << 20
SIDES = range(2)
PEERS = range(3)
UP, Q, K, V, DOWN, OUT = range(6)


def norm_rows(hidden_f, gain, bias):
    row_mean = jnp.mean(hidden_f, axis=-1, keepdims=True)
    centered = hidden_f - row_mean
    row_var = jnp.mean(centered * centered, axis=-1, keepdims=True)
    return (centered * lax.rsqrt(row_var + LN_EPS) * gain + bias).astype(BF16)


def rope(heads, cos, sin):
    return (heads * cos + pltpu.roll(heads, heads.shape[-1] // 2, 1) * sin).astype(BF16)


def gelu(values):
    return (0.5 * values * (1.0 + lax.erf(values * math.sqrt(0.5)))).astype(BF16)


def attend(query, keys, values, seq_len):
    rows, head_dim = query.shape
    block = 2 * seq_len
    row = lax.broadcasted_iota(jnp.int32, (block, block), 0)
    col = lax.broadcasted_iota(jnp.int32, (block, block), 1)
    allowed = (row >= col) & (row // seq_len == col // seq_len)
    contexts = []
    for first in range(0, rows, block):
        at = slice(first, first + block)
        scores = lax.dot_general(query[at], keys[at], (((1,), (1,)), ((), ())), preferred_element_type=F32) * (head_dim ** -0.5)
        scores = jnp.where(allowed, scores, -1e30)
        weights = jnp.exp(scores - jnp.max(scores, axis=-1, keepdims=True))
        probs = (weights / jnp.sum(weights, axis=-1, keepdims=True)).astype(BF16)
        contexts.append(jnp.dot(probs, values[at], preferred_element_type=F32).astype(BF16))
    return jnp.concatenate(contexts, axis=0)


def context_of(proj, cos_ref, sin_ref, seq_len):
    head_dim = cos_ref.shape[1]
    query = rope(proj[:, :head_dim], cos_ref[...], sin_ref[...])
    keys = rope(proj[:, head_dim : 2 * head_dim], cos_ref[...], sin_ref[...])
    return attend(query, keys, proj[:, 2 * head_dim :].astype(BF16), seq_len)


def head_context(normed, qkv_w, cos_ref, sin_ref, seq_len):
    return context_of(jnp.dot(normed, qkv_w, preferred_element_type=F32), cos_ref, sin_ref, seq_len)


class Place:
    def __init__(self, n_dp, n_tp):
        side = math.isqrt(n_dp)
        assert side * side == n_dp and side % 2 == 0 and n_tp % 4 == 0
        self.n_tp, self.nz = n_tp, n_tp // 2
        self.dp, self.tp = lax.axis_index("dp"), lax.axis_index("tp")
        self.z, self.core = self.tp // 2, self.tp % 2
        x, y = self.dp // side, self.dp % side
        xf, yf = x + 1 - 2 * (x % 2), y + 1 - 2 * (y % 2)
        self.q = (x % 2) * 2 + y % 2
        self.peers = [{"dp": xf * side + y}, {"dp": x * side + yf}, {"dp": xf * side + yf}]
        self.peer_q = [(1 - x % 2) * 2 + y % 2, (x % 2) * 2 + 1 - y % 2, (1 - x % 2) * 2 + 1 - y % 2]
        self.sib = {"tp": 2 * self.z + 1 - self.core}
        self.right = {"tp": 2 * ((self.z + 1) % self.nz) + self.core}
        self.left = {"tp": 2 * ((self.z + self.nz - 1) % self.nz) + self.core}

    def z_at(self, side, s):
        return (self.z + self.nz - s) % self.nz if side == 0 else (self.z + s) % self.nz

    def others(self):
        return [self.sib, self.right, self.left, *self.peers]

    def greet(self):
        barrier = pltpu.get_barrier_semaphore()
        for other in self.others():
            pl.semaphore_signal(barrier, inc=1, device_id=other, device_id_type=MESH)

    def meet(self):
        pl.semaphore_wait(pltpu.get_barrier_semaphore(), len(self.others()))


def remote(src, dst, send_sem, recv_sem, device):
    return pltpu.make_async_remote_copy(src_ref=src, dst_ref=dst, send_sem=send_sem, recv_sem=recv_sem, device_id=device, device_id_type=MESH)


def piece(kind, source, n_tp, cols, rows):
    if kind == UP:
        return cols.at[source]
    if kind == DOWN:
        return rows.at[source]
    head = source // 8 * 2 + source % 2
    if kind == OUT:
        return rows.at[n_tp + head]
    return cols.at[n_tp + 3 * head + kind - Q]


class SecondLayer:
    def __init__(self, place, nall, acc, qkv_v, out_v, up_v, down_v, gcols, grows, cos_ref, sin_ref, sem):
        self.place, self.nall, self.acc, self.sem = place, nall, acc, sem
        self.qkv_v, self.out_v, self.up_v, self.down_v = qkv_v, out_v, up_v, down_v
        self.gcols, self.grows, self.cos_ref, self.sin_ref = gcols, grows, cos_ref, sin_ref
        self.seq_len = nall.shape[1] // 4
        far = place.nz // 2
        self.order = [(0, 0)] + [(side, s) for s in range(1, far) for side in SIDES] + [(0, far)]

    def slab_loads(self, number):
        slot, zs = number % 2, self.place.z_at(*self.order[number])
        copies = []
        for c in SIDES:
            at = pl.ds(c * LANES, LANES)
            copies.append((self.gcols.at[2 * zs + c], self.up_v.at[slot, :, at], self.sem.at[slot, 0]))
            copies.append((self.grows.at[2 * zs + c], self.down_v.at[slot, at, :], self.sem.at[slot, 1]))
        return [pltpu.make_async_copy(*copy) for copy in copies]

    def head_loads(self, first):
        n_tp, head_dim = self.place.n_tp, self.cos_ref.shape[1]
        copies = []
        for n in SIDES:
            for i in range(3):
                at = pl.ds((3 * n + i) * head_dim, head_dim)
                copies.append((self.gcols.at[n_tp + 3 * (first + n) + i], self.qkv_v.at[:, at], self.sem.at[2, 0]))
            copies.append((self.grows.at[n_tp + first + n], self.out_v.at[pl.ds(n * head_dim, head_dim)], self.sem.at[2, 1]))
        return [pltpu.make_async_copy(*copy) for copy in copies]

    def wait_slab(self, number):
        slot = number % 2
        settle(self.up_v.at[slot], self.sem.at[slot, 0])
        settle(self.down_v.at[slot], self.sem.at[slot, 1])

    def wait_heads(self):
        settle(self.qkv_v, self.sem.at[2, 0])
        settle(self.out_v, self.sem.at[2, 1])

    def clear(self, tiles):
        for i in tiles:
            self.acc[i] = jnp.zeros(self.acc.shape[1:], F32)

    def slab(self, slot, p):
        nall, acc = self.nall, self.acc
        pair, kept = (2 * p, 2 * p + 1), acc.shape[0]
        hidden = [gelu(jnp.dot(nall[i], self.up_v[slot], preferred_element_type=F32)) for i in pair]
        step = 512
        for first in range(0, acc.shape[2], step):
            cols = pl.ds(first, step)
            for i, rows in zip(pair, hidden):
                acc[i % kept, :, cols] += jnp.dot(rows, self.down_v[slot, :, cols], preferred_element_type=F32)

    def heads(self, i):
        nall, acc, head_dim = self.nall, self.acc, self.cos_ref.shape[1]
        proj = jnp.dot(nall[i], self.qkv_v[...], preferred_element_type=F32)
        both = [context_of(proj[:, 3 * head_dim * n : 3 * head_dim * (n + 1)], self.cos_ref, self.sin_ref, self.seq_len) for n in SIDES]
        context = jnp.concatenate(both, axis=1)
        step = 512
        for first in range(0, acc.shape[2], step):
            cols = pl.ds(first, step)
            acc[i % acc.shape[0], :, cols] += jnp.dot(context, self.out_v[:, cols], preferred_element_type=F32)

    def round_off(self, i):
        self.nall[i] = self.acc[i % self.acc.shape[0]].astype(BF16)

    def run(self, program, actions, late_step=None):
        steps, events, late = [], [], None

        def end(unit):
            nonlocal events, late
            steps.append((events, late, unit))
            events, late = [], None

        for word in " ".join(program).split():
            letter, rest = word[0], word[1:]
            if letter in "SH":
                end([int(digit) for digit in rest])
                continue
            if late is not None:
                end([])
            if letter == "R":
                late = int(rest)
            else:
                events.append(functools.partial(actions[letter], rest))
        if events or late is not None:
            end([])

        def pick(values, default):
            def at(u):
                found = jnp.int32(default)
                for k, value in enumerate(values):
                    if value is not None:
                        found = jnp.where(u == k, value, found)
                return found
            return at

        late = pick([step[1] for step in steps], -1)
        slab = [step[2] if len(step[2]) == 2 else [None, None] for step in steps]
        slot = pick([number if number is None else number % 2 for number, _ in slab], -1)
        pair = pick([p for _, p in slab], 0)
        tile = pick([step[2][0] if len(step[2]) == 1 else None for step in steps], -1)

        def turn(u, carry):
            for k, step in enumerate(steps):
                if step[0]:
                    @pl.when(u == k)
                    def _():
                        for event in step[0]:
                            event()

            if late_step:
                @pl.when(late(u) >= 0)
                def _():
                    late_step(late(u))

            @pl.when(slot(u) >= 0)
            def _():
                self.slab(slot(u), pair(u))

            @pl.when(tile(u) >= 0)
            def _():
                self.heads(tile(u))

            return carry

        lax.fori_loop(0, len(steps), turn, 0)


def settle(ref, sem):
    pltpu.make_async_copy(ref, ref, sem).wait()


def start(copies):
    for copy in copies:
        copy.start()


def wait(copies):
    for copy in copies:
        copy.wait()


def kernel(n_dp, n_tp, x, gains_h, biases_h, cos_h, sin_h, qkv, out_w, up, down,
           out, gcols, grows,
           gains, biases, cos_ref, sin_ref, done, qkv_v, out_v, up_v, down_v, normed, ctx, act, own, nall, acc, part_in, st_cols, st_rows,
           w_sem, x_sem, sib_send, sib_recv, r_send, r_recv, e_send, e_recv,
           st_sem, loc_sem, w_send, wr_recv, ws_recv, n_send, n_recv, slab_sem, p_send, p_recv, small_sem, g_send, g_recv, s_recv):
    me = Place(n_dp, n_tp)
    me.greet()
    nz, core, z, q = me.nz, me.core, me.z, me.q
    n_seq, seq_len, d_model = x.shape
    head_dim, ff = out_w.shape[1], up.shape[2]
    per = n_seq // n_tp
    half = per // 2
    steps = nz * half

    wide = ff // 2
    assert (per, nz, n_tp // 4) == (6, 8, 4)

    def ring_at(side, i):
        s, j = i // half, i % half
        return jnp.where(j == half - 1, per * (2 * s + side) + j, per * s + half * side + j)

    def loc_at(side, s):
        return per * (2 * s + side) + per - 1

    def sib_in(i):
        return out.at[pl.ds(per * (nz + i % 4), 2)]

    def sib_out(i):
        return out.at[pl.ds(per * (nz + 4 + i % 2), 2)]

    def x_at(i, place):
        return per * (nz + 2 * (i % 3) + place // 2) + half + place % 2

    first_w = [pltpu.make_async_copy(src, dst, w_sem.at[i]) for i, (src, dst) in
               enumerate(((qkv.at[0], qkv_v.at[:, pl.ds(0, qkv.shape[2])]), (up.at[0, :, pl.ds(0, wide)], up_v.at[0]), (up.at[0, :, pl.ds(wide, wide)], up_v.at[1]),
                         (out_w.at[0], out_v.at[pl.ds(0, head_dim)]), (down.at[0, pl.ds(0, wide)], down_v.at[0]), (down.at[0, pl.ds(wide, wide)], down_v.at[1])))]

    def owner_seq(zo, co, j):
        return per * (2 * zo + co) + j

    def tile_seqs(i):
        s, j = i // half, i % half
        zr, zl = (z + 2 * nz - 1 - s) % nz, (z + 1 + s) % nz
        return [owner_seq(zr, core, j), owner_seq(zl, core, half + j), owner_seq(zr, 1 - core, j), owner_seq(zl, 1 - core, half + j)]

    def fetch(i):
        for place, seq in enumerate(tile_seqs(i)):
            pltpu.make_async_copy(x.at[seq], out.at[x_at(i, place)], x_sem.at[i % 3]).start()

    small = [pltpu.make_async_copy(src, dst, small_sem.at[i]) for i, (src, dst) in enumerate(((gains_h, gains), (biases_h, biases), (cos_h, cos_ref), (sin_h, sin_ref)))]
    loads = {UP: (up.at[1, :, pl.ds(pl.multiple_of(q * LANES, LANES), LANES)], st_cols.at[UP]),
             DOWN: (down.at[1, pl.ds(pl.multiple_of(q * LANES, LANES), LANES), :], st_rows.at[0]),
             OUT: (out_w.at[1], st_rows.at[1])}
    for kind in (Q, K, V):
        loads[kind] = (qkv.at[1, :, pl.ds((kind - Q) * head_dim, head_dim)], st_cols.at[kind])
    kinds = (Q, K, V, OUT, UP, DOWN)
    loads = {kind: pltpu.make_async_copy(*loads[kind], st_sem.at[kind]) for kind in kinds}

    loads[UP].start()
    fetch(0)
    start(small)
    start(first_w[:3])

    def start_rest():
        wait(small)
        start(first_w[3:])
        start([loads[kind] for kind in kinds if kind != UP])

    def has(kind, source):
        return source >= 0 if kind in (UP, DOWN) else (source // 2 + 2 * (source % 2)) % 4 == q

    def staged(kind):
        return st_rows.at[kind - DOWN] if kind >= DOWN else st_cols.at[kind]

    def piece_hops(kind):
        src, dst = staged(kind), piece(kind, me.tp, n_tp, gcols, grows)
        return [remote(src, dst, w_send.at[kind], wr_recv.at[0, 0, kind], me.right),
                remote(src, dst, w_send.at[kind], wr_recv.at[1, 0, kind], me.left),
                remote(src, dst, w_send.at[kind], sib_sem(z, kind), me.sib),
                pltpu.make_async_copy(src, dst, loc_sem.at[kind])]

    def sib_sem(zs, kind):
        return ws_recv.at[zs] if kind in (UP, DOWN) else ws_recv.at[nz]

    def send_first(kind):
        loads[kind].wait()

        @pl.when(has(kind, me.tp))
        def _():
            start(piece_hops(kind))

    for side in SIDES:
        for i in range(half):
            out[ring_at(side, i)] = jnp.zeros(out.shape[1:], BF16)

    to = (me.right, me.left)

    def send_sib(i):
        return remote(sib_out(i), sib_in(i), sib_send.at[i % 2], sib_recv.at[i % 4], me.sib)

    def send_ring(side, i):
        return remote(out.at[ring_at(side, i)], out.at[ring_at(side, i + half)], r_send.at[side], r_recv.at[side, i // half * (half - 1) + i % half], to[side])

    def rows_of(member):
        return pl.ds(pl.multiple_of(member * seq_len, seq_len), seq_len)

    def rows_sem(tile):
        return n_recv.at[tile - 2] if isinstance(tile, int) and tile >= per - 2 else n_recv.at[tile // 2]

    def send_n(tile, peer):
        at = nall.at[tile, rows_of(q)]
        return remote(at, at, n_send.at[tile], rows_sem(tile), me.peers[peer])

    def compute(i, waits=(), then=None):
        slot = i % 3
        settle(out.at[pl.ds(0, 4)], x_sem.at[slot])
        if then:
            then()

        @pl.when(i + 1 < steps)
        def _():
            fetch(i + 1)

        @pl.when(i >= 2)
        def _():
            send_sib(i - 2).wait_send()

        for member in range(4):
            normed[pl.ds(member * seq_len, seq_len), :] = norm_rows(out[x_at(i, member)].astype(F32), gains[pl.ds(0, 1), :], biases[pl.ds(0, 1), :])
        wait(waits[:3])
        ctx[...] = head_context(normed[...], qkv_v[:, : 3 * head_dim], cos_ref, sin_ref, seq_len)
        for n in SIDES:
            act[:, n * wide : (n + 1) * wide] = gelu(jnp.dot(normed[...], up_v[n], preferred_element_type=F32))
        wait(waits[3:])
        step = 512
        for first in range(0, d_model, step):
            cols = pl.ds(first, step)
            part = jnp.dot(ctx[...], out_v[:head_dim, cols], preferred_element_type=F32)
            for n in SIDES:
                part += jnp.dot(act[:, n * wide : (n + 1) * wide], down_v[n, :, cols], preferred_element_type=F32)
            own[i % 2, :, cols] = part[: 2 * seq_len]
            for side in SIDES:
                sib_out(i)[side, :, cols] = part[(2 + side) * seq_len : (3 + side) * seq_len].astype(BF16)

    def finish(i):
        send_sib(i).wait_recv()
        late = i % half == half - 1
        last = i >= steps - half

        def local(side, at):
            return own[i % 2, pl.ds(side * seq_len + at.start, at.size), :] + sib_in(i)[side, at, :].astype(F32)

        whole = pl.ds(0, seq_len)

        @pl.when(late)
        def _():
            for side in SIDES:
                out[loc_at(side, i // half)] = local(side, whole).astype(BF16)

        @pl.when(late & last)
        def _():
            for side in SIDES:
                done[per - 2 + side] = out[x_at(i, side)]

        @pl.when((i >= half) & jnp.logical_not(late))
        def _():
            for side in SIDES:
                send_ring(side, i - half).wait_recv()

        @pl.when(jnp.logical_not(last | late))
        def _():
            for side in SIDES:
                at = ring_at(side, i)
                out[at] = (local(side, whole) + out[at].astype(F32)).astype(BF16)
            for side in SIDES:
                send_ring(side, i).start()

        @pl.when(i == steps - half - 2)
        def _():
            for kind in kinds:
                if kind != UP:
                    send_first(kind)

        @pl.when(last & jnp.logical_not(late))
        def _():
            rows = seq_len // 2
            for side in SIDES:
                tile = 2 * (i % half) + side
                for h in SIDES:
                    at = pl.ds(h * rows, rows)
                    update = (local(side, at) + out[ring_at(side, i), at, :].astype(F32)).astype(BF16)
                    close(tile, at, out[x_at(i, side), at, :], update)
                start_n(tile)

    def close(tile, at, hidden, update):
        hidden = (hidden.astype(F32) + update.astype(F32)).astype(BF16)
        done[tile, at, :] = hidden
        mine = pl.ds(pl.multiple_of(q * seq_len + at.start, at.size), at.size)
        nall[tile, mine, :] = norm_rows(hidden.astype(F32), gains[pl.ds(1, 1), :], biases[pl.ds(1, 1), :])

    def start_n(tile):
        for peer in PEERS:
            send_n(tile, peer).start()

    me.meet()
    send_first(UP)
    compute(0, first_w, start_rest)
    send_sib(0).start()

    def turn(i, carry):
        @pl.when(i < steps)
        def _():
            compute(i)
            send_sib(i).start()

        finish(i - 1)
        return carry

    lax.fori_loop(1, steps + 1, turn, 0)

    def hops(side, kind):
        longer = (core + (kind in (Q, V, DOWN))) % 2
        return nz // 2 - longer if side == 0 else nz // 2 - 1 + longer

    def source_of(side, s):
        return 2 * me.z_at(side, s) + core

    def onward(side, s, kind):
        at = piece(kind, source_of(side, s), n_tp, gcols, grows)
        return remote(at, at, w_send.at[kind], wr_recv.at[side, s, kind], to[side])

    def arrival(side, s, kind):
        at = piece(kind, source_of(side, s), n_tp, gcols, grows)
        return remote(at, at, w_send.at[kind], wr_recv.at[side, s - 1, kind], to[side])

    def across(side, s, kind):
        source = source_of(side, s)
        at = piece(kind, source, n_tp, gcols, grows)
        return remote(at, at, w_send.at[kind], sib_sem(source // 2, kind), me.sib)

    def take(side, s, kind):
        @pl.when(has(kind, source_of(side, s)) & (s <= hops(side, kind)))
        def _():
            arrival(side, s, kind).wait_recv()

            @pl.when(s < hops(side, kind))
            def _():
                onward(side, s, kind).start()

            across(side, s, kind).start()

    def take_both(s, kind):
        for side in SIDES:
            take(side, s, kind)

    cut = seq_len // 2

    def late_send(side, s, h):
        at, i = pl.ds(h * cut, cut), half * s + half - 1
        return remote(out.at[ring_at(side, i), at], out.at[ring_at(side, i + half), at], e_send.at[side], e_recv.at[side, s, h], to[side])

    def late_step(s):
        for h in SIDES:
            at, i = pl.ds(h * cut, cut), half * s + half - 1
            for side in SIDES:
                @pl.when(s > 0)
                def _():
                    late_send(side, s - 1, h).wait_recv()

                total = (out[loc_at(side, s), at, :].astype(F32) + out[ring_at(side, i), at, :].astype(F32)).astype(BF16)

                @pl.when(s < nz - 1)
                def _():
                    out[ring_at(side, i), at, :] = total

                @pl.when(s == nz - 1)
                def _():
                    tile = per - 2 + side
                    close(tile, at, done[tile, at, :], total)

            @pl.when(s < nz - 1)
            def _():
                for side in SIDES:
                    late_send(side, s, h).start()

    layer = SecondLayer(me, nall, acc, qkv_v, out_v, up_v, down_v, gcols, grows, cos_ref, sin_ref, slab_sem)

    def start_slab(number):
        settle(gcols.at[pl.ds(0, 2)], ws_recv.at[me.z_at(*layer.order[number])])
        if number == 0:
            for kind in (UP, DOWN):
                piece_hops(kind)[3].wait()
        start(layer.slab_loads(number))

    def await_rows(which):
        if which < 2:
            settle(nall.at[pl.ds(2 * which, 2), pl.ds(0, 3 * seq_len)], n_recv.at[which])
        else:
            settle(nall.at[which, pl.ds(0, 3 * seq_len)], n_recv.at[which - 2])

    def send_part(k, peer):
        return remote(nall.at[k, rows_of(me.peer_q[peer])], part_in.at[k, peer], p_send.at[k], p_recv.at[k], me.peers[peer])

    def start_parts(k):
        for peer in PEERS:
            send_part(k, peer).start()

    def hand_out(k):
        settle(nall.at[k, pl.ds(0, 3 * seq_len)], n_send.at[k])
        layer.round_off(k)
        if k not in (2, 3):
            start_parts(k)

    def summed(k):
        settle(part_in.at[k], p_recv.at[k])
        total = acc[k % acc.shape[0], rows_of(q), :]
        for peer in PEERS:
            total = total + part_in[k, peer].astype(F32)
        return (done[k].astype(F32) + total.astype(BF16).astype(F32)).astype(BF16)

    def seq_of(zs, co, k):
        return per * (2 * zs + co) + k % 2 * half + k // 2

    def first_hops(k):
        at = out.at[seq_of(z, core, k)]
        return [remote(at, at, g_send.at[k], g_recv.at[0, k, 0], me.right),
                remote(at, at, g_send.at[k], g_recv.at[1, k, 0], me.left),
                remote(at, at, g_send.at[k], s_recv.at[k], me.sib)]

    def reach(side, k):
        longer = (k + core) % 2
        return nz // 2 - longer if side == 0 else nz // 2 - 1 + longer

    def passing(side, k, s, hop):
        at = out.at[seq_of(me.z_at(side, s), core, k)]
        return remote(at, at, g_send.at[k], g_recv.at[side, k, hop], to[side])

    def stage(name):
        k, s = int(name[0]), int(name[1])
        if s == 0:
            out[seq_of(z, core, k)] = summed(k)
            start(first_hops(k))
            return
        for side in SIDES:
            @pl.when(s <= reach(side, k))
            def _():
                passing(side, k, s, s - 1).wait_recv()

                @pl.when(s < reach(side, k))
                def _():
                    passing(side, k, s, s).start()

                at = out.at[seq_of(me.z_at(side, s), core, k)]
                remote(at, at, g_send.at[k], s_recv.at[k], me.sib).start()

    def drain(k):
        settle(out.at[pl.ds(0, 2 * nz - 1)], g_send.at[k])
        settle(out.at[pl.ds(0, nz)], s_recv.at[k])

    def late_pair():
        start_parts(2)
        for side in SIDES:
            start_n(per - 2 + side)
        start_parts(3)
        for side in SIDES:
            settle(out.at[pl.ds(0, nz - 1)], e_send.at[side])

    def drain_rings():
        for side in SIDES:
            settle(out.at[pl.ds(0, (nz - 1) * (half - 1))], r_send.at[side])
        send_sib(steps - 2).wait_send()
        send_sib(steps - 1).wait_send()

    def drain_weights():
        for kind in kinds:
            sent = jnp.where(has(kind, me.tp), 3, 0)
            for s in range(1, nz // 2 + 1):
                for side in SIDES:
                    here = has(kind, source_of(side, s))
                    sent += jnp.where(here & (s <= hops(side, kind)), 1, 0) + jnp.where(here & (s < hops(side, kind)), 1, 0)
            for count in [2 * nz - 1] if kind in (UP, DOWN) else [3, 4]:
                @pl.when(sent == count)
                def _():
                    settle(gcols.at[pl.ds(0, count)], w_send.at[kind])

    attn = (Q, K, V, OUT)

    def own_heads_kept():
        for kind in attn:
            @pl.when(has(kind, me.tp))
            def _():
                piece_hops(kind)[3].wait()

        settle(gcols.at[pl.ds(0, 2 * len(attn))], ws_recv.at[nz])

    layer.clear(range(acc.shape[0]))
    actions = {
        "T": lambda rest: take_both(int(rest[0]), letters[rest[1]]),
        "N": lambda rest: await_rows(int(rest)),
        "L": lambda rest: start_slab(int(rest)),
        "M": lambda rest: start(layer.slab_loads(int(rest))),
        "W": lambda rest: layer.wait_slab(int(rest)),
        "A": lambda rest: own_heads_kept(),
        "X": lambda rest: start(layer.head_loads(int(rest))),
        "Y": lambda rest: layer.wait_heads(),
        "P": lambda rest: hand_out(int(rest)),
        "B": lambda rest: drain_rings(),
        "Z": lambda rest: drain_weights(),
        "G": stage,
        "E": lambda rest: late_pair(),
        "F": lambda rest: layer.clear(SIDES),
    }
    letters = {"U": UP, "D": DOWN, "Q": Q, "K": K, "V": V, "O": OUT}
    layer.run([
        "L0 T1K T2K T1V",
        "T1O T2V T2O T1Q",
        "T2Q T1D N0 T3V",
        "T1U N1 W0 S00",
        "L1 S01 L2 T3K",
        "B W1 S10 S11",
        "T3Q T3O T4O T2D",
        "T2U T4K L3 T4Q",
        "T4V W2 S20 A",
        "X0 S21 L4 Y",
        "H0 H1 H2 H3",
        "X2 R0 W3 S30",
        "T3U S31 T3D L5",
        "W4 S40 S41 L6",
        "R1 Y H0 H1",
        "W5 S50 T4D W6",
        "S60 T4U R2 L7",
        "W7 S70 P0 R3",
        "P1 H2 R4 H3",
        "R5 S71 R6 M5",
        "S61 W5 S51 P2",
        "P3 Z M0 M1",
        "X0 G00 R7 E",
        "G10 F G01 G20",
        "G11 G02 G12 N4",
        "G21 Y H4 G03",
        "N5 H5 X2 W0",
        "S02 M2 G13 W1",
        "S12 M3 W2 S22",
        "M4 W3 S32 M5",
        "G22 W4 S42 M6",
        "W5 S52 M7 W6",
        "S62 W7 S72 G30",
        "Y H4 P4 G23",
        "G31 H5 G14 P5",
    ], actions, late_step)
    for name in "04 24".split():
        stage(name)
    early = 2
    for k in range(early):
        drain(k)
    for name in (*"40 32 50".split(), *"41 51 33".split()):
        stage(name)
    for k in range(per):
        settle(part_in.at[k], p_send.at[k])
    for name in (*"52 42 53".split(), *"43 44 34 54".split()):
        stage(name)
    for k in range(early, per):
        drain(k)


def rope_rows(seq_len, head_dim, copies):
    inv_freq = ROPE_BASE ** (-2.0 * np.arange(head_dim // 2) / head_dim)
    angles = np.arange(seq_len)[:, None] * inv_freq[None, :]
    cos, sin = np.cos(angles), np.sin(angles)
    return [np.tile(np.concatenate(halves, 1), (copies, 1)).astype(np.float32) for halves in ((cos, cos), (-sin, sin))]


def solution(mesh):
    n_dp, n_tp = mesh.shape["dp"], mesh.shape["tp"]
    nz = n_tp // 2
    any_spec = pl.BlockSpec(memory_space=pl.ANY)
    vmem_spec = pl.BlockSpec(memory_space=pltpu.VMEM)
    dma = pltpu.SemaphoreType.DMA

    def sems(counts):
        return [dma((int(count),)) for count in counts.split()]

    def shard_body(act_in, ln_gain, ln_bias, w_qkv, w_out, w_up, w_down):
        n_seq, seq_len, d_model = act_in.shape
        layers, _, _, qkv_cols = w_qkv.shape
        head_dim, ff = w_out.shape[1], w_up.shape[2]
        per = n_seq // n_tp
        half = per // 2
        heads = n_tp // 4
        tile = 4 * seq_len
        w_qkv = w_qkv.reshape(layers, d_model, qkv_cols)
        cos, sin = rope_rows(seq_len, head_dim, 4)
        seq_block = (seq_len, d_model)
        n_cols, n_rows = n_tp + 3 * heads, n_tp + heads
        steps = nz * half
        return pl.pallas_call(
            functools.partial(kernel, n_dp, n_tp),
            name="two_layers",
            out_shape=(pltpu.VMEM(act_in.shape, BF16), jax.ShapeDtypeStruct((n_cols, d_model, LANES), BF16), jax.ShapeDtypeStruct((n_rows, LANES, d_model), BF16)),
            in_specs=[any_spec] * 9,
            out_specs=(vmem_spec, any_spec, any_spec),
            scratch_shapes=[
                pltpu.VMEM(ln_gain.shape, F32), pltpu.VMEM(ln_bias.shape, F32), pltpu.VMEM(cos.shape, F32), pltpu.VMEM(sin.shape, F32), pltpu.VMEM((per, *seq_block), BF16),
                pltpu.VMEM((d_model, 2 * qkv_cols), BF16), pltpu.VMEM((2 * head_dim, d_model), BF16), pltpu.VMEM((2, d_model, ff // 2), BF16), pltpu.VMEM((2, ff // 2, d_model), BF16),
                pltpu.VMEM((tile, d_model), BF16), pltpu.VMEM((tile, head_dim), BF16), pltpu.VMEM((tile, ff), BF16), pltpu.VMEM((2, 2 * seq_len, d_model), F32),
                pltpu.VMEM((per, tile, d_model), BF16), pltpu.VMEM((4, tile, d_model), F32), pltpu.VMEM((per, 3, *seq_block), BF16),
                pltpu.VMEM((4, d_model, LANES), BF16), pltpu.VMEM((2, LANES, d_model), BF16),
                *sems("6 3 2 4"), dma((2,)), dma((2, (nz - 1) * (half - 1))), dma((2,)), dma((2, nz - 1, 2)),
                *sems("6 6 6"), dma((2, nz // 2, 6)), dma((nz + 1,)), *sems("6 4"), dma((3, 2)), *sems("6 6 4 6"), dma((2, per, nz // 2)), dma((per,)),
            ],
            compiler_params=pltpu.CompilerParams(collective_id=1, has_side_effects=True, vmem_limit_bytes=39 * MIB),
        )(act_in, ln_gain, ln_bias, cos, sin, w_qkv, w_out, w_up, w_down)[0]

    return jax.shard_map(shard_body, mesh=mesh, in_specs=(P("dp"), P(), P(), P(None, None, "tp"), P(None, "tp"), P(None, None, "tp"), P(None, "tp")), out_specs=P("dp"), check_vma=False)
```

```python
import functools
import math

import jax
import jax.numpy as jnp
import numpy as np
from jax import lax
from jax.experimental import pallas as pl
from jax.experimental.pallas import tpu as pltpu
from jax.sharding import PartitionSpec as P

LN_EPS = 1e-5
ROPE_BASE = 10000.0
MESH = pl.DeviceIdType.MESH
BF16 = jnp.bfloat16
F32 = jnp.float32
LANES = 128
MIB = 1 << 20
SIDES = range(2)
PEERS = range(3)
UP, Q, K, V, DOWN, OUT = range(6)


def norm_rows(hidden_f, gain, bias):
    row_mean = jnp.mean(hidden_f, axis=-1, keepdims=True)
    centered = hidden_f - row_mean
    row_var = jnp.mean(centered * centered, axis=-1, keepdims=True)
    return (centered * lax.rsqrt(row_var + LN_EPS) * gain + bias).astype(BF16)


def rope(heads, cos, sin):
    return (heads * cos + pltpu.roll(heads, heads.shape[-1] // 2, 1) * sin).astype(BF16)


def gelu(values):
    return (0.5 * values * (1.0 + lax.erf(values * math.sqrt(0.5)))).astype(BF16)


def attend(query, keys, values, seq_len):
    rows, head_dim = query.shape
    block = 2 * seq_len
    row = lax.broadcasted_iota(jnp.int32, (block, block), 0)
    col = lax.broadcasted_iota(jnp.int32, (block, block), 1)
    allowed = (row >= col) & (row // seq_len == col // seq_len)
    contexts = []
    for first in range(0, rows, block):
        at = slice(first, first + block)
        scores = lax.dot_general(query[at], keys[at], (((1,), (1,)), ((), ())), preferred_element_type=F32) * (head_dim ** -0.5)
        scores = jnp.where(allowed, scores, -1e30)
        weights = jnp.exp(scores - jnp.max(scores, axis=-1, keepdims=True))
        probs = (weights / jnp.sum(weights, axis=-1, keepdims=True)).astype(BF16)
        contexts.append(jnp.dot(probs, values[at], preferred_element_type=F32).astype(BF16))
    return jnp.concatenate(contexts, axis=0)


def context_of(proj, cos_ref, sin_ref, seq_len):
    head_dim = cos_ref.shape[1]
    query = rope(proj[:, :head_dim], cos_ref[...], sin_ref[...])
    keys = rope(proj[:, head_dim : 2 * head_dim], cos_ref[...], sin_ref[...])
    return attend(query, keys, proj[:, 2 * head_dim :].astype(BF16), seq_len)


def head_context(normed, qkv_w, cos_ref, sin_ref, seq_len):
    return context_of(jnp.dot(normed, qkv_w, preferred_element_type=F32), cos_ref, sin_ref, seq_len)


class Place:
    def __init__(self, n_dp, n_tp):
        side = math.isqrt(n_dp)
        assert side * side == n_dp and side % 2 == 0 and n_tp % 4 == 0
        self.n_tp, self.nz = n_tp, n_tp // 2
        self.dp, self.tp = lax.axis_index("dp"), lax.axis_index("tp")
        self.z, self.core = self.tp // 2, self.tp % 2
        x, y = self.dp // side, self.dp % side
        xf, yf = x + 1 - 2 * (x % 2), y + 1 - 2 * (y % 2)
        self.q = (x % 2) * 2 + y % 2
        self.peers = [{"dp": xf * side + y}, {"dp": x * side + yf}, {"dp": xf * side + yf}]
        self.peer_q = [(1 - x % 2) * 2 + y % 2, (x % 2) * 2 + 1 - y % 2, (1 - x % 2) * 2 + 1 - y % 2]
        self.sib = {"tp": 2 * self.z + 1 - self.core}
        self.right = {"tp": 2 * ((self.z + 1) % self.nz) + self.core}
        self.left = {"tp": 2 * ((self.z + self.nz - 1) % self.nz) + self.core}

    def z_at(self, side, s):
        return (self.z + self.nz - s) % self.nz if side == 0 else (self.z + s) % self.nz

    def others(self):
        return [self.sib, self.right, self.left, *self.peers]

    def greet(self):
        barrier = pltpu.get_barrier_semaphore()
        for other in self.others():
            pl.semaphore_signal(barrier, inc=1, device_id=other, device_id_type=MESH)

    def meet(self):
        pl.semaphore_wait(pltpu.get_barrier_semaphore(), len(self.others()))


def remote(src, dst, send_sem, recv_sem, device):
    return pltpu.make_async_remote_copy(src_ref=src, dst_ref=dst, send_sem=send_sem, recv_sem=recv_sem, device_id=device, device_id_type=MESH)


def piece(kind, source, n_tp, cols, rows):
    if kind == UP:
        return cols.at[source]
    if kind == DOWN:
        return rows.at[source]
    head = source // 8 * 2 + source % 2
    if kind == OUT:
        return rows.at[n_tp + head]
    return cols.at[n_tp + 3 * head + kind - Q]


class SecondLayer:
    def __init__(self, place, nall, acc, qkv_v, out_v, up_v, down_v, gcols, grows, cos_ref, sin_ref, sem):
        self.place, self.nall, self.acc, self.sem = place, nall, acc, sem
        self.qkv_v, self.out_v, self.up_v, self.down_v = qkv_v, out_v, up_v, down_v
        self.gcols, self.grows, self.cos_ref, self.sin_ref = gcols, grows, cos_ref, sin_ref
        self.seq_len = nall.shape[1] // 4
        far = place.nz // 2
        self.order = [(0, 0)] + [(side, s) for s in range(1, far) for side in SIDES] + [(0, far)]

    def slab_loads(self, number):
        slot, zs = number % 2, self.place.z_at(*self.order[number])
        copies = []
        for c in SIDES:
            at = pl.ds(c * LANES, LANES)
            copies.append((self.gcols.at[2 * zs + c], self.up_v.at[slot, :, at], self.sem.at[slot, 0]))
            copies.append((self.grows.at[2 * zs + c], self.down_v.at[slot, at, :], self.sem.at[slot, 1]))
        return [pltpu.make_async_copy(*copy) for copy in copies]

    def head_loads(self, first):
        n_tp, head_dim = self.place.n_tp, self.cos_ref.shape[1]
        copies = []
        for n in SIDES:
            for i in range(3):
                at = pl.ds((3 * n + i) * head_dim, head_dim)
                copies.append((self.gcols.at[n_tp + 3 * (first + n) + i], self.qkv_v.at[:, at], self.sem.at[2, 0]))
            copies.append((self.grows.at[n_tp + first + n], self.out_v.at[pl.ds(n * head_dim, head_dim)], self.sem.at[2, 1]))
        return [pltpu.make_async_copy(*copy) for copy in copies]

    def wait_slab(self, number):
        slot = number % 2
        settle(self.up_v.at[slot], self.sem.at[slot, 0])
        settle(self.down_v.at[slot], self.sem.at[slot, 1])

    def wait_heads(self):
        settle(self.qkv_v, self.sem.at[2, 0])
        settle(self.out_v, self.sem.at[2, 1])

    def clear(self, tiles):
        for i in tiles:
            self.acc[i] = jnp.zeros(self.acc.shape[1:], F32)

    def slab(self, slot, p):
        nall, acc = self.nall, self.acc
        pair, kept = (2 * p, 2 * p + 1), acc.shape[0]
        hidden = [gelu(jnp.dot(nall[i], self.up_v[slot], preferred_element_type=F32)) for i in pair]
        step = 512
        for first in range(0, acc.shape[2], step):
            cols = pl.ds(first, step)
            for i, rows in zip(pair, hidden):
                acc[i % kept, :, cols] += jnp.dot(rows, self.down_v[slot, :, cols], preferred_element_type=F32)

    def heads(self, i):
        nall, acc, head_dim = self.nall, self.acc, self.cos_ref.shape[1]
        proj = jnp.dot(nall[i], self.qkv_v[...], preferred_element_type=F32)
        both = [context_of(proj[:, 3 * head_dim * n : 3 * head_dim * (n + 1)], self.cos_ref, self.sin_ref, self.seq_len) for n in SIDES]
        context = jnp.concatenate(both, axis=1)
        step = 512
        for first in range(0, acc.shape[2], step):
            cols = pl.ds(first, step)
            acc[i % acc.shape[0], :, cols] += jnp.dot(context, self.out_v[:, cols], preferred_element_type=F32)

    def round_off(self, i):
        self.nall[i] = self.acc[i % self.acc.shape[0]].astype(BF16)

    def run(self, program, actions, late_step=None):
        steps, events, late = [], [], None

        def end(unit):
            nonlocal events, late
            steps.append((events, late, unit))
            events, late = [], None

        for word in " ".join(program).split():
            letter, rest = word[0], word[1:]
            if letter in "SH":
                end([int(digit) for digit in rest])
                continue
            if late is not None:
                end([])
            if letter == "R":
                late = int(rest)
            else:
                events.append(functools.partial(actions[letter], rest))
        if events or late is not None:
            end([])

        def pick(values, default):
            def at(u):
                found = jnp.int32(default)
                for k, value in enumerate(values):
                    if value is not None:
                        found = jnp.where(u == k, value, found)
                return found
            return at

        late = pick([step[1] for step in steps], -1)
        slab = [step[2] if len(step[2]) == 2 else [None, None] for step in steps]
        slot = pick([number if number is None else number % 2 for number, _ in slab], -1)
        pair = pick([p for _, p in slab], 0)
        tile = pick([step[2][0] if len(step[2]) == 1 else None for step in steps], -1)

        def turn(u, carry):
            for k, step in enumerate(steps):
                if step[0]:
                    @pl.when(u == k)
                    def _():
                        for event in step[0]:
                            event()

            if late_step:
                @pl.when(late(u) >= 0)
                def _():
                    late_step(late(u))

            @pl.when(slot(u) >= 0)
            def _():
                self.slab(slot(u), pair(u))

            @pl.when(tile(u) >= 0)
            def _():
                self.heads(tile(u))

            return carry

        lax.fori_loop(0, len(steps), turn, 0)


def settle(ref, sem):
    pltpu.make_async_copy(ref, ref, sem).wait()


def start(copies):
    for copy in copies:
        copy.start()


def wait(copies):
    for copy in copies:
        copy.wait()


def kernel(n_dp, n_tp, x, gains_h, biases_h, cos_h, sin_h, qkv, out_w, up, down,
           out, gcols, grows,
           gains, biases, cos_ref, sin_ref, done, qkv_v, out_v, up_v, down_v, normed, ctx, act, own, nall, acc, part_in, st_cols, st_rows,
           w_sem, x_sem, sib_send, sib_recv, r_send, r_recv, e_send,
           st_sem, loc_sem, w_send, wr_recv, ws_recv, n_send, n_recv, slab_sem, p_send, p_recv, small_sem, g_send, s_recv):
    me = Place(n_dp, n_tp)
    me.greet()
    nz, core, z, q = me.nz, me.core, me.z, me.q
    n_seq, seq_len, d_model = x.shape
    head_dim, ff = out_w.shape[1], up.shape[2]
    per = n_seq // n_tp
    half = per // 2
    steps = nz * half

    wide = ff // 2
    assert (per, nz, n_tp // 4) == (6, 8, 4)

    def ring_at(side, i):
        s, j = i // half, i % half
        return jnp.where(j == half - 1, per * (2 * s + side) + j, per * s + half * side + j)

    def loc_at(side, s):
        return per * (2 * s + side) + per - 1

    def sib_in(i):
        return out.at[pl.ds(per * (nz + i % 4), 2)]

    def sib_out(i):
        return out.at[pl.ds(per * (nz + 4 + i % 2), 2)]

    def x_at(i, place):
        return per * (nz + 2 * (i % 3) + place // 2) + half + place % 2

    first_w = [pltpu.make_async_copy(src, dst, w_sem.at[i]) for i, (src, dst) in
               enumerate(((qkv.at[0], qkv_v.at[:, pl.ds(0, qkv.shape[2])]), (up.at[0, :, pl.ds(0, wide)], up_v.at[0]), (up.at[0, :, pl.ds(wide, wide)], up_v.at[1]),
                         (out_w.at[0], out_v.at[pl.ds(0, head_dim)]), (down.at[0, pl.ds(0, wide)], down_v.at[0]), (down.at[0, pl.ds(wide, wide)], down_v.at[1])))]

    def owner_seq(zo, co, j):
        return per * (2 * zo + co) + j

    def tile_seqs(i):
        s, j = i // half, i % half
        zr, zl = (z + 2 * nz - 1 - s) % nz, (z + 1 + s) % nz
        return [owner_seq(zr, core, j), owner_seq(zl, core, half + j), owner_seq(zr, 1 - core, j), owner_seq(zl, 1 - core, half + j)]

    def fetch(i):
        for place, seq in enumerate(tile_seqs(i)):
            pltpu.make_async_copy(x.at[seq], out.at[x_at(i, place)], x_sem.at[i % 3]).start()

    small = [pltpu.make_async_copy(src, dst, small_sem.at[i]) for i, (src, dst) in enumerate(((gains_h, gains), (biases_h, biases), (cos_h, cos_ref), (sin_h, sin_ref)))]
    loads = {UP: (up.at[1, :, pl.ds(pl.multiple_of(q * LANES, LANES), LANES)], st_cols.at[UP]),
             DOWN: (down.at[1, pl.ds(pl.multiple_of(q * LANES, LANES), LANES), :], st_rows.at[0]),
             OUT: (out_w.at[1], st_rows.at[1])}
    for kind in (Q, K, V):
        loads[kind] = (qkv.at[1, :, pl.ds((kind - Q) * head_dim, head_dim)], st_cols.at[kind])
    kinds = (Q, K, V, OUT, UP, DOWN)
    loads = {kind: pltpu.make_async_copy(*loads[kind], st_sem.at[kind]) for kind in kinds}

    loads[UP].start()
    fetch(0)
    start(small)
    start(first_w[:3])

    def start_rest():
        wait(small)
        start(first_w[3:])
        start([loads[kind] for kind in kinds if kind != UP])

    def has(kind, source):
        return source >= 0 if kind in (UP, DOWN) else (source // 2 + 2 * (source % 2)) % 4 == q

    def staged(kind):
        return st_rows.at[kind - DOWN] if kind >= DOWN else st_cols.at[kind]

    def piece_hops(kind):
        src, dst = staged(kind), piece(kind, me.tp, n_tp, gcols, grows)
        return [remote(src, dst, w_send.at[kind], wr_recv.at[0, 0, kind], me.right),
                remote(src, dst, w_send.at[kind], wr_recv.at[1, 0, kind], me.left),
                remote(src, dst, w_send.at[kind], sib_sem(z, kind), me.sib),
                pltpu.make_async_copy(src, dst, loc_sem.at[kind])]

    def sib_sem(zs, kind):
        return ws_recv.at[zs] if kind in (UP, DOWN) else ws_recv.at[nz]

    def send_first(kind):
        loads[kind].wait()

        @pl.when(has(kind, me.tp))
        def _():
            start(piece_hops(kind))

    for side in SIDES:
        for i in range(half):
            out[ring_at(side, i)] = jnp.zeros(out.shape[1:], BF16)

    to = (me.right, me.left)

    def send_sib(i):
        return remote(sib_out(i), sib_in(i), sib_send.at[i % 2], sib_recv.at[i % 4], me.sib)

    def send_ring(side, i):
        return remote(out.at[ring_at(side, i)], out.at[ring_at(side, i + half)], r_send.at[side], r_recv.at[side, i // half * (half - 1) + i % half], to[side])

    def rows_of(member):
        return pl.ds(pl.multiple_of(member * seq_len, seq_len), seq_len)

    def rows_sem(tile):
        return n_recv.at[tile - 2] if isinstance(tile, int) and tile >= per - 2 else n_recv.at[tile // 2]

    def send_n(tile, peer):
        at = nall.at[tile, rows_of(q)]
        return remote(at, at, n_send.at[tile], rows_sem(tile), me.peers[peer])

    def compute(i, waits=(), then=None):
        slot = i % 3
        settle(out.at[pl.ds(0, 4)], x_sem.at[slot])
        if then:
            then()

        @pl.when(i + 1 < steps)
        def _():
            fetch(i + 1)

        @pl.when(i >= 2)
        def _():
            send_sib(i - 2).wait_send()

        for member in range(4):
            normed[pl.ds(member * seq_len, seq_len), :] = norm_rows(out[x_at(i, member)].astype(F32), gains[pl.ds(0, 1), :], biases[pl.ds(0, 1), :])
        wait(waits[:3])
        ctx[...] = head_context(normed[...], qkv_v[:, : 3 * head_dim], cos_ref, sin_ref, seq_len)
        for n in SIDES:
            act[:, n * wide : (n + 1) * wide] = gelu(jnp.dot(normed[...], up_v[n], preferred_element_type=F32))
        wait(waits[3:])
        step = 512
        for first in range(0, d_model, step):
            cols = pl.ds(first, step)
            part = jnp.dot(ctx[...], out_v[:head_dim, cols], preferred_element_type=F32)
            for n in SIDES:
                part += jnp.dot(act[:, n * wide : (n + 1) * wide], down_v[n, :, cols], preferred_element_type=F32)
            own[i % 2, :, cols] = part[: 2 * seq_len]
            for side in SIDES:
                sib_out(i)[side, :, cols] = part[(2 + side) * seq_len : (3 + side) * seq_len].astype(BF16)

    def finish(i):
        send_sib(i).wait_recv()
        late = i % half == half - 1
        last = i >= steps - half

        def local(side, at):
            return own[i % 2, pl.ds(side * seq_len + at.start, at.size), :] + sib_in(i)[side, at, :].astype(F32)

        whole = pl.ds(0, seq_len)

        @pl.when(late)
        def _():
            for side in SIDES:
                out[loc_at(side, i // half)] = local(side, whole).astype(BF16)

        @pl.when(late & last)
        def _():
            for side in SIDES:
                done[per - 2 + side] = out[x_at(i, side)]

        @pl.when((i >= half) & jnp.logical_not(late))
        def _():
            for side in SIDES:
                send_ring(side, i - half).wait_recv()

        @pl.when(jnp.logical_not(last | late))
        def _():
            for side in SIDES:
                at = ring_at(side, i)
                out[at] = (local(side, whole) + out[at].astype(F32)).astype(BF16)
            for side in SIDES:
                send_ring(side, i).start()

        @pl.when(i == steps - half - 2)
        def _():
            for kind in kinds:
                if kind != UP:
                    send_first(kind)

        @pl.when(last & jnp.logical_not(late))
        def _():
            rows = seq_len // 2
            for side in SIDES:
                tile = 2 * (i % half) + side
                for h in SIDES:
                    at = pl.ds(h * rows, rows)
                    update = (local(side, at) + out[ring_at(side, i), at, :].astype(F32)).astype(BF16)
                    close(tile, at, out[x_at(i, side), at, :], update)
                start_n(tile)

    def close(tile, at, hidden, update):
        hidden = (hidden.astype(F32) + update.astype(F32)).astype(BF16)
        done[tile, at, :] = hidden
        mine = pl.ds(pl.multiple_of(q * seq_len + at.start, at.size), at.size)
        nall[tile, mine, :] = norm_rows(hidden.astype(F32), gains[pl.ds(1, 1), :], biases[pl.ds(1, 1), :])

    def start_n(tile):
        for peer in PEERS:
            send_n(tile, peer).start()

    me.meet()
    send_first(UP)
    compute(0, first_w, start_rest)
    send_sib(0).start()

    def turn(i, carry):
        @pl.when(i < steps)
        def _():
            compute(i)
            send_sib(i).start()

        finish(i - 1)
        return carry

    lax.fori_loop(1, steps + 1, turn, 0)

    def hops(side, kind):
        longer = (core + (kind in (Q, V, DOWN))) % 2
        return nz // 2 - longer if side == 0 else nz // 2 - 1 + longer

    def source_of(side, s):
        return 2 * me.z_at(side, s) + core

    def onward(side, s, kind):
        at = piece(kind, source_of(side, s), n_tp, gcols, grows)
        return remote(at, at, w_send.at[kind], wr_recv.at[side, s, kind], to[side])

    def arrival(side, s, kind):
        at = piece(kind, source_of(side, s), n_tp, gcols, grows)
        return remote(at, at, w_send.at[kind], wr_recv.at[side, s - 1, kind], to[side])

    def across(side, s, kind):
        source = source_of(side, s)
        at = piece(kind, source, n_tp, gcols, grows)
        return remote(at, at, w_send.at[kind], sib_sem(source // 2, kind), me.sib)

    def take(side, s, kind):
        @pl.when(has(kind, source_of(side, s)) & (s <= hops(side, kind)))
        def _():
            arrival(side, s, kind).wait_recv()

            @pl.when(s < hops(side, kind))
            def _():
                onward(side, s, kind).start()

            across(side, s, kind).start()

    def take_both(s, kind):
        for side in SIDES:
            take(side, s, kind)

    cut = seq_len // 2

    def late_send(side, s, h):
        at, i = pl.ds(h * cut, cut), half * s + half - 1
        return remote(out.at[ring_at(side, i), at], out.at[ring_at(side, i + half), at], e_send.at[side], r_recv.at[side, 2 * s + h], to[side])

    def late_step(s):
        for h in SIDES:
            at, i = pl.ds(h * cut, cut), half * s + half - 1
            for side in SIDES:
                @pl.when(s > 0)
                def _():
                    late_send(side, s - 1, h).wait_recv()

                total = (out[loc_at(side, s), at, :].astype(F32) + out[ring_at(side, i), at, :].astype(F32)).astype(BF16)

                @pl.when(s < nz - 1)
                def _():
                    out[ring_at(side, i), at, :] = total

                @pl.when(s == nz - 1)
                def _():
                    tile = per - 2 + side
                    close(tile, at, done[tile, at, :], total)

            @pl.when(s < nz - 1)
            def _():
                for side in SIDES:
                    late_send(side, s, h).start()

    layer = SecondLayer(me, nall, acc, qkv_v, out_v, up_v, down_v, gcols, grows, cos_ref, sin_ref, slab_sem)

    def start_slab(number):
        settle(gcols.at[pl.ds(0, 2)], ws_recv.at[me.z_at(*layer.order[number])])
        if number == 0:
            for kind in (UP, DOWN):
                piece_hops(kind)[3].wait()
        start(layer.slab_loads(number))

    def await_rows(which):
        if which < 2:
            settle(nall.at[pl.ds(2 * which, 2), pl.ds(0, 3 * seq_len)], n_recv.at[which])
        else:
            settle(nall.at[which, pl.ds(0, 3 * seq_len)], n_recv.at[which - 2])

    def send_part(k, peer):
        return remote(nall.at[k, rows_of(me.peer_q[peer])], part_in.at[k, peer], p_send.at[k], p_recv.at[k], me.peers[peer])

    def start_parts(k):
        for peer in PEERS:
            send_part(k, peer).start()

    def hand_out(k):
        settle(nall.at[k, pl.ds(0, 3 * seq_len)], n_send.at[k])
        layer.round_off(k)
        if k not in (2, 3):
            start_parts(k)

    def summed(k):
        settle(part_in.at[k], p_recv.at[k])
        total = acc[k % acc.shape[0], rows_of(q), :]
        for peer in PEERS:
            total = total + part_in[k, peer].astype(F32)
        return (done[k].astype(F32) + total.astype(BF16).astype(F32)).astype(BF16)

    def seq_of(zs, co, k):
        return per * (2 * zs + co) + k % 2 * half + k // 2

    def first_hops(k):
        at = out.at[seq_of(z, core, k)]
        return [remote(at, at, g_send.at[k], wr_recv.at[0, 0, k], me.right),
                remote(at, at, g_send.at[k], wr_recv.at[1, 0, k], me.left),
                remote(at, at, g_send.at[k], s_recv.at[k], me.sib)]

    def reach(side, k):
        longer = (k + core) % 2
        return nz // 2 - longer if side == 0 else nz // 2 - 1 + longer

    def passing(side, k, s, hop):
        at = out.at[seq_of(me.z_at(side, s), core, k)]
        return remote(at, at, g_send.at[k], wr_recv.at[side, hop, k], to[side])

    def stage(name):
        k, s = int(name[0]), int(name[1])
        if s == 0:
            out[seq_of(z, core, k)] = summed(k)
            start(first_hops(k))
            return
        for side in SIDES:
            @pl.when(s <= reach(side, k))
            def _():
                passing(side, k, s, s - 1).wait_recv()

                @pl.when(s < reach(side, k))
                def _():
                    passing(side, k, s, s).start()

                at = out.at[seq_of(me.z_at(side, s), core, k)]
                remote(at, at, g_send.at[k], s_recv.at[k], me.sib).start()

    def drain(k):
        settle(out.at[pl.ds(0, 2 * nz - 1)], g_send.at[k])
        settle(out.at[pl.ds(0, nz)], s_recv.at[k])

    def late_pair():
        start_parts(2)
        for side in SIDES:
            start_n(per - 2 + side)
        start_parts(3)
        for side in SIDES:
            settle(out.at[pl.ds(0, nz - 1)], e_send.at[side])

    def drain_rings():
        for side in SIDES:
            settle(out.at[pl.ds(0, (nz - 1) * (half - 1))], r_send.at[side])
        send_sib(steps - 2).wait_send()
        send_sib(steps - 1).wait_send()

    def drain_weights():
        for kind in kinds:
            sent = jnp.where(has(kind, me.tp), 3, 0)
            for s in range(1, nz // 2 + 1):
                for side in SIDES:
                    here = has(kind, source_of(side, s))
                    sent += jnp.where(here & (s <= hops(side, kind)), 1, 0) + jnp.where(here & (s < hops(side, kind)), 1, 0)
            for count in [2 * nz - 1] if kind in (UP, DOWN) else [3, 4]:
                @pl.when(sent == count)
                def _():
                    settle(gcols.at[pl.ds(0, count)], w_send.at[kind])

    attn = (Q, K, V, OUT)

    def own_heads_kept():
        for kind in attn:
            @pl.when(has(kind, me.tp))
            def _():
                piece_hops(kind)[3].wait()

        settle(gcols.at[pl.ds(0, 2 * len(attn))], ws_recv.at[nz])

    layer.clear(range(acc.shape[0]))
    actions = {
        "T": lambda rest: take_both(int(rest[0]), letters[rest[1]]),
        "N": lambda rest: await_rows(int(rest)),
        "L": lambda rest: start_slab(int(rest)),
        "M": lambda rest: start(layer.slab_loads(int(rest))),
        "W": lambda rest: layer.wait_slab(int(rest)),
        "A": lambda rest: own_heads_kept(),
        "X": lambda rest: start(layer.head_loads(int(rest))),
        "Y": lambda rest: layer.wait_heads(),
        "P": lambda rest: hand_out(int(rest)),
        "B": lambda rest: drain_rings(),
        "Z": lambda rest: drain_weights(),
        "G": stage,
        "E": lambda rest: late_pair(),
        "F": lambda rest: layer.clear(SIDES),
    }
    letters = {"U": UP, "D": DOWN, "Q": Q, "K": K, "V": V, "O": OUT}
    layer.run([
        "L0 T1K T2K T1V",
        "T1O T2V T2O T1Q",
        "T2Q T1D N0 T3V",
        "T1U N1 W0 S00",
        "L1 S01 L2 T3K",
        "B W1 S10 S11",
        "T3Q T3O T4O T2D",
        "T2U T4K L3 T4Q",
        "T4V W2 S20 A",
        "X0 S21 L4 Y",
        "H0 H1 H2 H3",
        "X2 R0 W3 S30",
        "T3U S31 T3D L5",
        "W4 S40 S41 L6",
        "R1 Y H0 H1",
        "W5 S50 T4D W6",
        "S60 T4U R2 L7",
        "W7 S70 P0 R3",
        "P1 H2 R4 H3",
        "R5 S71 R6 M5",
        "S61 W5 S51 P2",
        "P3 Z M0 M1",
        "X0 G00 R7 E",
        "G10 F G01 G20",
        "G11 G02 G12 N4",
        "G21 Y H4 G03",
        "N5 H5 X2 W0",
        "S02 M2 G13 W1",
        "S12 M3 W2 S22",
        "M4 W3 S32 M5",
        "G22 W4 S42 M6",
        "W5 S52 M7 W6",
        "S62 W7 S72 G30",
        "Y H4 P4 G23",
        "G31 H5 G14 P5",
    ], actions, late_step)
    for name in "04 24".split():
        stage(name)
    early = 2
    for k in range(early):
        drain(k)
    for name in (*"40 32 50".split(), *"41 51 33".split()):
        stage(name)
    for k in range(per):
        settle(part_in.at[k], p_send.at[k])
    for name in (*"52 42 53".split(), *"43 44 34 54".split()):
        stage(name)
    for k in range(early, per):
        drain(k)


def store_kernel(src, dst, sem):
    blocks = src.shape[0] // sem.shape[0]
    copies = [pltpu.make_async_copy(src.at[pl.ds(i * blocks, blocks)], dst.at[pl.ds(i * blocks, blocks)], sem.at[i]) for i in range(sem.shape[0])]
    start(copies)
    wait(copies)


def rope_rows(seq_len, head_dim, copies):
    inv_freq = ROPE_BASE ** (-2.0 * np.arange(head_dim // 2) / head_dim)
    angles = np.arange(seq_len)[:, None] * inv_freq[None, :]
    cos, sin = np.cos(angles), np.sin(angles)
    return [np.tile(np.concatenate(halves, 1), (copies, 1)).astype(np.float32) for halves in ((cos, cos), (-sin, sin))]


def solution(mesh):
    n_dp, n_tp = mesh.shape["dp"], mesh.shape["tp"]
    nz = n_tp // 2
    any_spec = pl.BlockSpec(memory_space=pl.ANY)
    vmem_spec = pl.BlockSpec(memory_space=pltpu.VMEM)
    dma = pltpu.SemaphoreType.DMA

    def sems(counts):
        return [dma((int(count),)) for count in counts.split()]

    def shard_body(act_in, ln_gain, ln_bias, w_qkv, w_out, w_up, w_down):
        n_seq, seq_len, d_model = act_in.shape
        layers, _, _, qkv_cols = w_qkv.shape
        head_dim, ff = w_out.shape[1], w_up.shape[2]
        per = n_seq // n_tp
        half = per // 2
        heads = n_tp // 4
        tile = 4 * seq_len
        w_qkv = w_qkv.reshape(layers, d_model, qkv_cols)
        cos, sin = rope_rows(seq_len, head_dim, 4)
        seq_block = (seq_len, d_model)
        n_cols, n_rows = n_tp + 3 * heads, n_tp + heads
        steps = nz * half
        gathered = pl.pallas_call(
            functools.partial(kernel, n_dp, n_tp),
            name="two_layers",
            out_shape=(pltpu.VMEM(act_in.shape, BF16), jax.ShapeDtypeStruct((n_cols, d_model, LANES), BF16), jax.ShapeDtypeStruct((n_rows, LANES, d_model), BF16)),
            in_specs=[any_spec] * 9,
            out_specs=(vmem_spec, any_spec, any_spec),
            scratch_shapes=[
                pltpu.VMEM(ln_gain.shape, F32), pltpu.VMEM(ln_bias.shape, F32), pltpu.VMEM(cos.shape, F32), pltpu.VMEM(sin.shape, F32), pltpu.VMEM((per, *seq_block), BF16),
                pltpu.VMEM((d_model, 2 * qkv_cols), BF16), pltpu.VMEM((2 * head_dim, d_model), BF16), pltpu.VMEM((2, d_model, ff // 2), BF16), pltpu.VMEM((2, ff // 2, d_model), BF16),
                pltpu.VMEM((tile, d_model), BF16), pltpu.VMEM((tile, head_dim), BF16), pltpu.VMEM((tile, ff), BF16), pltpu.VMEM((2, 2 * seq_len, d_model), F32),
                pltpu.VMEM((per, tile, d_model), BF16), pltpu.VMEM((4, tile, d_model), F32), pltpu.VMEM((per, 3, *seq_block), BF16),
                pltpu.VMEM((4, d_model, LANES), BF16), pltpu.VMEM((2, LANES, d_model), BF16),
                *sems("6 3 2 4"), dma((2,)), dma((2, (nz - 1) * (half - 1))), dma((2,)),
                *sems("6 6 6"), dma((2, nz // 2, 6)), dma((nz + 1,)), *sems("6 4"), dma((3, 2)), *sems("6 6 4 6"), dma((per,)),
            ],
            compiler_params=pltpu.CompilerParams(collective_id=1, has_side_effects=True, vmem_limit_bytes=39 * MIB),
        )(act_in, ln_gain, ln_bias, cos, sin, w_qkv, w_out, w_up, w_down)[0]
        return pl.pallas_call(
            store_kernel,
            name="store",
            out_shape=jax.ShapeDtypeStruct(act_in.shape, BF16),
            in_specs=[vmem_spec],
            out_specs=any_spec,
            scratch_shapes=[dma((n_tp,))],
            compiler_params=pltpu.CompilerParams(vmem_limit_bytes=MIB),
        )(pltpu.with_memory_space_constraint(gathered, pltpu.VMEM))

    return jax.shard_map(shard_body, mesh=mesh, in_specs=(P("dp"), P(), P(), P(None, None, "tp"), P(None, "tp"), P(None, None, "tp"), P(None, "tp")), out_specs=P("dp"), check_vma=False)
```

```python
import functools
import math

import jax
import jax.numpy as jnp
import numpy as np
from jax import lax
from jax.experimental import pallas as pl
from jax.experimental.pallas import tpu as pltpu
from jax.sharding import PartitionSpec as P

LN_EPS = 1e-5
ROPE_BASE = 10000.0
MESH = pl.DeviceIdType.MESH
BF16 = jnp.bfloat16
F32 = jnp.float32
LANES = 128
MIB = 1 << 20
SIDES = range(2)
PEERS = range(3)
UP, Q, K, V, DOWN, OUT = range(6)


def norm_rows(hidden_f, gain, bias):
    row_mean = jnp.mean(hidden_f, axis=-1, keepdims=True)
    centered = hidden_f - row_mean
    row_var = jnp.mean(centered * centered, axis=-1, keepdims=True)
    return (centered * lax.rsqrt(row_var + LN_EPS) * gain + bias).astype(BF16)


def rope(heads, cos, sin):
    return (heads * cos + pltpu.roll(heads, heads.shape[-1] // 2, 1) * sin).astype(BF16)


def gelu(values):
    return (0.5 * values * (1.0 + lax.erf(values * math.sqrt(0.5)))).astype(BF16)


def attend(query, keys, values, seq_len):
    rows, head_dim = query.shape
    block = 2 * seq_len
    row = lax.broadcasted_iota(jnp.int32, (block, block), 0)
    col = lax.broadcasted_iota(jnp.int32, (block, block), 1)
    allowed = (row >= col) & (row // seq_len == col // seq_len)
    contexts = []
    for first in range(0, rows, block):
        at = slice(first, first + block)
        scores = lax.dot_general(query[at], keys[at], (((1,), (1,)), ((), ())), preferred_element_type=F32) * (head_dim ** -0.5)
        scores = jnp.where(allowed, scores, -1e30)
        weights = jnp.exp(scores - jnp.max(scores, axis=-1, keepdims=True))
        probs = (weights / jnp.sum(weights, axis=-1, keepdims=True)).astype(BF16)
        contexts.append(jnp.dot(probs, values[at], preferred_element_type=F32).astype(BF16))
    return jnp.concatenate(contexts, axis=0)


def context_of(proj, cos_ref, sin_ref, seq_len):
    head_dim = cos_ref.shape[1]
    query = rope(proj[:, :head_dim], cos_ref[...], sin_ref[...])
    keys = rope(proj[:, head_dim : 2 * head_dim], cos_ref[...], sin_ref[...])
    return attend(query, keys, proj[:, 2 * head_dim :].astype(BF16), seq_len)


def head_context(normed, qkv_w, cos_ref, sin_ref, seq_len):
    return context_of(jnp.dot(normed, qkv_w, preferred_element_type=F32), cos_ref, sin_ref, seq_len)


class Place:
    def __init__(self, n_dp, n_tp):
        side = math.isqrt(n_dp)
        assert side * side == n_dp and side % 2 == 0 and n_tp % 4 == 0
        self.n_tp, self.nz = n_tp, n_tp // 2
        self.dp, self.tp = lax.axis_index("dp"), lax.axis_index("tp")
        self.z, self.core = self.tp // 2, self.tp % 2
        x, y = self.dp // side, self.dp % side
        xf, yf = x + 1 - 2 * (x % 2), y + 1 - 2 * (y % 2)
        self.q = (x % 2) * 2 + y % 2
        self.peers = [{"dp": xf * side + y}, {"dp": x * side + yf}, {"dp": xf * side + yf}]
        self.peer_q = [(1 - x % 2) * 2 + y % 2, (x % 2) * 2 + 1 - y % 2, (1 - x % 2) * 2 + 1 - y % 2]
        self.sib = {"tp": 2 * self.z + 1 - self.core}
        self.right = {"tp": 2 * ((self.z + 1) % self.nz) + self.core}
        self.left = {"tp": 2 * ((self.z + self.nz - 1) % self.nz) + self.core}

    def z_at(self, side, s):
        return (self.z + self.nz - s) % self.nz if side == 0 else (self.z + s) % self.nz

    def others(self):
        return [self.sib, self.right, self.left, *self.peers]

    def greet(self):
        barrier = pltpu.get_barrier_semaphore()
        for other in self.others():
            pl.semaphore_signal(barrier, inc=1, device_id=other, device_id_type=MESH)

    def meet(self):
        pl.semaphore_wait(pltpu.get_barrier_semaphore(), len(self.others()))


def remote(src, dst, send_sem, recv_sem, device):
    return pltpu.make_async_remote_copy(src_ref=src, dst_ref=dst, send_sem=send_sem, recv_sem=recv_sem, device_id=device, device_id_type=MESH)


def piece(kind, source, n_tp, cols, rows):
    if kind == UP:
        return cols.at[source]
    if kind == DOWN:
        return rows.at[source]
    head = source // 8 * 2 + source % 2
    if kind == OUT:
        return rows.at[n_tp + head]
    return cols.at[n_tp + 3 * head + kind - Q]


class SecondLayer:
    def __init__(self, place, nall, acc, qkv_v, out_v, up_v, down_v, gcols, grows, cos_ref, sin_ref, sem):
        self.place, self.nall, self.acc, self.sem = place, nall, acc, sem
        self.qkv_v, self.out_v, self.up_v, self.down_v = qkv_v, out_v, up_v, down_v
        self.gcols, self.grows, self.cos_ref, self.sin_ref = gcols, grows, cos_ref, sin_ref
        self.seq_len = nall.shape[1] // 4
        far = place.nz // 2
        self.order = [(0, 0)] + [(side, s) for s in range(1, far) for side in SIDES] + [(0, far)]

    def slab_loads(self, number):
        slot, zs = number % 2, self.place.z_at(*self.order[number])
        copies = []
        for c in SIDES:
            at = pl.ds(c * LANES, LANES)
            copies.append((self.gcols.at[2 * zs + c], self.up_v.at[slot, :, at], self.sem.at[slot, 0]))
            copies.append((self.grows.at[2 * zs + c], self.down_v.at[slot, at, :], self.sem.at[slot, 1]))
        return [pltpu.make_async_copy(*copy) for copy in copies]

    def head_loads(self, first):
        n_tp, head_dim = self.place.n_tp, self.cos_ref.shape[1]
        copies = []
        for n in SIDES:
            for i in range(3):
                at = pl.ds((3 * n + i) * head_dim, head_dim)
                copies.append((self.gcols.at[n_tp + 3 * (first + n) + i], self.qkv_v.at[:, at], self.sem.at[2, 0]))
            copies.append((self.grows.at[n_tp + first + n], self.out_v.at[pl.ds(n * head_dim, head_dim)], self.sem.at[2, 1]))
        return [pltpu.make_async_copy(*copy) for copy in copies]

    def wait_slab(self, number):
        slot = number % 2
        settle(self.up_v.at[slot], self.sem.at[slot, 0])
        settle(self.down_v.at[slot], self.sem.at[slot, 1])

    def wait_heads(self):
        settle(self.qkv_v, self.sem.at[2, 0])
        settle(self.out_v, self.sem.at[2, 1])

    def clear(self, tiles):
        for i in tiles:
            self.acc[i] = jnp.zeros(self.acc.shape[1:], F32)

    def slab(self, slot, p):
        nall, acc = self.nall, self.acc
        pair, kept = (2 * p, 2 * p + 1), acc.shape[0]
        hidden = [gelu(jnp.dot(nall[i], self.up_v[slot], preferred_element_type=F32)) for i in pair]
        step = 512
        for first in range(0, acc.shape[2], step):
            cols = pl.ds(first, step)
            for i, rows in zip(pair, hidden):
                acc[i % kept, :, cols] += jnp.dot(rows, self.down_v[slot, :, cols], preferred_element_type=F32)

    def heads(self, i):
        nall, acc, head_dim = self.nall, self.acc, self.cos_ref.shape[1]
        proj = jnp.dot(nall[i], self.qkv_v[...], preferred_element_type=F32)
        both = [context_of(proj[:, 3 * head_dim * n : 3 * head_dim * (n + 1)], self.cos_ref, self.sin_ref, self.seq_len) for n in SIDES]
        context = jnp.concatenate(both, axis=1)
        step = 512
        for first in range(0, acc.shape[2], step):
            cols = pl.ds(first, step)
            acc[i % acc.shape[0], :, cols] += jnp.dot(context, self.out_v[:, cols], preferred_element_type=F32)

    def round_off(self, i):
        self.nall[i] = self.acc[i % self.acc.shape[0]].astype(BF16)

    def run(self, program, actions, late_step=None):
        steps, events, late = [], [], None

        def end(unit):
            nonlocal events, late
            steps.append((events, late, unit))
            events, late = [], None

        for word in " ".join(program).split():
            letter, rest = word[0], word[1:]
            if letter in "SH":
                end([int(digit) for digit in rest])
                continue
            if late is not None:
                end([])
            if letter == "R":
                late = int(rest)
            else:
                events.append(functools.partial(actions[letter], rest))
        if events or late is not None:
            end([])

        def pick(values, default):
            def at(u):
                found = jnp.int32(default)
                for k, value in enumerate(values):
                    if value is not None:
                        found = jnp.where(u == k, value, found)
                return found
            return at

        late = pick([step[1] for step in steps], -1)
        slab = [step[2] if len(step[2]) == 2 else [None, None] for step in steps]
        slot = pick([number if number is None else number % 2 for number, _ in slab], -1)
        pair = pick([p for _, p in slab], 0)
        tile = pick([step[2][0] if len(step[2]) == 1 else None for step in steps], -1)

        def turn(u, carry):
            for k, step in enumerate(steps):
                if step[0]:
                    @pl.when(u == k)
                    def _():
                        for event in step[0]:
                            event()

            if late_step:
                @pl.when(late(u) >= 0)
                def _():
                    late_step(late(u))

            @pl.when(slot(u) >= 0)
            def _():
                self.slab(slot(u), pair(u))

            @pl.when(tile(u) >= 0)
            def _():
                self.heads(tile(u))

            return carry

        lax.fori_loop(0, len(steps), turn, 0)


def settle(ref, sem):
    pltpu.make_async_copy(ref, ref, sem).wait()


def start(copies):
    for copy in copies:
        copy.start()


def wait(copies):
    for copy in copies:
        copy.wait()


def kernel(n_dp, n_tp, x, gains_h, biases_h, cos_h, sin_h, qkv, out_w, up, down,
           out, gcols, grows,
           gains, biases, cos_ref, sin_ref, done, qkv_v, out_v, up_v, down_v, normed, ctx, act, own, nall, acc, part_in, st_cols, st_rows,
           w_sem, x_sem, sib_send, sib_recv, r_send, r_recv, e_send,
           st_sem, loc_sem, w_send, wr_recv, ws_recv, n_send, n_recv, slab_sem, p_send, p_recv, small_sem, g_send, s_recv):
    me = Place(n_dp, n_tp)
    me.greet()
    nz, core, z, q = me.nz, me.core, me.z, me.q
    n_seq, seq_len, d_model = x.shape
    head_dim, ff = out_w.shape[1], up.shape[2]
    per = n_seq // n_tp
    half = per // 2
    steps = nz * half

    wide = ff // 2
    assert (per, nz, n_tp // 4) == (6, 8, 4)

    def ring_at(side, i):
        s, j = i // half, i % half
        return jnp.where(j == half - 1, per * (2 * s + side) + j, per * s + half * side + j)

    def loc_at(side, s):
        return per * (2 * s + side) + per - 1

    def sib_in(i):
        return out.at[pl.ds(per * (nz + i % 4), 2)]

    def sib_out(i):
        return out.at[pl.ds(per * (nz + 4 + i % 2), 2)]

    def x_at(i, place):
        return per * (nz + 2 * (i % 3) + place // 2) + half + place % 2

    first_w = [pltpu.make_async_copy(src, dst, w_sem.at[i]) for i, (src, dst) in
               enumerate(((qkv.at[0], qkv_v.at[:, pl.ds(0, qkv.shape[2])]), (up.at[0, :, pl.ds(0, wide)], up_v.at[0]), (up.at[0, :, pl.ds(wide, wide)], up_v.at[1]),
                         (out_w.at[0], out_v.at[pl.ds(0, head_dim)]), (down.at[0, pl.ds(0, wide)], down_v.at[0]), (down.at[0, pl.ds(wide, wide)], down_v.at[1])))]

    def owner_seq(zo, co, j):
        return per * (2 * zo + co) + j

    def tile_seqs(i):
        s, j = i // half, i % half
        zr, zl = (z + 2 * nz - 1 - s) % nz, (z + 1 + s) % nz
        return [owner_seq(zr, core, j), owner_seq(zl, core, half + j), owner_seq(zr, 1 - core, j), owner_seq(zl, 1 - core, half + j)]

    def fetch(i):
        for place, seq in enumerate(tile_seqs(i)):
            pltpu.make_async_copy(x.at[seq], out.at[x_at(i, place)], x_sem.at[i % 3]).start()

    small = [pltpu.make_async_copy(src, dst, small_sem.at[i]) for i, (src, dst) in enumerate(((gains_h, gains), (biases_h, biases), (cos_h, cos_ref), (sin_h, sin_ref)))]
    loads = {UP: (up.at[1, :, pl.ds(pl.multiple_of(q * LANES, LANES), LANES)], st_cols.at[UP]),
             DOWN: (down.at[1, pl.ds(pl.multiple_of(q * LANES, LANES), LANES), :], st_rows.at[0]),
             OUT: (out_w.at[1], st_rows.at[1])}
    for kind in (Q, K, V):
        loads[kind] = (qkv.at[1, :, pl.ds((kind - Q) * head_dim, head_dim)], st_cols.at[kind])
    kinds = (Q, K, V, OUT, UP, DOWN)
    loads = {kind: pltpu.make_async_copy(*loads[kind], st_sem.at[kind]) for kind in kinds}

    loads[UP].start()
    fetch(0)
    start(small)
    start(first_w[:3])

    def start_rest():
        wait(small)
        start(first_w[3:])
        start([loads[kind] for kind in kinds if kind != UP])

    def has(kind, source):
        return source >= 0 if kind in (UP, DOWN) else (source // 2 + 2 * (source % 2)) % 4 == q

    def staged(kind):
        return st_rows.at[kind - DOWN] if kind >= DOWN else st_cols.at[kind]

    def piece_hops(kind):
        src, dst = staged(kind), piece(kind, me.tp, n_tp, gcols, grows)
        return [remote(src, dst, w_send.at[kind], wr_recv.at[0, 0, kind], me.right),
                remote(src, dst, w_send.at[kind], wr_recv.at[1, 0, kind], me.left),
                remote(src, dst, w_send.at[kind], sib_sem(z, kind), me.sib),
                pltpu.make_async_copy(src, dst, loc_sem.at[kind])]

    def sib_sem(zs, kind):
        return ws_recv.at[zs] if kind in (UP, DOWN) else ws_recv.at[nz]

    def send_first(kind):
        loads[kind].wait()

        @pl.when(has(kind, me.tp))
        def _():
            start(piece_hops(kind))

    for side in SIDES:
        for i in range(half):
            out[ring_at(side, i)] = jnp.zeros(out.shape[1:], BF16)

    to = (me.right, me.left)

    def send_sib(i):
        return remote(sib_out(i), sib_in(i), sib_send.at[i % 2], sib_recv.at[i % 4], me.sib)

    def send_ring(side, i):
        return remote(out.at[ring_at(side, i)], out.at[ring_at(side, i + half)], r_send.at[side], r_recv.at[side, i // half * (half - 1) + i % half], to[side])

    def rows_of(member):
        return pl.ds(pl.multiple_of(member * seq_len, seq_len), seq_len)

    def rows_sem(tile):
        return n_recv.at[tile - 2] if isinstance(tile, int) and tile >= per - 2 else n_recv.at[tile // 2]

    def send_n(tile, peer):
        at = nall.at[tile, rows_of(q)]
        return remote(at, at, n_send.at[tile], rows_sem(tile), me.peers[peer])

    def compute(i, waits=(), then=None):
        slot = i % 3
        settle(out.at[pl.ds(0, 4)], x_sem.at[slot])
        if then:
            then()

        @pl.when(i + 1 < steps)
        def _():
            fetch(i + 1)

        @pl.when(i >= 2)
        def _():
            send_sib(i - 2).wait_send()

        for member in range(4):
            normed[pl.ds(member * seq_len, seq_len), :] = norm_rows(out[x_at(i, member)].astype(F32), gains[pl.ds(0, 1), :], biases[pl.ds(0, 1), :])
        wait(waits[:3])
        ctx[...] = head_context(normed[...], qkv_v[:, : 3 * head_dim], cos_ref, sin_ref, seq_len)
        for n in SIDES:
            act[:, n * wide : (n + 1) * wide] = gelu(jnp.dot(normed[...], up_v[n], preferred_element_type=F32))
        wait(waits[3:])
        step = 512
        for first in range(0, d_model, step):
            cols = pl.ds(first, step)
            part = jnp.dot(ctx[...], out_v[:head_dim, cols], preferred_element_type=F32)
            for n in SIDES:
                part += jnp.dot(act[:, n * wide : (n + 1) * wide], down_v[n, :, cols], preferred_element_type=F32)
            own[i % 2, :, cols] = part[: 2 * seq_len]
            for side in SIDES:
                sib_out(i)[side, :, cols] = part[(2 + side) * seq_len : (3 + side) * seq_len].astype(BF16)

    def finish(i):
        send_sib(i).wait_recv()
        late = i % half == half - 1
        last = i >= steps - half

        def local(side, at):
            return own[i % 2, pl.ds(side * seq_len + at.start, at.size), :] + sib_in(i)[side, at, :].astype(F32)

        whole = pl.ds(0, seq_len)

        @pl.when(late)
        def _():
            for side in SIDES:
                out[loc_at(side, i // half)] = local(side, whole).astype(BF16)

        @pl.when(late & last)
        def _():
            for side in SIDES:
                done[per - 2 + side] = out[x_at(i, side)]

        @pl.when((i >= half) & jnp.logical_not(late))
        def _():
            for side in SIDES:
                send_ring(side, i - half).wait_recv()

        @pl.when(jnp.logical_not(last | late))
        def _():
            for side in SIDES:
                at = ring_at(side, i)
                out[at] = (local(side, whole) + out[at].astype(F32)).astype(BF16)
            for side in SIDES:
                send_ring(side, i).start()

        @pl.when(i == steps - half - 2)
        def _():
            for kind in kinds:
                if kind != UP:
                    send_first(kind)

        @pl.when(last & jnp.logical_not(late))
        def _():
            rows = seq_len // 2
            for side in SIDES:
                tile = 2 * (i % half) + side
                for h in SIDES:
                    at = pl.ds(h * rows, rows)
                    update = (local(side, at) + out[ring_at(side, i), at, :].astype(F32)).astype(BF16)
                    close(tile, at, out[x_at(i, side), at, :], update)
                start_n(tile)

    def close(tile, at, hidden, update):
        hidden = (hidden.astype(F32) + update.astype(F32)).astype(BF16)
        done[tile, at, :] = hidden
        mine = pl.ds(pl.multiple_of(q * seq_len + at.start, at.size), at.size)
        nall[tile, mine, :] = norm_rows(hidden.astype(F32), gains[pl.ds(1, 1), :], biases[pl.ds(1, 1), :])

    def start_n(tile):
        for peer in PEERS:
            send_n(tile, peer).start()

    me.meet()
    send_first(UP)
    compute(0, first_w, start_rest)
    send_sib(0).start()

    def turn(i, carry):
        @pl.when(i < steps)
        def _():
            compute(i)
            send_sib(i).start()

        finish(i - 1)
        return carry

    lax.fori_loop(1, steps + 1, turn, 0)

    def hops(side, kind):
        longer = (core + (kind in (Q, V, DOWN))) % 2
        return nz // 2 - longer if side == 0 else nz // 2 - 1 + longer

    def source_of(side, s):
        return 2 * me.z_at(side, s) + core

    def onward(side, s, kind):
        at = piece(kind, source_of(side, s), n_tp, gcols, grows)
        return remote(at, at, w_send.at[kind], wr_recv.at[side, s, kind], to[side])

    def arrival(side, s, kind):
        at = piece(kind, source_of(side, s), n_tp, gcols, grows)
        return remote(at, at, w_send.at[kind], wr_recv.at[side, s - 1, kind], to[side])

    def across(side, s, kind):
        source = source_of(side, s)
        at = piece(kind, source, n_tp, gcols, grows)
        return remote(at, at, w_send.at[kind], sib_sem(source // 2, kind), me.sib)

    def take(side, s, kind):
        @pl.when(has(kind, source_of(side, s)) & (s <= hops(side, kind)))
        def _():
            arrival(side, s, kind).wait_recv()

            @pl.when(s < hops(side, kind))
            def _():
                onward(side, s, kind).start()

            across(side, s, kind).start()

    def take_both(s, kind):
        for side in SIDES:
            take(side, s, kind)

    cut = seq_len // 2

    def late_send(side, s, h):
        at, i = pl.ds(h * cut, cut), half * s + half - 1
        return remote(out.at[ring_at(side, i), at], out.at[ring_at(side, i + half), at], e_send.at[side], r_recv.at[side, 2 * s + h], to[side])

    def late_step(s):
        for h in SIDES:
            at, i = pl.ds(h * cut, cut), half * s + half - 1
            for side in SIDES:
                @pl.when(s > 0)
                def _():
                    late_send(side, s - 1, h).wait_recv()

                total = (out[loc_at(side, s), at, :].astype(F32) + out[ring_at(side, i), at, :].astype(F32)).astype(BF16)

                @pl.when(s < nz - 1)
                def _():
                    out[ring_at(side, i), at, :] = total

                @pl.when(s == nz - 1)
                def _():
                    tile = per - 2 + side
                    close(tile, at, done[tile, at, :], total)

            @pl.when(s < nz - 1)
            def _():
                for side in SIDES:
                    late_send(side, s, h).start()

    layer = SecondLayer(me, nall, acc, qkv_v, out_v, up_v, down_v, gcols, grows, cos_ref, sin_ref, slab_sem)

    def start_slab(number):
        settle(gcols.at[pl.ds(0, 2)], ws_recv.at[me.z_at(*layer.order[number])])
        if number == 0:
            for kind in (UP, DOWN):
                piece_hops(kind)[3].wait()
        start(layer.slab_loads(number))

    def await_rows(which):
        if which < 2:
            settle(nall.at[pl.ds(2 * which, 2), pl.ds(0, 3 * seq_len)], n_recv.at[which])
        else:
            settle(nall.at[which, pl.ds(0, 3 * seq_len)], n_recv.at[which - 2])

    def send_part(k, peer):
        return remote(nall.at[k, rows_of(me.peer_q[peer])], part_in.at[k, peer], p_send.at[k], p_recv.at[k], me.peers[peer])

    def start_parts(k):
        for peer in PEERS:
            send_part(k, peer).start()

    def hand_out(k):
        settle(nall.at[k, pl.ds(0, 3 * seq_len)], n_send.at[k])
        layer.round_off(k)
        start_parts(k)

    def summed(k):
        settle(part_in.at[k], p_recv.at[k])
        total = acc[k % acc.shape[0], rows_of(q), :]
        for peer in PEERS:
            total = total + part_in[k, peer].astype(F32)
        return (done[k].astype(F32) + total.astype(BF16).astype(F32)).astype(BF16)

    def seq_of(zs, co, k):
        return per * (2 * zs + co) + k % 2 * half + k // 2

    def first_hops(k):
        at = out.at[seq_of(z, core, k)]
        return [remote(at, at, g_send.at[k], wr_recv.at[0, 0, k], me.right),
                remote(at, at, g_send.at[k], wr_recv.at[1, 0, k], me.left),
                remote(at, at, g_send.at[k], s_recv.at[k], me.sib)]

    def reach(side, k):
        longer = (k + core) % 2
        return nz // 2 - longer if side == 0 else nz // 2 - 1 + longer

    def passing(side, k, s, hop):
        at = out.at[seq_of(me.z_at(side, s), core, k)]
        return remote(at, at, g_send.at[k], wr_recv.at[side, hop, k], to[side])

    def stage(name):
        k, s = int(name[0]), int(name[1])
        if s == 0:
            out[seq_of(z, core, k)] = summed(k)
            start(first_hops(k))
            return
        for side in SIDES:
            @pl.when(s <= reach(side, k))
            def _():
                passing(side, k, s, s - 1).wait_recv()

                @pl.when(s < reach(side, k))
                def _():
                    passing(side, k, s, s).start()

                at = out.at[seq_of(me.z_at(side, s), core, k)]
                remote(at, at, g_send.at[k], s_recv.at[k], me.sib).start()

    def drain(k):
        settle(out.at[pl.ds(0, 2 * nz - 1)], g_send.at[k])
        settle(out.at[pl.ds(0, nz)], s_recv.at[k])

    def late_pair():
        start_n(per - 2)
        for side in SIDES:
            settle(out.at[pl.ds(0, nz - 1)], e_send.at[side])

    def drain_rings():
        for side in SIDES:
            settle(out.at[pl.ds(0, (nz - 1) * (half - 1))], r_send.at[side])
        send_sib(steps - 2).wait_send()
        send_sib(steps - 1).wait_send()

    def drain_weights():
        for kind in kinds:
            sent = jnp.where(has(kind, me.tp), 3, 0)
            for s in range(1, nz // 2 + 1):
                for side in SIDES:
                    here = has(kind, source_of(side, s))
                    sent += jnp.where(here & (s <= hops(side, kind)), 1, 0) + jnp.where(here & (s < hops(side, kind)), 1, 0)
            for count in [2 * nz - 1] if kind in (UP, DOWN) else [3, 4]:
                @pl.when(sent == count)
                def _():
                    settle(gcols.at[pl.ds(0, count)], w_send.at[kind])

    attn = (Q, K, V, OUT)

    def own_heads_kept():
        for kind in attn:
            @pl.when(has(kind, me.tp))
            def _():
                piece_hops(kind)[3].wait()

        settle(gcols.at[pl.ds(0, 2 * len(attn))], ws_recv.at[nz])

    layer.clear(range(acc.shape[0]))
    actions = {
        "T": lambda rest: take_both(int(rest[0]), letters[rest[1]]),
        "N": lambda rest: await_rows(int(rest)),
        "L": lambda rest: start_slab(int(rest)),
        "M": lambda rest: start(layer.slab_loads(int(rest))),
        "W": lambda rest: layer.wait_slab(int(rest)),
        "A": lambda rest: own_heads_kept(),
        "X": lambda rest: start(layer.head_loads(int(rest))),
        "Y": lambda rest: layer.wait_heads(),
        "P": lambda rest: hand_out(int(rest)),
        "B": lambda rest: drain_rings(),
        "Z": lambda rest: drain_weights(),
        "G": stage,
        "E": lambda rest: late_pair(),
        "F": lambda rest: layer.clear(SIDES),
        "I": lambda rest: start_n(per - 1),
    }
    letters = {"U": UP, "D": DOWN, "Q": Q, "K": K, "V": V, "O": OUT}
    layer.run([
        "L0 T1K T2K T1V",
        "T1O T2V T2O T1Q",
        "T2Q T1D N0 T3V",
        "T1U N1 W0 S00",
        "L1 S01 L2 T3K",
        "B W1 S10 S11",
        "T3Q T3O T4O T2D",
        "T2U T4K L3 T4Q",
        "T4V W2 S20 A",
        "X0 S21 L4 Y",
        "H0 H1 H2 H3",
        "X2 R0 W3 S30",
        "T3U S31 T3D L5",
        "W4 S40 S41 L6",
        "R1 Y H0 H1",
        "W5 S50 T4D W6",
        "S60 T4U R2 L7",
        "W7 S70 P0 R3",
        "P1 H2 R4 H3",
        "R5 S71 M5 X0",
        "R6 G00 R7 E",
        "G10 S61 M0 W5",
        "S51 M1 P2 I",
        "P3 F G01 G11",
        "G02 G20 N4 Y",
        "H4 G12 G21 G03",
        "N5 H5 X2 Z",
        "W0 S02 M2 W1",
        "S12 M3 W2 S22",
        "M4 W3 S32 M5",
        "G22 W4 S42 M6",
        "W5 S52 G30 M7",
        "W6 S62 W7 S72",
        "G13 Y H4 P4",
        "G04 G14 H5 G31",
        "P5",
    ], actions, late_step)
    stage("23")
    early = 2
    for k in range(early):
        drain(k)
    for name in (*"40 32 50".split(), *"41 51 42".split()):
        stage(name)
    for k in range(per):
        settle(part_in.at[k], p_send.at[k])
    for name in (*"52 33 43 53".split(), *"54 24 44 34".split()):
        stage(name)
    for k in range(early, per):
        drain(k)


def store_kernel(src, dst, sem):
    blocks = src.shape[0] // sem.shape[0]
    copies = [pltpu.make_async_copy(src.at[pl.ds(i * blocks, blocks)], dst.at[pl.ds(i * blocks, blocks)], sem.at[i]) for i in range(sem.shape[0])]
    start(copies)
    wait(copies)


def rope_rows(seq_len, head_dim, copies):
    inv_freq = ROPE_BASE ** (-2.0 * np.arange(head_dim // 2) / head_dim)
    angles = np.arange(seq_len)[:, None] * inv_freq[None, :]
    cos, sin = np.cos(angles), np.sin(angles)
    return [np.tile(np.concatenate(halves, 1), (copies, 1)).astype(np.float32) for halves in ((cos, cos), (-sin, sin))]


def solution(mesh):
    n_dp, n_tp = mesh.shape["dp"], mesh.shape["tp"]
    nz = n_tp // 2
    any_spec = pl.BlockSpec(memory_space=pl.ANY)
    vmem_spec = pl.BlockSpec(memory_space=pltpu.VMEM)
    dma = pltpu.SemaphoreType.DMA

    def sems(counts):
        return [dma((int(count),)) for count in counts.split()]

    def shard_body(act_in, ln_gain, ln_bias, w_qkv, w_out, w_up, w_down):
        n_seq, seq_len, d_model = act_in.shape
        layers, _, _, qkv_cols = w_qkv.shape
        head_dim, ff = w_out.shape[1], w_up.shape[2]
        per = n_seq // n_tp
        half = per // 2
        heads = n_tp // 4
        tile = 4 * seq_len
        w_qkv = w_qkv.reshape(layers, d_model, qkv_cols)
        cos, sin = rope_rows(seq_len, head_dim, 4)
        seq_block = (seq_len, d_model)
        n_cols, n_rows = n_tp + 3 * heads, n_tp + heads
        steps = nz * half
        gathered = pl.pallas_call(
            functools.partial(kernel, n_dp, n_tp),
            name="two_layers",
            out_shape=(pltpu.VMEM(act_in.shape, BF16), jax.ShapeDtypeStruct((n_cols, d_model, LANES), BF16), jax.ShapeDtypeStruct((n_rows, LANES, d_model), BF16)),
            in_specs=[any_spec] * 9,
            out_specs=(vmem_spec, any_spec, any_spec),
            scratch_shapes=[
                pltpu.VMEM(ln_gain.shape, F32), pltpu.VMEM(ln_bias.shape, F32), pltpu.VMEM(cos.shape, F32), pltpu.VMEM(sin.shape, F32), pltpu.VMEM((per, *seq_block), BF16),
                pltpu.VMEM((d_model, 2 * qkv_cols), BF16), pltpu.VMEM((2 * head_dim, d_model), BF16), pltpu.VMEM((2, d_model, ff // 2), BF16), pltpu.VMEM((2, ff // 2, d_model), BF16),
                pltpu.VMEM((tile, d_model), BF16), pltpu.VMEM((tile, head_dim), BF16), pltpu.VMEM((tile, ff), BF16), pltpu.VMEM((2, 2 * seq_len, d_model), F32),
                pltpu.VMEM((per, tile, d_model), BF16), pltpu.VMEM((4, tile, d_model), F32), pltpu.VMEM((per, 3, *seq_block), BF16),
                pltpu.VMEM((4, d_model, LANES), BF16), pltpu.VMEM((2, LANES, d_model), BF16),
                *sems("6 3 2 4"), dma((2,)), dma((2, (nz - 1) * (half - 1))), dma((2,)),
                *sems("6 6 6"), dma((2, nz // 2, 6)), dma((nz + 1,)), *sems("6 4"), dma((3, 2)), *sems("6 6 4 6"), dma((per,)),
            ],
            compiler_params=pltpu.CompilerParams(collective_id=1, has_side_effects=True, vmem_limit_bytes=39 * MIB),
        )(act_in, ln_gain, ln_bias, cos, sin, w_qkv, w_out, w_up, w_down)[0]
        return pl.pallas_call(
            store_kernel,
            name="store",
            out_shape=jax.ShapeDtypeStruct(act_in.shape, BF16),
            in_specs=[vmem_spec],
            out_specs=any_spec,
            scratch_shapes=[dma((n_tp,))],
            compiler_params=pltpu.CompilerParams(vmem_limit_bytes=MIB),
        )(pltpu.with_memory_space_constraint(gathered, pltpu.VMEM))

    return jax.shard_map(shard_body, mesh=mesh, in_specs=(P("dp"), P(), P(), P(None, None, "tp"), P(None, "tp"), P(None, None, "tp"), P(None, "tp")), out_specs=P("dp"), check_vma=False)
```

```python
import functools
import math

import jax
import jax.numpy as jnp
import numpy as np
from jax import lax
from jax.experimental import pallas as pl
from jax.experimental.pallas import tpu as pltpu
from jax.sharding import PartitionSpec as P

LN_EPS = 1e-5
ROPE_BASE = 10000.0
MESH = pl.DeviceIdType.MESH
BF16 = jnp.bfloat16
F32 = jnp.float32
LANES = 128
MIB = 1 << 20
SIDES = range(2)
PEERS = range(3)
UP, Q, K, V, DOWN, OUT = range(6)


def norm_rows(hidden_f, gain, bias):
    row_mean = jnp.mean(hidden_f, axis=-1, keepdims=True)
    centered = hidden_f - row_mean
    row_var = jnp.mean(centered * centered, axis=-1, keepdims=True)
    return (centered * lax.rsqrt(row_var + LN_EPS) * gain + bias).astype(BF16)


def rope(heads, cos, sin):
    return (heads * cos + pltpu.roll(heads, heads.shape[-1] // 2, 1) * sin).astype(BF16)


def gelu(values):
    return (0.5 * values * (1.0 + lax.erf(values * math.sqrt(0.5)))).astype(BF16)


def attend(query, keys, values, seq_len):
    rows, head_dim = query.shape
    block = 2 * seq_len
    row = lax.broadcasted_iota(jnp.int32, (block, block), 0)
    col = lax.broadcasted_iota(jnp.int32, (block, block), 1)
    allowed = (row >= col) & (row // seq_len == col // seq_len)
    contexts = []
    for first in range(0, rows, block):
        at = slice(first, first + block)
        scores = lax.dot_general(query[at], keys[at], (((1,), (1,)), ((), ())), preferred_element_type=F32) * (head_dim ** -0.5)
        scores = jnp.where(allowed, scores, -1e30)
        weights = jnp.exp(scores - jnp.max(scores, axis=-1, keepdims=True))
        probs = (weights / jnp.sum(weights, axis=-1, keepdims=True)).astype(BF16)
        contexts.append(jnp.dot(probs, values[at], preferred_element_type=F32).astype(BF16))
    return jnp.concatenate(contexts, axis=0)


def context_of(proj, cos_ref, sin_ref, seq_len):
    head_dim = cos_ref.shape[1]
    query = rope(proj[:, :head_dim], cos_ref[...], sin_ref[...])
    keys = rope(proj[:, head_dim : 2 * head_dim], cos_ref[...], sin_ref[...])
    return attend(query, keys, proj[:, 2 * head_dim :].astype(BF16), seq_len)


def head_context(normed, qkv_w, cos_ref, sin_ref, seq_len):
    return context_of(jnp.dot(normed, qkv_w, preferred_element_type=F32), cos_ref, sin_ref, seq_len)


class Place:
    def __init__(self, n_dp, n_tp):
        side = math.isqrt(n_dp)
        assert side * side == n_dp and side % 2 == 0 and n_tp % 4 == 0
        self.n_tp, self.nz = n_tp, n_tp // 2
        self.dp, self.tp = lax.axis_index("dp"), lax.axis_index("tp")
        self.z, self.core = self.tp // 2, self.tp % 2
        x, y = self.dp // side, self.dp % side
        xf, yf = x + 1 - 2 * (x % 2), y + 1 - 2 * (y % 2)
        self.q = (x % 2) * 2 + y % 2
        self.peers = [{"dp": xf * side + y}, {"dp": x * side + yf}, {"dp": xf * side + yf}]
        self.peer_q = [(1 - x % 2) * 2 + y % 2, (x % 2) * 2 + 1 - y % 2, (1 - x % 2) * 2 + 1 - y % 2]
        self.sib = {"tp": 2 * self.z + 1 - self.core}
        self.right = {"tp": 2 * ((self.z + 1) % self.nz) + self.core}
        self.left = {"tp": 2 * ((self.z + self.nz - 1) % self.nz) + self.core}

    def z_at(self, side, s):
        return (self.z + self.nz - s) % self.nz if side == 0 else (self.z + s) % self.nz

    def others(self):
        return [self.sib, self.right, self.left, *self.peers]

    def greet(self):
        barrier = pltpu.get_barrier_semaphore()
        for other in self.others():
            pl.semaphore_signal(barrier, inc=1, device_id=other, device_id_type=MESH)

    def meet(self):
        pl.semaphore_wait(pltpu.get_barrier_semaphore(), len(self.others()))


def remote(src, dst, send_sem, recv_sem, device):
    return pltpu.make_async_remote_copy(src_ref=src, dst_ref=dst, send_sem=send_sem, recv_sem=recv_sem, device_id=device, device_id_type=MESH)


def piece(kind, source, n_tp, cols, rows):
    if kind == UP:
        return cols.at[source]
    if kind == DOWN:
        return rows.at[source]
    head = source // 8 * 2 + source % 2
    if kind == OUT:
        return rows.at[n_tp + head]
    return cols.at[n_tp + 3 * head + kind - Q]


class SecondLayer:
    def __init__(self, place, nall, acc, qkv_v, out_v, up_v, down_v, gcols, grows, cos_ref, sin_ref, sem):
        self.place, self.nall, self.acc, self.sem = place, nall, acc, sem
        self.qkv_v, self.out_v, self.up_v, self.down_v = qkv_v, out_v, up_v, down_v
        self.gcols, self.grows, self.cos_ref, self.sin_ref = gcols, grows, cos_ref, sin_ref
        self.seq_len = nall.shape[1] // 4
        far = place.nz // 2
        self.order = [(0, 0)] + [(side, s) for s in range(1, far) for side in SIDES] + [(0, far)]

    def slab_loads(self, number):
        slot, zs = number % 2, self.place.z_at(*self.order[number])
        copies = []
        for c in SIDES:
            at = pl.ds(c * LANES, LANES)
            copies.append((self.gcols.at[2 * zs + c], self.up_v.at[slot, :, at], self.sem.at[slot, 0]))
            copies.append((self.grows.at[2 * zs + c], self.down_v.at[slot, at, :], self.sem.at[slot, 1]))
        return [pltpu.make_async_copy(*copy) for copy in copies]

    def head_loads(self, first):
        n_tp, head_dim = self.place.n_tp, self.cos_ref.shape[1]
        copies = []
        for n in SIDES:
            for i in range(3):
                at = pl.ds((3 * n + i) * head_dim, head_dim)
                copies.append((self.gcols.at[n_tp + 3 * (first + n) + i], self.qkv_v.at[:, at], self.sem.at[2, 0]))
            copies.append((self.grows.at[n_tp + first + n], self.out_v.at[pl.ds(n * head_dim, head_dim)], self.sem.at[2, 1]))
        return [pltpu.make_async_copy(*copy) for copy in copies]

    def wait_slab(self, number):
        slot = number % 2
        settle(self.up_v.at[slot], self.sem.at[slot, 0])
        settle(self.down_v.at[slot], self.sem.at[slot, 1])

    def wait_heads(self):
        settle(self.qkv_v, self.sem.at[2, 0])
        settle(self.out_v, self.sem.at[2, 1])

    def clear(self, tiles):
        for i in tiles:
            self.acc[i] = jnp.zeros(self.acc.shape[1:], F32)

    def slab(self, slot, p):
        nall, acc = self.nall, self.acc
        pair, kept = (2 * p, 2 * p + 1), acc.shape[0]
        hidden = [gelu(jnp.dot(nall[i], self.up_v[slot], preferred_element_type=F32)) for i in pair]
        step = 512
        for first in range(0, acc.shape[2], step):
            cols = pl.ds(first, step)
            for i, rows in zip(pair, hidden):
                acc[i % kept, :, cols] += jnp.dot(rows, self.down_v[slot, :, cols], preferred_element_type=F32)

    def heads(self, i):
        nall, acc, head_dim = self.nall, self.acc, self.cos_ref.shape[1]
        proj = jnp.dot(nall[i], self.qkv_v[...], preferred_element_type=F32)
        both = [context_of(proj[:, 3 * head_dim * n : 3 * head_dim * (n + 1)], self.cos_ref, self.sin_ref, self.seq_len) for n in SIDES]
        context = jnp.concatenate(both, axis=1)
        step = 512
        for first in range(0, acc.shape[2], step):
            cols = pl.ds(first, step)
            acc[i % acc.shape[0], :, cols] += jnp.dot(context, self.out_v[:, cols], preferred_element_type=F32)

    def round_off(self, i):
        self.nall[i] = self.acc[i % self.acc.shape[0]].astype(BF16)

    def run(self, program, actions, late_step=None):
        steps, events, late = [], [], None

        def end(unit):
            nonlocal events, late
            steps.append((events, late, unit))
            events, late = [], None

        for word in " ".join(program).split():
            letter, rest = word[0], word[1:]
            if letter in "SH":
                end([int(digit) for digit in rest])
                continue
            if late is not None:
                end([])
            if letter == "R":
                late = int(rest)
            else:
                events.append(functools.partial(actions[letter], rest))
        if events or late is not None:
            end([])

        def pick(values, default):
            def at(u):
                found = jnp.int32(default)
                for k, value in enumerate(values):
                    if value is not None:
                        found = jnp.where(u == k, value, found)
                return found
            return at

        late = pick([step[1] for step in steps], -1)
        slab = [step[2] if len(step[2]) == 2 else [None, None] for step in steps]
        slot = pick([number if number is None else number % 2 for number, _ in slab], -1)
        pair = pick([p for _, p in slab], 0)
        tile = pick([step[2][0] if len(step[2]) == 1 else None for step in steps], -1)

        def turn(u, carry):
            for k, step in enumerate(steps):
                if step[0]:
                    @pl.when(u == k)
                    def _():
                        for event in step[0]:
                            event()

            if late_step:
                @pl.when(late(u) >= 0)
                def _():
                    late_step(late(u))

            @pl.when(slot(u) >= 0)
            def _():
                self.slab(slot(u), pair(u))

            @pl.when(tile(u) >= 0)
            def _():
                self.heads(tile(u))

            return carry

        lax.fori_loop(0, len(steps), turn, 0)


def settle(ref, sem):
    pltpu.make_async_copy(ref, ref, sem).wait()


def start(copies):
    for copy in copies:
        copy.start()


def wait(copies):
    for copy in copies:
        copy.wait()


def kernel(n_dp, n_tp, x, gains_h, biases_h, cos_h, sin_h, qkv, out_w, up, down,
           out, gcols, grows,
           gains, biases, cos_ref, sin_ref, done, qkv_v, out_v, up_v, down_v, normed, ctx, act, own, nall, acc, part_in, st_cols, st_rows,
           w_sem, x_sem, sib_send, sib_recv, r_send, r_recv, e_send,
           st_sem, loc_sem, w_send, wr_recv, ws_recv, n_send, n_recv, slab_sem, p_send, p_recv, small_sem, g_send, s_recv):
    me = Place(n_dp, n_tp)
    me.greet()
    nz, core, z, q = me.nz, me.core, me.z, me.q
    n_seq, seq_len, d_model = x.shape
    head_dim, ff = out_w.shape[1], up.shape[2]
    per = n_seq // n_tp
    half = per // 2
    steps = nz * half

    wide = ff // 2
    assert (per, nz, n_tp // 4) == (6, 8, 4)

    def ring_at(side, i):
        s, j = i // half, i % half
        return jnp.where(j == half - 1, per * (2 * s + side) + j, per * s + half * side + j)

    def loc_at(side, s):
        return per * (2 * s + side) + per - 1

    def sib_in(i):
        return out.at[pl.ds(per * (nz + i % 4), 2)]

    def sib_out(i):
        return out.at[pl.ds(per * (nz + 4 + i % 2), 2)]

    def x_at(i, place):
        return per * (nz + 2 * (i % 3) + place // 2) + half + place % 2

    first_w = [pltpu.make_async_copy(src, dst, w_sem.at[i]) for i, (src, dst) in
               enumerate(((qkv.at[0], qkv_v.at[:, pl.ds(0, qkv.shape[2])]), (up.at[0, :, pl.ds(0, wide)], up_v.at[0]), (up.at[0, :, pl.ds(wide, wide)], up_v.at[1]),
                         (out_w.at[0], out_v.at[pl.ds(0, head_dim)]), (down.at[0, pl.ds(0, wide)], down_v.at[0]), (down.at[0, pl.ds(wide, wide)], down_v.at[1])))]

    def owner_seq(zo, co, j):
        return per * (2 * zo + co) + j

    def tile_seqs(i):
        s, j = i // half, i % half
        zr, zl = (z + 2 * nz - 1 - s) % nz, (z + 1 + s) % nz
        return [owner_seq(zr, core, j), owner_seq(zl, core, half + j), owner_seq(zr, 1 - core, j), owner_seq(zl, 1 - core, half + j)]

    def fetch(i):
        for place, seq in enumerate(tile_seqs(i)):
            pltpu.make_async_copy(x.at[seq], out.at[x_at(i, place)], x_sem.at[i % 3]).start()

    small = [pltpu.make_async_copy(src, dst, small_sem.at[i]) for i, (src, dst) in enumerate(((gains_h, gains), (biases_h, biases), (cos_h, cos_ref), (sin_h, sin_ref)))]
    loads = {UP: (up.at[1, :, pl.ds(pl.multiple_of(q * LANES, LANES), LANES)], st_cols.at[UP]),
             DOWN: (down.at[1, pl.ds(pl.multiple_of(q * LANES, LANES), LANES), :], st_rows.at[0]),
             OUT: (out_w.at[1], st_rows.at[1])}
    for kind in (Q, K, V):
        loads[kind] = (qkv.at[1, :, pl.ds((kind - Q) * head_dim, head_dim)], st_cols.at[kind])
    kinds = (Q, K, V, OUT, UP, DOWN)
    loads = {kind: pltpu.make_async_copy(*loads[kind], st_sem.at[kind]) for kind in kinds}

    loads[UP].start()
    fetch(0)
    start(small)
    start(first_w[:3])

    def start_rest():
        wait(small)
        start(first_w[3:])
        start([loads[kind] for kind in kinds if kind != UP])

    def has(kind, source):
        return source >= 0 if kind in (UP, DOWN) else (source // 2 + 2 * (source % 2)) % 4 == q

    def staged(kind):
        return st_rows.at[kind - DOWN] if kind >= DOWN else st_cols.at[kind]

    def piece_hops(kind):
        src, dst = staged(kind), piece(kind, me.tp, n_tp, gcols, grows)
        return [remote(src, dst, w_send.at[kind], wr_recv.at[0, 0, kind], me.right),
                remote(src, dst, w_send.at[kind], wr_recv.at[1, 0, kind], me.left),
                remote(src, dst, w_send.at[kind], sib_sem(z, kind), me.sib),
                pltpu.make_async_copy(src, dst, loc_sem.at[kind])]

    def sib_sem(zs, kind):
        return ws_recv.at[zs] if kind in (UP, DOWN) else ws_recv.at[nz]

    def send_first(kind):
        loads[kind].wait()

        @pl.when(has(kind, me.tp))
        def _():
            start(piece_hops(kind))

    for side in SIDES:
        for i in range(half):
            out[ring_at(side, i)] = jnp.zeros(out.shape[1:], BF16)

    to = (me.right, me.left)

    def send_sib(i):
        return remote(sib_out(i), sib_in(i), sib_send.at[i % 2], sib_recv.at[i % 4], me.sib)

    def send_ring(side, i):
        return remote(out.at[ring_at(side, i)], out.at[ring_at(side, i + half)], r_send.at[side], r_recv.at[side, i // half * (half - 1) + i % half], to[side])

    def rows_of(member):
        return pl.ds(pl.multiple_of(member * seq_len, seq_len), seq_len)

    def rows_sem(tile):
        return n_recv.at[tile - 2] if isinstance(tile, int) and tile >= per - 2 else n_recv.at[tile // 2]

    def send_n(tile, peer):
        at = nall.at[tile, rows_of(q)]
        return remote(at, at, n_send.at[tile], rows_sem(tile), me.peers[peer])

    def compute(i, waits=(), then=None):
        slot = i % 3
        settle(out.at[pl.ds(0, 4)], x_sem.at[slot])
        if then:
            then()

        @pl.when(i + 1 < steps)
        def _():
            fetch(i + 1)

        @pl.when(i >= 2)
        def _():
            send_sib(i - 2).wait_send()

        for member in range(4):
            normed[pl.ds(member * seq_len, seq_len), :] = norm_rows(out[x_at(i, member)].astype(F32), gains[pl.ds(0, 1), :], biases[pl.ds(0, 1), :])
        wait(waits[:3])
        ctx[...] = head_context(normed[...], qkv_v[:, : 3 * head_dim], cos_ref, sin_ref, seq_len)
        for n in SIDES:
            act[:, n * wide : (n + 1) * wide] = gelu(jnp.dot(normed[...], up_v[n], preferred_element_type=F32))
        wait(waits[3:])
        step = 512
        for first in range(0, d_model, step):
            cols = pl.ds(first, step)
            part = jnp.dot(ctx[...], out_v[:head_dim, cols], preferred_element_type=F32)
            for n in SIDES:
                part += jnp.dot(act[:, n * wide : (n + 1) * wide], down_v[n, :, cols], preferred_element_type=F32)
            own[i % 2, :, cols] = part[: 2 * seq_len]
            for side in SIDES:
                sib_out(i)[side, :, cols] = part[(2 + side) * seq_len : (3 + side) * seq_len].astype(BF16)

    def finish(i):
        send_sib(i).wait_recv()
        late = i % half == half - 1
        last = i >= steps - half

        def local(side, at):
            return own[i % 2, pl.ds(side * seq_len + at.start, at.size), :] + sib_in(i)[side, at, :].astype(F32)

        whole = pl.ds(0, seq_len)

        @pl.when(late)
        def _():
            for side in SIDES:
                out[loc_at(side, i // half)] = local(side, whole).astype(BF16)

        @pl.when(late & last)
        def _():
            for side in SIDES:
                done[per - 2 + side] = out[x_at(i, side)]

        @pl.when((i >= half) & jnp.logical_not(late))
        def _():
            for side in SIDES:
                send_ring(side, i - half).wait_recv()

        @pl.when(jnp.logical_not(last | late))
        def _():
            for side in SIDES:
                at = ring_at(side, i)
                out[at] = (local(side, whole) + out[at].astype(F32)).astype(BF16)
            for side in SIDES:
                send_ring(side, i).start()

        @pl.when(i == steps - half - 2)
        def _():
            for kind in kinds:
                if kind != UP:
                    send_first(kind)

        @pl.when(last & jnp.logical_not(late))
        def _():
            rows = seq_len // 2
            for side in SIDES:
                tile = 2 * (i % half) + side
                for h in SIDES:
                    at = pl.ds(h * rows, rows)
                    update = (local(side, at) + out[ring_at(side, i), at, :].astype(F32)).astype(BF16)
                    close(tile, at, out[x_at(i, side), at, :], update)
                start_n(tile)

    def close(tile, at, hidden, update):
        hidden = (hidden.astype(F32) + update.astype(F32)).astype(BF16)
        done[tile, at, :] = hidden
        mine = pl.ds(pl.multiple_of(q * seq_len + at.start, at.size), at.size)
        nall[tile, mine, :] = norm_rows(hidden.astype(F32), gains[pl.ds(1, 1), :], biases[pl.ds(1, 1), :])

    def start_n(tile):
        for peer in PEERS:
            send_n(tile, peer).start()

    me.meet()
    send_first(UP)
    compute(0, first_w, start_rest)
    send_sib(0).start()

    def turn(i, carry):
        @pl.when(i < steps)
        def _():
            compute(i)
            send_sib(i).start()

        finish(i - 1)
        return carry

    lax.fori_loop(1, steps + 1, turn, 0)

    def hops(side, kind):
        longer = (core + (kind in (Q, V, DOWN))) % 2
        return nz // 2 - longer if side == 0 else nz // 2 - 1 + longer

    def source_of(side, s):
        return 2 * me.z_at(side, s) + core

    def onward(side, s, kind):
        at = piece(kind, source_of(side, s), n_tp, gcols, grows)
        return remote(at, at, w_send.at[kind], wr_recv.at[side, s, kind], to[side])

    def arrival(side, s, kind):
        at = piece(kind, source_of(side, s), n_tp, gcols, grows)
        return remote(at, at, w_send.at[kind], wr_recv.at[side, s - 1, kind], to[side])

    def across(side, s, kind):
        source = source_of(side, s)
        at = piece(kind, source, n_tp, gcols, grows)
        return remote(at, at, w_send.at[kind], sib_sem(source // 2, kind), me.sib)

    def take(side, s, kind):
        @pl.when(has(kind, source_of(side, s)) & (s <= hops(side, kind)))
        def _():
            arrival(side, s, kind).wait_recv()

            @pl.when(s < hops(side, kind))
            def _():
                onward(side, s, kind).start()

            across(side, s, kind).start()

    def take_both(s, kind):
        for side in SIDES:
            take(side, s, kind)

    cut = seq_len // 2

    def late_send(side, s, h):
        at, i = pl.ds(h * cut, cut), half * s + half - 1
        return remote(out.at[ring_at(side, i), at], out.at[ring_at(side, i + half), at], e_send.at[side], r_recv.at[side, 2 * s + h], to[side])

    def late_step(s):
        for h in SIDES:
            at, i = pl.ds(h * cut, cut), half * s + half - 1
            for side in SIDES:
                @pl.when(s > 0)
                def _():
                    late_send(side, s - 1, h).wait_recv()

                total = (out[loc_at(side, s), at, :].astype(F32) + out[ring_at(side, i), at, :].astype(F32)).astype(BF16)

                @pl.when(s < nz - 1)
                def _():
                    out[ring_at(side, i), at, :] = total

                @pl.when(s == nz - 1)
                def _():
                    tile = per - 2 + side
                    close(tile, at, done[tile, at, :], total)

            @pl.when(s < nz - 1)
            def _():
                for side in SIDES:
                    late_send(side, s, h).start()

    layer = SecondLayer(me, nall, acc, qkv_v, out_v, up_v, down_v, gcols, grows, cos_ref, sin_ref, slab_sem)

    def start_slab(number):
        settle(gcols.at[pl.ds(0, 2)], ws_recv.at[me.z_at(*layer.order[number])])
        if number == 0:
            for kind in (UP, DOWN):
                piece_hops(kind)[3].wait()
        start(layer.slab_loads(number))

    def await_rows(which):
        if which < 2:
            settle(nall.at[pl.ds(2 * which, 2), pl.ds(0, 3 * seq_len)], n_recv.at[which])
        else:
            settle(nall.at[which, pl.ds(0, 3 * seq_len)], n_recv.at[which - 2])

    def send_part(k, peer):
        return remote(nall.at[k, rows_of(me.peer_q[peer])], part_in.at[k, peer], p_send.at[k], p_recv.at[k], me.peers[peer])

    def start_parts(k):
        for peer in PEERS:
            send_part(k, peer).start()

    def hand_out(k):
        settle(nall.at[k, pl.ds(0, 3 * seq_len)], n_send.at[k])
        layer.round_off(k)
        if k not in (2, 3):
            start_parts(k)

    def summed(k):
        settle(part_in.at[k], p_recv.at[k])
        total = acc[k % acc.shape[0], rows_of(q), :]
        for peer in PEERS:
            total = total + part_in[k, peer].astype(F32)
        return (done[k].astype(F32) + total.astype(BF16).astype(F32)).astype(BF16)

    def seq_of(zs, co, k):
        return per * (2 * zs + co) + k % 2 * half + k // 2

    def first_hops(k):
        at = out.at[seq_of(z, core, k)]
        return [remote(at, at, g_send.at[k], wr_recv.at[0, 0, k], me.right),
                remote(at, at, g_send.at[k], wr_recv.at[1, 0, k], me.left),
                remote(at, at, g_send.at[k], s_recv.at[k], me.sib)]

    def reach(side, k):
        longer = (k + core) % 2
        return nz // 2 - longer if side == 0 else nz // 2 - 1 + longer

    def passing(side, k, s, hop):
        at = out.at[seq_of(me.z_at(side, s), core, k)]
        return remote(at, at, g_send.at[k], wr_recv.at[side, hop, k], to[side])

    def stage(name):
        k, s = int(name[0]), int(name[1])
        if s == 0:
            out[seq_of(z, core, k)] = summed(k)
            start(first_hops(k))
            return
        for side in SIDES:
            @pl.when(s <= reach(side, k))
            def _():
                passing(side, k, s, s - 1).wait_recv()

                @pl.when(s < reach(side, k))
                def _():
                    passing(side, k, s, s).start()

                at = out.at[seq_of(me.z_at(side, s), core, k)]
                remote(at, at, g_send.at[k], s_recv.at[k], me.sib).start()

    def drain(k):
        settle(out.at[pl.ds(0, 2 * nz - 1)], g_send.at[k])
        settle(out.at[pl.ds(0, nz)], s_recv.at[k])

    def late_pair():
        start_parts(2)
        for side in SIDES:
            start_n(per - 2 + side)
        start_parts(3)
        for side in SIDES:
            settle(out.at[pl.ds(0, nz - 1)], e_send.at[side])

    def drain_rings():
        for side in SIDES:
            settle(out.at[pl.ds(0, (nz - 1) * (half - 1))], r_send.at[side])
        send_sib(steps - 2).wait_send()
        send_sib(steps - 1).wait_send()

    def drain_weights():
        for kind in kinds:
            sent = jnp.where(has(kind, me.tp), 3, 0)
            for s in range(1, nz // 2 + 1):
                for side in SIDES:
                    here = has(kind, source_of(side, s))
                    sent += jnp.where(here & (s <= hops(side, kind)), 1, 0) + jnp.where(here & (s < hops(side, kind)), 1, 0)
            for count in [2 * nz - 1] if kind in (UP, DOWN) else [3, 4]:
                @pl.when(sent == count)
                def _():
                    settle(gcols.at[pl.ds(0, count)], w_send.at[kind])

    attn = (Q, K, V, OUT)

    def own_heads_kept():
        for kind in attn:
            @pl.when(has(kind, me.tp))
            def _():
                piece_hops(kind)[3].wait()

        settle(gcols.at[pl.ds(0, 2 * len(attn))], ws_recv.at[nz])

    layer.clear(range(acc.shape[0]))
    actions = {
        "T": lambda rest: take_both(int(rest[0]), letters[rest[1]]),
        "N": lambda rest: await_rows(int(rest)),
        "L": lambda rest: start_slab(int(rest)),
        "M": lambda rest: start(layer.slab_loads(int(rest))),
        "W": lambda rest: layer.wait_slab(int(rest)),
        "A": lambda rest: own_heads_kept(),
        "X": lambda rest: start(layer.head_loads(int(rest))),
        "Y": lambda rest: layer.wait_heads(),
        "P": lambda rest: hand_out(int(rest)),
        "B": lambda rest: drain_rings(),
        "Z": lambda rest: drain_weights(),
        "G": stage,
        "E": lambda rest: late_pair(),
        "F": lambda rest: layer.clear(SIDES),
    }
    letters = {"U": UP, "D": DOWN, "Q": Q, "K": K, "V": V, "O": OUT}
    layer.run([
        "L0 T1K T2K T1V",
        "T1O T2V T2O T1Q",
        "T2Q T1D N0 T3V",
        "T1U N1 W0 S00",
        "L1 S01 L2 T3K",
        "B W1 S10 S11",
        "T3Q T3O T4O T2D",
        "T2U T4K L3 T4Q",
        "T4V W2 S20 A",
        "X0 S21 L4 Y",
        "H0 H1 H2 H3",
        "X2 R0 W3 S30",
        "T3U S31 T3D L5",
        "W4 S40 S41 L6",
        "R1 Y H0 H1",
        "W5 S50 T4D W6",
        "S60 T4U R2 L7",
        "W7 S70 P0 R3",
        "P1 H2 R4 H3",
        "R5 S71 M5 S61",
        "R6 W5 S51 P2",
        "P3 G00 R7 E",
        "Z M0 M1 X0",
        "G10 F G01 G20",
        "G11 G02 G12 N4",
        "G21 Y H4 G03",
        "N5 H5 X2 W0",
        "S02 M2 G13 W1",
        "S12 M3 W2 S22",
        "M4 W3 S32 M5",
        "G22 W4 S42 M6",
        "W5 S52 M7 W6",
        "S62 W7 S72 G30",
        "Y H4 P4 G23",
        "G31 H5 G14 P5",
    ], actions, late_step)
    for name in "04 24".split():
        stage(name)
    early = 2
    for k in range(early):
        drain(k)
    for name in (*"40 32 50".split(), *"41 51 33".split()):
        stage(name)
    for k in range(per):
        settle(part_in.at[k], p_send.at[k])
    for name in (*"52 42 53".split(), *"43 44 34 54".split()):
        stage(name)
    for k in range(early, per):
        drain(k)


def store_kernel(src, dst, sem):
    blocks = src.shape[0] // sem.shape[0]
    copies = [pltpu.make_async_copy(src.at[pl.ds(i * blocks, blocks)], dst.at[pl.ds(i * blocks, blocks)], sem.at[i]) for i in range(sem.shape[0])]
    start(copies)
    wait(copies)


def rope_rows(seq_len, head_dim, copies):
    inv_freq = ROPE_BASE ** (-2.0 * np.arange(head_dim // 2) / head_dim)
    angles = np.arange(seq_len)[:, None] * inv_freq[None, :]
    cos, sin = np.cos(angles), np.sin(angles)
    return [np.tile(np.concatenate(halves, 1), (copies, 1)).astype(np.float32) for halves in ((cos, cos), (-sin, sin))]


def solution(mesh):
    n_dp, n_tp = mesh.shape["dp"], mesh.shape["tp"]
    nz = n_tp // 2
    any_spec = pl.BlockSpec(memory_space=pl.ANY)
    vmem_spec = pl.BlockSpec(memory_space=pltpu.VMEM)
    dma = pltpu.SemaphoreType.DMA

    def sems(counts):
        return [dma((int(count),)) for count in counts.split()]

    def shard_body(act_in, ln_gain, ln_bias, w_qkv, w_out, w_up, w_down):
        n_seq, seq_len, d_model = act_in.shape
        layers, _, _, qkv_cols = w_qkv.shape
        head_dim, ff = w_out.shape[1], w_up.shape[2]
        per = n_seq // n_tp
        half = per // 2
        heads = n_tp // 4
        tile = 4 * seq_len
        w_qkv = w_qkv.reshape(layers, d_model, qkv_cols)
        cos, sin = rope_rows(seq_len, head_dim, 4)
        seq_block = (seq_len, d_model)
        n_cols, n_rows = n_tp + 3 * heads, n_tp + heads
        steps = nz * half
        gathered = pl.pallas_call(
            functools.partial(kernel, n_dp, n_tp),
            name="two_layers",
            out_shape=(pltpu.VMEM(act_in.shape, BF16), jax.ShapeDtypeStruct((n_cols, d_model, LANES), BF16), jax.ShapeDtypeStruct((n_rows, LANES, d_model), BF16)),
            in_specs=[any_spec] * 9,
            out_specs=(vmem_spec, any_spec, any_spec),
            scratch_shapes=[
                pltpu.VMEM(ln_gain.shape, F32), pltpu.VMEM(ln_bias.shape, F32), pltpu.VMEM(cos.shape, F32), pltpu.VMEM(sin.shape, F32), pltpu.VMEM((per, *seq_block), BF16),
                pltpu.VMEM((d_model, 2 * qkv_cols), BF16), pltpu.VMEM((2 * head_dim, d_model), BF16), pltpu.VMEM((2, d_model, ff // 2), BF16), pltpu.VMEM((2, ff // 2, d_model), BF16),
                pltpu.VMEM((tile, d_model), BF16), pltpu.VMEM((tile, head_dim), BF16), pltpu.VMEM((tile, ff), BF16), pltpu.VMEM((2, 2 * seq_len, d_model), F32),
                pltpu.VMEM((per, tile, d_model), BF16), pltpu.VMEM((4, tile, d_model), F32), pltpu.VMEM((per, 3, *seq_block), BF16),
                pltpu.VMEM((4, d_model, LANES), BF16), pltpu.VMEM((2, LANES, d_model), BF16),
                *sems("6 3 2 4"), dma((2,)), dma((2, (nz - 1) * (half - 1))), dma((2,)),
                *sems("6 6 6"), dma((2, nz // 2, 6)), dma((nz + 1,)), *sems("6 4"), dma((3, 2)), *sems("6 6 4 6"), dma((per,)),
            ],
            compiler_params=pltpu.CompilerParams(collective_id=1, has_side_effects=True, vmem_limit_bytes=39 * MIB),
        )(act_in, ln_gain, ln_bias, cos, sin, w_qkv, w_out, w_up, w_down)[0]
        return pl.pallas_call(
            store_kernel,
            name="store",
            out_shape=jax.ShapeDtypeStruct(act_in.shape, BF16),
            in_specs=[vmem_spec],
            out_specs=any_spec,
            scratch_shapes=[dma((n_tp,))],
            compiler_params=pltpu.CompilerParams(vmem_limit_bytes=MIB),
        )(pltpu.with_memory_space_constraint(gathered, pltpu.VMEM))

    return jax.shard_map(shard_body, mesh=mesh, in_specs=(P("dp"), P(), P(), P(None, None, "tp"), P(None, "tp"), P(None, None, "tp"), P(None, "tp")), out_specs=P("dp"), check_vma=False)
```
